128 devices in a mesh: patch: 128 (over y, z, x, core).
Axes of the slice: x: 4, y: 4, z: 4, core: 2. Of those that a mesh axis runs over, the one named last changes fastest.
Arguments:
- positions: float32 [3, 262144], P(None, 'patch'), may hold values from -6 to 6
- densities: float32 [3, 262144], P(None, 'patch'), may hold values from -6 to 6
- near_src: int32 [2048, 8], P('patch'), may hold values from 0 to 2047, as said below
- near_count: int32 [2048], P('patch'), may hold values from 1 to 8
- far_slot: int32 [2048, 32], P('patch'), may hold values from 0 to 511
- far_class: int32 [2048, 32], P('patch'), may hold values from 0 to 188
- far_count: int32 [2048], P('patch'), may hold values from 1 to 32
- requests: int32 [128, 128, 4], P('patch'), may hold values from 0 to 15, as said below
- up_basis: bfloat16 [2048, 144, 384], P('patch'), may hold values from -0.3125 to 0.3125
- transfer_table: bfloat16 [189, 20736], replicated, may hold values from -0.5 to 0.5
- down_basis: bfloat16 [2048, 144, 9, 128], P('patch'), may hold values from -0.09375 to 0.09375
Outputs:
- shape_grad: float32 [3, 262144], P(None, 'patch')
The draws below stay inside these ranges and needn't reach their ends.
Inputs may be any that keep to these rules, and one draw needn't show every extreme that they name: `near_src`: the source leaf of each near-field block is held by the device of its target leaf or by the device just before or after it along patch. `requests`: each row names 4 different leaves of the source device, by their index on that device.
All inputs are finite; a program needn't handle non-finite values.
Results may differ from the reference program's by a relative error of at most 0.0042.
Values may be sent and summed in bfloat16 or wider, within the bound.
No kernel may reach another device: no remote copies, remote signals or barrier semaphores. Data moves between devices by JAX's collectives and lax.ppermute only.
A program may use at most 192 MiB of HBM per device.

```python
import math
import jax
import jax.numpy as jnp
from jax import lax

P_SIZE = 128
RANK = 48
LEAF_DEV = 16
NEAR = 8
FAR = 32
CLASSES = 189
CAP = 4
LEAVES = 2048
NODES = 262144
SLOTS = 512
N_PATCH = 128


def draw_near_src(key, part):
    leaves = jnp.arange(LEAVES, dtype=jnp.int32)
    owner = leaves // LEAF_DEV
    last_dev = LEAVES // LEAF_DEV - 1
    span = jnp.where((owner == 0) | (owner == last_dev), 2 * LEAF_DEV, 3 * LEAF_DEV)
    lowest = jnp.where(owner == 0, 0, (owner - 1) * LEAF_DEV)
    raw = jax.random.randint(jax.random.fold_in(key, 11), (LEAVES, NEAR), 0, 1 << 30)
    return (lowest[:, None] + raw % span[:, None]).astype(jnp.int32)


def draw_near_count(key, part):
    first, second, third = jax.random.split(jax.random.fold_in(key, 12), 3)
    ndev = LEAVES // LEAF_DEV
    level = jax.random.randint(first, (ndev,), max(1, NEAR // 4), NEAR + 1)
    raw = jax.random.randint(second, (LEAVES,), 0, 1 << 30)
    count = 1 + raw % jnp.repeat(level, LEAF_DEV)
    chosen = jax.random.randint(third, (), 0, ndev)
    leaves = jnp.arange(LEAVES, dtype=jnp.int32)
    return jnp.where(leaves == chosen * LEAF_DEV, NEAR, count).astype(jnp.int32)


def draw_requests(key, part):
    ndev = LEAVES // LEAF_DEV
    scores = jax.random.randint(jax.random.fold_in(key, 13), (ndev, ndev, LEAF_DEV), 0, 1 << 20)
    scores = scores * LEAF_DEV + jnp.arange(LEAF_DEV, dtype=jnp.int32)
    order = jnp.argsort(scores, axis=-1, stable=True)
    return order[:, :, :CAP].astype(jnp.int32)


def with_ends(entries, own_key, least, top_value):
    longest = entries.shape.index(max(entries.shape))
    spots = []
    for shift in (0, 1):
        where = [jax.random.randint(jax.random.fold_in(own_key, axis), (), 0, length) for axis, length in enumerate(entries.shape)]
        where[longest] = (where[longest] + shift) % entries.shape[longest]
        spots.append(tuple(where))
    return entries.at[spots[0]].set(least).at[spots[1]].set(top_value)


def steps_of(stream_key, shape, cuts, low, high):
    def one(position, blocks):
        draws = jax.random.uniform(jax.random.fold_in(jax.random.fold_in(stream_key, 6), position), (blocks,), jnp.float32, low / len(cuts), high / len(cuts))
        return jnp.repeat(jnp.exp(draws), shape[position] // blocks).reshape((-1,) + (1,) * (len(shape) - position - 1))

    factor_of = one(*cuts[0])
    for cut in cuts[1:]:
        factor_of = factor_of * one(*cut)
    return factor_of


def gaussian(own_key, extent, spread, most, pieces=(), kind=jnp.bfloat16):
    gain = steps_of(own_key, extent, pieces, -0.22, 0.18) if pieces else 1.0
    entries = jax.random.normal(own_key, extent, jnp.float32) * spread * gain
    return jnp.minimum(jnp.maximum(entries, -most), most).astype(kind)


def setup_inputs(seed: int = 0) -> dict:
    splits = jax.random.split(jax.random.key(seed), 12)
    positions = gaussian(splits[0], (3, NODES), 1.0, 6.0, ((1, 128),), jnp.float32)
    densities = gaussian(splits[1], (3, NODES), 1.0, 6.0, ((1, 128),), jnp.float32)
    near_src = draw_near_src(jax.random.fold_in(splits[11], 71), 0)
    near_count = draw_near_count(jax.random.fold_in(splits[11], 71), 0)
    far_slot = with_ends(jax.random.randint(splits[4], (LEAVES, FAR), 0, SLOTS), jax.random.fold_in(splits[4], 1), 0, SLOTS - 1).astype(jnp.int32)
    far_class = with_ends(jax.random.randint(splits[5], (LEAVES, FAR), 0, CLASSES), jax.random.fold_in(splits[5], 1), 0, CLASSES - 1).astype(jnp.int32)
    far_count = with_ends(jax.random.randint(splits[6], (LEAVES,), 1, FAR + 1), jax.random.fold_in(splits[6], 1), 1, FAR).astype(jnp.int32)
    requests = draw_requests(jax.random.fold_in(splits[11], 71), 0)
    up_basis = gaussian(splits[8], (LEAVES, 3 * RANK, 3 * P_SIZE), (3 * P_SIZE) ** -0.5, 0.3125, ((0, 128),))
    transfer_table = gaussian(splits[9], (CLASSES, 9 * RANK * RANK), (3 * RANK) ** -0.5, 0.5)
    down_basis = gaussian(splits[10], (LEAVES, 3 * RANK, 9, P_SIZE), (3 * RANK * FAR) ** -0.5, 0.09375, ((0, 128),))
    return dict(positions=positions, densities=densities, near_src=near_src, near_count=near_count, far_slot=far_slot, far_class=far_class, far_count=far_count, requests=requests, up_basis=up_basis, transfer_table=transfer_table, down_basis=down_basis)


KERNEL = 1.0 / (8.0 * math.pi)
BLOB = 0.25

def pair_terms(target, source):
    xt = target[:, :3]
    ft = target[:, 3:]
    xs = source[:, :3]
    fs = source[:, 3:]
    sep = xt[:, :, :, None] - xs[:, :, None, :]
    rho_sq = lax.optimization_barrier(jnp.sum(sep * sep, axis=1)) + BLOB
    inv_one = lax.rsqrt(rho_sq)
    inv_three = inv_one / rho_sq
    inv_five = inv_three / rho_sq
    fa = ft[:, :, :, None]
    fb = fs[:, :, None, :]
    prod_ab = lax.optimization_barrier(jnp.sum(fa * fb, axis=1))
    prod_ar = lax.optimization_barrier(jnp.sum(fa * sep, axis=1))
    prod_br = lax.optimization_barrier(jnp.sum(fb * sep, axis=1))
    first = (fa * prod_br[:, None] + fb * prod_ar[:, None] - prod_ab[:, None] * sep) * inv_three[:, None]
    second = 3.0 * (prod_ar * prod_br * inv_five)[:, None] * sep
    return (first - second) * KERNEL

def reference(positions, densities, near_src, near_count, far_slot, far_class, far_count, requests, up_basis, transfer_table, down_basis):
    stacked = jnp.concatenate([positions, densities], 0).reshape(6, LEAVES, P_SIZE).transpose(1, 0, 2)
    blocks = jnp.arange(N_PATCH, dtype=jnp.int32)

    def slot_body(slot, grad):
        source = near_src[:, slot]
        live = (slot < near_count).astype(jnp.float32)

        def one_block(block):
            start = (block * LEAF_DEV).astype(jnp.int32)
            target = lax.dynamic_slice_in_dim(stacked, start, LEAF_DEV, 0)
            src_ids = lax.dynamic_slice_in_dim(source, start, LEAF_DEV, 0)
            weight = lax.dynamic_slice_in_dim(live, start, LEAF_DEV, 0)
            terms = pair_terms(target, stacked[src_ids]) * weight[:, None, None, None]
            return (lax.optimization_barrier(jnp.sum(terms, axis=3)), lax.optimization_barrier(jnp.sum(terms, axis=2)))
        tgt_sum, src_sum = lax.map(one_block, blocks)
        grad = grad + tgt_sum.reshape(LEAVES, 3, P_SIZE)
        return grad.at[source].add(-src_sum.reshape(LEAVES, 3, P_SIZE))
    near = lax.fori_loop(0, NEAR, slot_body, jnp.zeros((LEAVES, 3, P_SIZE), jnp.float32))
    dens_leaf = stacked[:, 3:]
    dens_round = lax.optimization_barrier(dens_leaf.reshape(LEAVES, 3 * P_SIZE).astype(jnp.bfloat16))
    dens_flat = dens_round.astype(jnp.float32)

    def upward(block):
        start = (block * LEAF_DEV).astype(jnp.int32)
        basis = lax.dynamic_slice_in_dim(up_basis, start, LEAF_DEV, 0).astype(jnp.float32)
        dens_b = lax.dynamic_slice_in_dim(dens_flat, start, LEAF_DEV, 0)
        return jnp.einsum('lrq,lq->lr', basis, dens_b, precision=lax.Precision.HIGHEST).astype(jnp.bfloat16)
    moments = lax.map(upward, blocks).reshape(LEAVES, 3 * RANK)
    moments = lax.optimization_barrier(moments).astype(jnp.float32)
    dev_of = jnp.arange(LEAVES, dtype=jnp.int32) // LEAF_DEV
    peer = far_slot // CAP
    place = far_slot % CAP
    source_ids = peer * LEAF_DEV + requests[dev_of[:, None], peer, place]

    def far_block(block):
        start = (block * LEAF_DEV).astype(jnp.int32)
        ids = lax.dynamic_slice_in_dim(source_ids, start, LEAF_DEV, 0)
        classes = lax.dynamic_slice_in_dim(far_class, start, LEAF_DEV, 0)
        counts = lax.dynamic_slice_in_dim(far_count, start, LEAF_DEV, 0)

        def far_step(slot, expansion):
            src = moments[ids[:, slot]]
            oper = transfer_table[classes[:, slot]].reshape(LEAF_DEV, 3 * RANK, 3 * RANK).astype(jnp.float32)
            live = (slot < counts).astype(jnp.float32)
            return expansion + live[:, None] * jnp.einsum('lij,lj->li', oper, src, precision=lax.Precision.HIGHEST)
        expansion = lax.fori_loop(0, FAR, far_step, jnp.zeros((LEAF_DEV, 3 * RANK), jnp.float32))
        expansion = lax.optimization_barrier(expansion.astype(jnp.bfloat16)).astype(jnp.float32)
        basis = lax.dynamic_slice_in_dim(down_basis, start, LEAF_DEV, 0).astype(jnp.float32)
        field = jnp.einsum('lr,lrqp->lqp', expansion, basis, precision=lax.Precision.HIGHEST)
        dens_b = lax.dynamic_slice_in_dim(dens_leaf, start, LEAF_DEV, 0)
        return jnp.einsum('lcp,lckp->lkp', dens_b, field.reshape(LEAF_DEV, 3, 3, P_SIZE), precision=lax.Precision.HIGHEST)
    far = lax.map(far_block, blocks).reshape(LEAVES, 3, P_SIZE)
    return (near + far).transpose(1, 0, 2).reshape(3, NODES)
```

```python
import functools
import math

import jax
import jax.numpy as jnp
from jax import lax
from jax.experimental import pallas as pl
from jax.experimental.pallas import tpu as pltpu
from jax.sharding import PartitionSpec as P

KERNEL = 1.0 / (8.0 * math.pi)
BLOB = 0.25
LANES = 128
GROUP = 16
F32 = jnp.float32
BF16 = jnp.bfloat16


def iota(shape, dim):
    return lax.broadcasted_iota(jnp.int32, shape, dim)


def moments_body(dens_ref, up_ref, out_ref):
    leaf_num, width, _ = up_ref.shape
    peers = out_ref.shape[0]
    lane = iota((width, LANES), 1)
    cols = jnp.zeros((width, LANES), F32)
    for leaf in range(leaf_num):
        total = None
        for comp in range(3):
            row = dens_ref[comp : comp + 1, leaf * LANES : (leaf + 1) * LANES]
            row = row.astype(BF16).astype(F32)
            part = up_ref[leaf, :, comp * LANES : (comp + 1) * LANES].astype(F32) * row
            total = part if total is None else total + part
        cols = jnp.where(lane == leaf, jnp.sum(total, axis=1, keepdims=True), cols)
    tail = jnp.concatenate([cols[LANES:], jnp.zeros((2 * LANES - width, LANES), F32)], 0)
    rows = jnp.concatenate([cols[:LANES].T[:leaf_num], tail.T[:leaf_num]], 1).astype(BF16)
    out_ref[...] = jnp.broadcast_to(rows[None], (peers,) + rows.shape)


def near_body(src_ref, count_ref, own_ref, left_ref, right_ref, near_ref, to_left_ref, to_right_ref, win, cols, tacc, sacc):
    leaf_num = count_ref.shape[0]
    device = lax.axis_index("patch")
    offset = (device - 1) * leaf_num
    for place, ref in enumerate((left_ref, own_ref, right_ref)):
        for leaf in range(leaf_num):
            win[place * leaf_num + leaf, 0:6] = ref[:, leaf * LANES : (leaf + 1) * LANES]
    sacc[...] = jnp.zeros(sacc.shape, F32)
    lane = iota((LANES, LANES), 1)

    def one_leaf(leaf, _):
        tile = jnp.concatenate([win[leaf_num + leaf], jnp.zeros((LANES - 8, LANES), F32)], 0).T
        for comp in range(6):
            cols[comp] = jnp.broadcast_to(tile[:, comp : comp + 1], (LANES, LANES))
        tacc[...] = jnp.zeros(tacc.shape, F32)

        def one_block(slot, _):
            source = src_ref[leaf, slot] - offset
            row = [jnp.broadcast_to(win[source, comp : comp + 1], (8, LANES)) for comp in range(6)]
            bx = row[3:]
            sums = [jnp.zeros((8, LANES), F32) for _ in range(3)]
            for part in range(LANES // 8):
                at = slice(part * 8, part * 8 + 8)
                ax = [cols[3 + k, at] for k in range(3)]
                sep = [cols[k, at] - row[k] for k in range(3)]
                rho_sq = sep[0] * sep[0] + sep[1] * sep[1] + (sep[2] * sep[2] + BLOB)
                inv_one = lax.rsqrt(rho_sq)
                inv_two = inv_one * inv_one
                inv_three = inv_two * inv_one
                ab = ax[0] * bx[0] + ax[1] * bx[1] + ax[2] * bx[2]
                ar = ax[0] * sep[0] + ax[1] * sep[1] + ax[2] * sep[2]
                br = bx[0] * sep[0] + bx[1] * sep[1] + bx[2] * sep[2]
                coef = (ab + ar * br * (3.0 * inv_two)) * inv_three
                ar = ar * inv_three
                br = br * inv_three
                for k in range(3):
                    term = ax[k] * br + bx[k] * ar - coef * sep[k]
                    tacc[k, at] = tacc[k, at] + term
                    sums[k] = sums[k] + term
            for k in range(3):
                sacc[source, k] = sacc[source, k] + sums[k]
            return 0

        lax.fori_loop(0, count_ref[leaf], one_block, 0)
        flat = jnp.zeros((LANES, LANES), F32)
        for k in range(3):
            flat = jnp.where(lane == k, jnp.sum(tacc[k], axis=1, keepdims=True), flat)
        win[leaf_num + leaf, 6:7] = win[leaf_num + leaf, 6:7]
        cols[0] = flat.T
        spot = pl.ds(pl.multiple_of(leaf * LANES, LANES), LANES)
        near_ref[:, spot] = cols[0, 0:3]
        return 0

    lax.fori_loop(0, leaf_num, one_leaf, 0)
    for place, ref in enumerate((to_left_ref, near_ref, to_right_ref)):
        for leaf in range(leaf_num):
            at = slice(leaf * LANES, (leaf + 1) * LANES)
            part = jnp.sum(sacc[place * leaf_num + leaf], axis=1)
            ref[:, at] = (ref[:, at] - part) * KERNEL if place == 1 else part * -KERNEL


def columns(scratch, value):
    rows, width = value.shape
    scratch[0:rows, 0:width] = value.astype(F32)
    return scratch[...].T


def prep_body(count_ref, slot_ref, class_ref, req_ref, pick_ref, hot_ref, scratch):
    leaf_num, far_num = slot_ref.shape
    cap, peers = req_ref.shape
    scratch[...] = jnp.zeros((LANES, LANES), F32)
    asked = columns(scratch, req_ref[...])
    asked = jnp.concatenate([jnp.broadcast_to(asked[:, t : t + 1], (peers, LANES)) for t in range(cap)], 0)
    asked = asked.astype(BF16)
    slots = columns(scratch, slot_ref[...])
    lane = iota((far_num, LANES), 1)
    for leaf in range(leaf_num):
        at = slice(leaf * far_num, (leaf + 1) * far_num)
        slot = jnp.broadcast_to(slots[:far_num, leaf : leaf + 1], (far_num, LANES)).astype(jnp.int32)
        peer = slot // cap
        key = (slot - peer * cap) * peers + peer - lane
        hots = [jnp.where(key == t * peers, 1.0, 0.0).astype(BF16) for t in range(cap)]
        local = jnp.dot(jnp.concatenate(hots, 1), asked, preferred_element_type=F32)
        key = peer * leaf_num + local.astype(jnp.int32) - lane
        for t in range(pick_ref.shape[1] // LANES):
            pick_ref[at, t * LANES : (t + 1) * LANES] = jnp.where(key == t * LANES, 1.0, 0.0).astype(BF16)
    classes = columns(scratch, class_ref[...])
    row = iota((far_num, LANES), 0)
    for leaf in range(leaf_num):
        at = slice(leaf * far_num, (leaf + 1) * far_num)
        kind = jnp.broadcast_to(classes[:far_num, leaf : leaf + 1], (far_num, LANES)).astype(jnp.int32)
        keep = (lane % leaf_num == leaf) & (row < count_ref[leaf])
        key = jnp.where(keep, kind - lane // leaf_num, -LANES)
        per = LANES // leaf_num
        for t in range(hot_ref.shape[1] // LANES):
            hot_ref[at, t * LANES : (t + 1) * LANES] = jnp.where(key == t * per, 1.0, 0.0).astype(BF16)


def far_body(mom_ref, pick_ref, hot_ref, table, down, dens_ref, near_ref, from_left_ref, from_right_ref, out_ref, pad, sums, tail, last):
    leaf_num, quads, width, _ = down.shape
    classes = table.shape[0]
    groups = pad.shape[0]
    src = jnp.dot(pick_ref[...], mom_ref[...], preferred_element_type=F32)
    src_t = jnp.concatenate([src[:, :LANES].T, src[:, LANES:].T[: width - LANES]], 0).astype(BF16)
    lead = 2 * LANES - width
    cols = GROUP * leaf_num
    for g in range(groups):
        pad[g, 0:lead] = jnp.zeros((lead, cols), BF16)
        pad[g, lead + width :] = jnp.zeros((pad.shape[1] - lead - width, cols), BF16)
        part = jnp.dot(src_t, hot_ref[:, g * cols : (g + 1) * cols], preferred_element_type=F32)
        pad[g, lead : lead + width] = part.astype(BF16)
    keep = classes - classes % 8
    tail[...] = jnp.zeros(tail.shape, F32)
    tail[0 : classes - keep] = table[keep:classes].astype(F32)
    last[0:8] = table[keep - 8 : keep]
    last[8:16] = tail[...].astype(BF16)
    step = width - LANES
    period = LANES // step
    tiles = period + 1
    blocks = width // period
    same = iota((blocks, GROUP, cols), 2) // leaf_num == iota((blocks, GROUP, cols), 1)
    for r in range(period):
        acc = None
        for g in range(groups):
            ref, first = (last, 0) if g == groups - 1 else (table, g * GROUP)
            rows = [ref[first : first + GROUP, (tiles * b + r) * LANES : (tiles * b + r + 2) * LANES] for b in range(blocks)]
            part = jnp.dot(jnp.concatenate(rows, 0), pad[g, lead - step * r : lead - step * r + 2 * LANES], preferred_element_type=F32)
            acc = part if acc is None else acc + part
        acc = jnp.where(same, acc.reshape(blocks, GROUP, cols), 0.0)
        acc = jnp.sum(acc, axis=1)
        for h in range(cols // LANES):
            sums[h, pl.ds(r, blocks, stride=period), :] = acc[:, h * LANES : (h + 1) * LANES]
    fold = jnp.where(iota((leaf_num, cols), 1) % leaf_num == iota((leaf_num, cols), 0), 1.0, 0.0)
    whole = jnp.concatenate([sums[h] for h in range(cols // LANES)], 1)
    expansion = lax.dot_general(fold, whole, (((1,), (1,)), ((), ())), precision=lax.Precision.HIGHEST, preferred_element_type=F32)
    which = iota((leaf_num, width), 0)
    field = [None] * quads
    for leaf in range(leaf_num):
        lhs = jnp.where(which == leaf, expansion, 0.0).astype(BF16)
        for q in range(0, quads, 2):
            both = [down[leaf, i] for i in range(q, min(q + 2, quads))]
            part = jnp.dot(lhs, jnp.concatenate(both, 1), preferred_element_type=F32)
            field[q] = part if field[q] is None else field[q] + part
    quad = [field[q - q % 2][:, (q % 2) * LANES : (q % 2 + 1) * LANES] for q in range(quads)]
    for leaf in range(leaf_num):
        at = slice(leaf * LANES, (leaf + 1) * LANES)
        base = near_ref[:, at] + from_left_ref[:, at] + from_right_ref[:, at]
        far = []
        for k in range(3):
            far.append(sum(dens_ref[c : c + 1, at] * quad[3 * c + k][leaf : leaf + 1] for c in range(3)))
        out_ref[:, at] = base + jnp.concatenate(far, 0)


SMEM = pl.BlockSpec(memory_space=pltpu.SMEM)
VMEM = pl.BlockSpec(memory_space=pltpu.VMEM)


def per_device(positions, densities, near_src, near_count, far_slot, far_class, far_count, requests, up_basis, transfer_table, down_basis):
    leaf_num, slot_num = near_src.shape
    nodes = positions.shape[1]
    width = up_basis.shape[1]
    far_num = far_slot.shape[1]
    peers = requests.shape[1]
    quads = down_basis.shape[2]
    classes = transfer_table.shape[0]
    groups = -(-classes // GROUP)
    own = jnp.concatenate([positions, densities], 0)
    up = [(i, i + 1) for i in range(peers - 1)]
    down = [(j, i) for i, j in up]
    left = lax.ppermute(own, "patch", up)
    right = lax.ppermute(own, "patch", down)
    message = pl.pallas_call(
        moments_body,
        out_shape=jax.ShapeDtypeStruct((peers, leaf_num, 2 * LANES), BF16),
        in_specs=[VMEM, VMEM],
        out_specs=VMEM,
        name="moments",
    )(densities, up_basis)
    table = lax.all_to_all(message, "patch", split_axis=0, concat_axis=0, tiled=True)
    table = table.reshape(peers * leaf_num, 2 * LANES)
    side = jax.ShapeDtypeStruct((3, nodes), F32)
    near, to_left, to_right = pl.pallas_call(
        near_body,
        out_shape=(side, side, side),
        in_specs=[SMEM, SMEM, VMEM, VMEM, VMEM],
        out_specs=(VMEM, VMEM, VMEM),
        scratch_shapes=[
            pltpu.VMEM((3 * leaf_num, 8, LANES), F32),
            pltpu.VMEM((6, LANES, LANES), F32),
            pltpu.VMEM((3, LANES, LANES), F32),
            pltpu.VMEM((3 * leaf_num, 3, 8, LANES), F32),
        ],
        name="near",
    )(near_src, near_count, own, left, right)
    from_right = lax.ppermute(to_left, "patch", down)
    from_left = lax.ppermute(to_right, "patch", up)
    pick, hot = pl.pallas_call(
        prep_body,
        out_shape=(
            jax.ShapeDtypeStruct((leaf_num * far_num, peers * leaf_num), BF16),
            jax.ShapeDtypeStruct((leaf_num * far_num, groups * GROUP * leaf_num), BF16),
        ),
        in_specs=[SMEM, VMEM, VMEM, VMEM],
        out_specs=(VMEM, VMEM),
        scratch_shapes=[pltpu.VMEM((LANES, LANES), F32)],
        name="prep",
    )(far_count, far_slot, far_class, requests[0].T)
    return pl.pallas_call(
        far_body,
        out_shape=side,
        in_specs=[VMEM] * 9,
        out_specs=VMEM,
        scratch_shapes=[
            pltpu.VMEM((groups, 2 * LANES + 2 * LANES - width, GROUP * leaf_num), BF16),
            pltpu.VMEM((GROUP * leaf_num // LANES, width, LANES), F32),
            pltpu.VMEM((8, width * width), F32),
            pltpu.VMEM((GROUP, width * width), BF16),
        ],
        name="far",
    )(table, pick, hot, transfer_table, down_basis.transpose(0, 2, 1, 3), densities, near, from_left, from_right)


def solution(mesh):
    placed = (
        P(None, "patch"),
        P(None, "patch"),
        P("patch", None),
        P("patch"),
        P("patch", None),
        P("patch", None),
        P("patch"),
        P("patch", None, None),
        P("patch", None, None),
        P(),
        P("patch", None, None, None),
    )
    return jax.shard_map(per_device, mesh=mesh, in_specs=placed, out_specs=P(None, "patch"), check_vma=False)
```

```python
import math

import jax
import jax.numpy as jnp
from jax import lax
from jax.experimental import pallas as pl
from jax.experimental.pallas import tpu as pltpu
from jax.sharding import PartitionSpec as P


KERNEL = 1.0 / (8.0 * math.pi)
BLOB = 0.25
LANES = 128
GROUP = 16
F32 = jnp.float32
BF16 = jnp.bfloat16


def iota(shape, dim):
    return lax.broadcasted_iota(jnp.int32, shape, dim)


def front_body(pos_hbm, dens_hbm, src_hbm, count_hbm, up_hbm, own_ref, out_ref, pos_ref, dens_ref, src_ref, count_ref, up_ref, sem):
    refs = ((pos_hbm, pos_ref), (dens_hbm, dens_ref), (src_hbm, src_ref), (count_hbm, count_ref), (up_hbm, up_ref))
    copies = [pltpu.make_async_copy(a, b, sem.at[i]) for i, (a, b) in enumerate(refs)]
    for copy in copies:
        copy.start()
    leaf_num, width, _ = up_ref.shape
    nodes = pos_ref.shape[1]
    slots = src_ref.shape[0]
    own_ref[6:, :nodes] = jnp.zeros((2, nodes), F32)
    own_ref[:, nodes:] = jnp.zeros((slots, LANES), F32)
    for copy in copies[:4]:
        copy.wait()
    own_ref[0:3, :nodes] = pos_ref[...]
    own_ref[3:6, :nodes] = dens_ref[...]
    live = iota((slots, leaf_num), 0) < count_ref[...]
    own_ref[:, nodes : nodes + leaf_num] = jnp.where(live, src_ref[...] + 1, 0).astype(F32)
    copies[4].wait()
    lane = iota((width, LANES), 1)
    cols = jnp.zeros((width, LANES), F32)
    for leaf in range(leaf_num):
        total = None
        for comp in range(3):
            row = dens_ref[comp : comp + 1, leaf * LANES : (leaf + 1) * LANES]
            row = row.astype(BF16).astype(F32)
            part = up_ref[leaf, :, comp * LANES : (comp + 1) * LANES].astype(F32) * row
            total = part if total is None else total + part
        cols = jnp.where(lane == leaf, jnp.sum(total, axis=1, keepdims=True), cols)
    step = width - LANES
    reps = LANES // step
    tails = jnp.concatenate([cols[LANES:]] * reps, 0).T[:leaf_num]
    tails = jnp.where(iota(tails.shape, 1) // step == iota(tails.shape, 0) % reps, tails, 0.0)
    tails = [jnp.sum(tails[i : i + reps], axis=0, keepdims=True) for i in range(0, leaf_num, reps)]
    rows = jnp.concatenate([cols[:LANES].T[:leaf_num]] + tails, 0)
    rows = jnp.concatenate([rows] * 8, 0).astype(BF16)
    for i in range(out_ref.shape[0] // rows.shape[0]):
        out_ref[i * rows.shape[0] : (i + 1) * rows.shape[0]] = rows


def split(x):
    high = x.astype(BF16).astype(F32)
    mid = (x - high).astype(BF16).astype(F32)
    low = (x - high - mid).astype(BF16).astype(F32)
    return high, mid, low


TARGET_PARTS = (0, 0, 1, 0, 2, 1)
SOURCE_PARTS = (0, 1, 0, 2, 0, 1)


def target_rows(tile):
    row = iota(tile.shape, 0)
    x = jnp.where(row < 3, tile, 0.0)
    f = jnp.where(row < 3, pltpu.roll(tile, 5, 0), 0.0)
    norm = jnp.sum(x * x, axis=0, keepdims=True) + BLOB
    cross = jnp.sum(x * f, axis=0, keepdims=True)
    parts, norms, crosses = split(tile), split(norm), split(cross)
    out = []
    for q in range(6):
        extra = norms[q] if q < 3 else crosses[q - 3]
        out.append(jnp.where(row < 6, parts[TARGET_PARTS[q]], jnp.where(row == 6, extra, 1.0 if q < 3 else 0.0)))
    return jnp.concatenate(out, 0)


def source_rows(tile):
    row = iota(tile.shape, 0)
    first, second = row < 3, (row >= 3) & (row < 6)
    x = jnp.where(first, tile, 0.0)
    f = jnp.where(first, pltpu.roll(tile, 5, 0), 0.0)
    norms = split(jnp.sum(x * x, axis=0, keepdims=True))
    crosses = split(-3.0 * jnp.sum(x * f, axis=0, keepdims=True))
    parts = split(tile)
    low = split(pltpu.roll(tile, 3, 0))
    triple = split(3.0 * f)
    rho, ab, ar, br = [], [], [], []
    for q in range(6):
        k = SOURCE_PARTS[q]
        main = jnp.where(first, -2.0 * parts[k], 0.0)
        if q < 3:
            main = jnp.where(row == 6, 1.0, jnp.where(row == 7, norms[q], main))
        rho.append(main)
        ab.append(jnp.where(second, parts[k], 0.0))
        ar.append(jnp.where(second, -low[k], jnp.where(row == 6, 0.0 if q < 3 else 1.0, 0.0)))
        br.append(jnp.where(first, triple[k], jnp.where(row == 7, crosses[q], 0.0) if q < 3 else 0.0))
    return [jnp.concatenate(rows, 0).astype(BF16) for rows in (rho, ab, ar, br)]


def middle_body(own_ref, left_ref, right_ref, count_ref, slot_ref, class_ref, req_ref, near_ref, main_ref, tail_ref, code_ref, kind_ref, win, lhs, rhs, acc, one, two, list_v, list_s, pairs, sem, flip):
    near_terms(own_ref, left_ref, right_ref, near_ref, win, lhs, rhs, acc, one, two, list_v, list_s, pairs, sem)
    select_terms(count_ref, slot_ref, class_ref, req_ref, main_ref, tail_ref, code_ref, kind_ref, flip)


def near_terms(own_ref, left_ref, right_ref, near_ref, win, lhs, rhs, acc, one, two, list_v, list_s, pairs, sem):
    leaf_num = acc.shape[0] - 1
    nodes = leaf_num * LANES
    slots = list_v.shape[1]
    device = lax.axis_index("patch")
    offset = (device - 1) * leaf_num + 1
    halo = (left_ref, own_ref, right_ref)
    for place, ref in enumerate(halo):
        list_v[place] = ref[:, nodes:].astype(jnp.int32)
    copy = pltpu.make_async_copy(list_v, list_s, sem)
    copy.start()
    acc[...] = jnp.zeros(acc.shape, F32)
    for place, ref in enumerate(halo):
        for leaf in range(leaf_num):
            tile = ref[:, leaf * LANES : (leaf + 1) * LANES]
            win[place * leaf_num + leaf] = tile
            for k, rows in enumerate(source_rows(tile)):
                rhs[place * leaf_num + leaf, :, k * LANES : (k + 1) * LANES] = rows
            if place == 1:
                lhs[leaf] = target_rows(tile).T.astype(BF16)
    lhs[leaf_num] = jnp.zeros(lhs.shape[1:], BF16)
    copy.wait()
    count = 0
    for place in range(3):
        def scan(leaf, count):
            for slot in range(slots):
                listed = list_s[place, slot, leaf]
                source = listed - offset
                mine = (listed > 0) & (source >= leaf_num) & (source < 2 * leaf_num)
                pairs[count] = (source - leaf_num) * 64 + (place * leaf_num + leaf)
                count = count + mine.astype(jnp.int32)
                if place == 1:
                    pairs[count] = leaf * 64 + source
                    count = count + (listed > 0).astype(jnp.int32)
            return count

        count = lax.fori_loop(0, leaf_num, scan, count)
    for i in range(3):
        pairs[count + i] = leaf_num * 64

    def products(at, buf):
        pair = pairs[at]
        buf[...] = jnp.dot(lhs[pair // 64], rhs[pair % 64], preferred_element_type=F32)

    def add_terms(at, buf):
        pair = pairs[at]
        target, source = pair // 64, pair % 64
        row = [jnp.broadcast_to(win[source, k : k + 1], (8, LANES)) for k in range(6)]
        for part in range(LANES // 8):
            i = slice(part * 8, part * 8 + 8)
            rho_sq, ab, ar, br = [buf[i, k * LANES : (k + 1) * LANES] for k in range(4)]
            inv_one = lax.rsqrt(rho_sq)
            inv_two = inv_one * inv_one
            inv_three = inv_two * inv_one
            coef = (ab + ar * br * inv_two) * inv_three
            ar = ar * inv_three
            acc[target, 0, i] += br * inv_three
            acc[target, 1, i] += coef
            for k in range(3):
                acc[target, 2 + k, i] += row[3 + k] * ar + row[k] * coef

    products(0, one)

    def two_blocks(step, _):
        products(2 * step + 1, two)
        add_terms(2 * step, one)
        products(2 * step + 2, one)
        add_terms(2 * step + 1, two)
        return 0

    lax.fori_loop(0, (count + 1) // 2, two_blocks, 0)
    lane = iota((LANES, LANES), 1)
    for leaf in range(leaf_num):
        flat = jnp.zeros((LANES, LANES), F32)
        for k in range(5):
            flat = jnp.where(lane == k, jnp.sum(acc[leaf, k], axis=1, keepdims=True), flat)
        flat = flat.T
        tile = win[leaf_num + leaf]
        total = flat[0:1] * tile[3:6] * (1.0 / 3.0) + flat[2:5] - flat[1:2] * tile[0:3]
        near_ref[:, leaf * LANES : (leaf + 1) * LANES] = total * KERNEL


def columns(scratch, value):
    rows, width = value.shape
    scratch[0:rows, 0:width] = value.astype(F32)
    return scratch[...].T


def select_terms(count_ref, slot_ref, class_ref, req_ref, main_ref, tail_ref, code_ref, kind_ref, scratch):
    leaf_num, far_num = slot_ref.shape
    cap, peers = req_ref.shape
    reps = LANES // leaf_num
    half = peers // 2
    rows = main_ref.shape[1] // half
    scratch[...] = jnp.zeros((LANES, LANES), F32)
    asked = columns(scratch, req_ref[...])
    asked = jnp.concatenate([jnp.broadcast_to(asked[:, t : t + 1], (peers, LANES)) for t in range(cap)], 0)
    asked = asked.astype(BF16)
    slots = columns(scratch, slot_ref[...])
    classes = columns(scratch, class_ref[...])
    lane = iota((far_num, LANES), 1)
    row = iota((far_num, LANES), 0)

    def hots(ref, at, key, stride):
        for t in range(ref.shape[1] // LANES):
            ref[at, t * LANES : (t + 1) * LANES] = jnp.where(key == t * stride, 1.0, 0.0).astype(BF16)

    for leaf in range(leaf_num):
        at = slice(leaf * far_num, (leaf + 1) * far_num)
        slot = jnp.broadcast_to(slots[:far_num, leaf : leaf + 1], (far_num, LANES)).astype(jnp.int32)
        peer = slot // cap
        key = (slot - peer * cap) * peers + peer - lane
        picks = [jnp.where(key == t * peers, 1.0, 0.0).astype(BF16) for t in range(cap)]
        local = jnp.dot(jnp.concatenate(picks, 1), asked, preferred_element_type=F32).astype(jnp.int32)
        upper = (peer >= half).astype(jnp.int32)
        base = (peer - upper * half) * rows - lane
        hots(main_ref, at, base + local, LANES)
        hots(tail_ref, at, base + leaf_num + local // reps, LANES)
        code_ref[at] = (upper + 2 * (lane // leaf_num == local % reps).astype(jnp.int32)).astype(BF16)
        kind = jnp.broadcast_to(classes[:far_num, leaf : leaf + 1], (far_num, LANES)).astype(jnp.int32)
        keep = (lane % leaf_num == leaf) & (row < count_ref[leaf])
        kind_ref[at] = jnp.where(keep, kind - lane // leaf_num, -LANES).astype(BF16)


def far_body(mom_ref, main_ref, tail_ref, code_ref, kind_ref, own_ref, near_ref, table_hbm, down_hbm, out_ref, table, down, pad, sums, tail, last, sem):
    fetch = pltpu.make_async_copy(table_hbm, table, sem.at[0])
    fetch_down = pltpu.make_async_copy(down_hbm, down, sem.at[1])
    fetch.start()
    fetch_down.start()
    leaf_num, quads, width, _ = down.shape
    classes = table.shape[0]
    groups = pad.shape[0]
    half = mom_ref.shape[0] // 2
    both = jnp.concatenate([mom_ref[:half], mom_ref[half:]], 1)
    main = jnp.dot(main_ref[...], both, preferred_element_type=F32)
    tails = jnp.dot(tail_ref[...], both, preferred_element_type=F32)
    code = code_ref[...].astype(F32)
    upper = (code == 1.0) | (code == 3.0)
    main = jnp.where(upper, main[:, LANES:], main[:, :LANES]).T
    tails = jnp.where(upper, tails[:, LANES:], tails[:, :LANES])
    tails = jnp.where(code >= 2, tails, 0.0).T
    extra = width - LANES
    tails = sum(tails[i * extra : (i + 1) * extra] for i in range(LANES // extra))
    src_t = jnp.concatenate([main, tails], 0).astype(BF16)
    kind = kind_ref[...]
    one, zero = jnp.ones((), BF16), jnp.zeros((), BF16)
    lead = 2 * LANES - width
    cols = GROUP * leaf_num
    for g in range(groups):
        pad[g, 0:lead] = jnp.zeros((lead, cols), BF16)
        pad[g, lead + width :] = jnp.zeros((pad.shape[1] - lead - width, cols), BF16)
        hot = [jnp.where(kind == (g * (cols // LANES) + h) * (LANES // leaf_num), one, zero) for h in range(cols // LANES)]
        part = jnp.dot(src_t, jnp.concatenate(hot, 1), preferred_element_type=F32)
        pad[g, lead : lead + width] = part.astype(BF16)
    fetch.wait()
    keep = classes - classes % 8
    tail[...] = jnp.zeros(tail.shape, F32)
    tail[0 : classes - keep] = table[keep:classes].astype(F32)
    last[0:8] = table[keep - 8 : keep]
    last[8:16] = tail[...].astype(BF16)
    step = width - LANES
    period = LANES // step
    tiles = period + 1
    blocks = width // period
    same = iota((blocks, GROUP, cols), 2) // leaf_num == iota((blocks, GROUP, cols), 1)
    for r in range(period):
        acc = None
        for g in range(groups):
            ref, first = (last, 0) if g == groups - 1 else (table, g * GROUP)
            rows = [ref[first : first + GROUP, (tiles * b + r) * LANES : (tiles * b + r + 2) * LANES] for b in range(blocks)]
            part = jnp.dot(jnp.concatenate(rows, 0), pad[g, lead - step * r : lead - step * r + 2 * LANES], preferred_element_type=F32)
            acc = part if acc is None else acc + part
        acc = jnp.where(same, acc.reshape(blocks, GROUP, cols), 0.0)
        acc = jnp.sum(acc, axis=1)
        for h in range(cols // LANES):
            sums[h, pl.ds(r, blocks, stride=period), :] = acc[:, h * LANES : (h + 1) * LANES]
    fold = jnp.where(iota((leaf_num, cols), 1) % leaf_num == iota((leaf_num, cols), 0), 1.0, 0.0)
    whole = jnp.concatenate([sums[h] for h in range(cols // LANES)], 1)
    expansion = lax.dot_general(fold, whole, (((1,), (1,)), ((), ())), precision=lax.Precision.HIGHEST, preferred_element_type=F32)
    fetch_down.wait()
    which = iota((leaf_num, width), 0)
    field = [None] * quads
    for leaf in range(leaf_num):
        lhs = jnp.where(which == leaf, expansion, 0.0).astype(BF16)
        for q in range(0, quads, 2):
            both = [down[leaf, i] for i in range(q, min(q + 2, quads))]
            part = jnp.dot(lhs, jnp.concatenate(both, 1), preferred_element_type=F32)
            field[q] = part if field[q] is None else field[q] + part
    quad = [field[q - q % 2][:, (q % 2) * LANES : (q % 2 + 1) * LANES] for q in range(quads)]
    for leaf in range(leaf_num):
        at = slice(leaf * LANES, (leaf + 1) * LANES)
        far = []
        for k in range(3):
            far.append(sum(own_ref[3 + c : 4 + c, at] * quad[3 * c + k][leaf : leaf + 1] for c in range(3)))
        out_ref[:, at] = near_ref[:, at] + jnp.concatenate(far, 0)


SMEM = pl.BlockSpec(memory_space=pltpu.SMEM)
VMEM = pl.BlockSpec(memory_space=pltpu.VMEM)
HBM = pl.BlockSpec(memory_space=pltpu.HBM)


def held(x, space=pltpu.VMEM):
    return pltpu.with_memory_space_constraint(x, space)


def call(body, outs, limit, **options):
    if outs is not None:
        shapes = tuple(pltpu.VMEM(o[:-1], o[-1]) for o in outs)
        options["out_shape"] = shapes if len(shapes) > 1 else shapes[0]
    params = pltpu.CompilerParams(vmem_limit_bytes=limit * 2**20)
    return pl.pallas_call(body, compiler_params=params, **options)


def per_device(positions, densities, near_src, near_count, far_slot, far_class, far_count, requests, up_basis, transfer_table, down_basis):
    leaf_num, slot_num = near_src.shape
    nodes = positions.shape[1]
    width = up_basis.shape[1]
    far_num = far_slot.shape[1]
    peers = requests.shape[1]
    classes = transfer_table.shape[0]
    groups = -(-classes // GROUP)
    rows = leaf_num * width // LANES
    up = [(i, i + 1) for i in range(peers - 1)]
    down = [(j, i) for i, j in up]
    slots = leaf_num * far_num
    own, message = call(
        front_body,
        [(8, nodes + LANES, F32), (peers * rows, LANES, BF16)],
        8,
        in_specs=[HBM] * 5,
        scratch_shapes=[
            pltpu.VMEM((3, nodes), F32),
            pltpu.VMEM((3, nodes), F32),
            pltpu.VMEM((slot_num, leaf_num), jnp.int32),
            pltpu.VMEM((1, leaf_num), jnp.int32),
            pltpu.VMEM(up_basis.shape, BF16),
            pltpu.SemaphoreType.DMA((5,)),
        ],
    )(*[held(x, pltpu.HBM) for x in (positions, densities, near_src.T, near_count[None], up_basis)])
    left = lax.ppermute(own, "patch", up)
    right = lax.ppermute(own, "patch", down)
    message = message.reshape(peers, rows // 2, 2, LANES)
    table = lax.all_to_all(message, "patch", split_axis=0, concat_axis=0, tiled=True)
    table = table.reshape(peers * rows, LANES)
    down_flat = down_basis.transpose(0, 2, 1, 3)
    near, *kept = call(
        middle_body,
        [
            (3, nodes, F32),
            (slots, peers * rows // 2, BF16),
            (slots, peers * rows // 2, BF16),
            (slots, LANES, BF16),
            (slots, LANES, BF16),
        ],
        14,
        in_specs=[VMEM] * 3 + [SMEM] + [VMEM] * 3,
        scratch_shapes=[
            pltpu.VMEM((3 * leaf_num, 8, LANES), F32),
            pltpu.VMEM((leaf_num + 1, LANES, 48), BF16),
            pltpu.VMEM((3 * leaf_num, 48, 4 * LANES), BF16),
            pltpu.VMEM((leaf_num + 1, 5, LANES, LANES), F32),
            pltpu.VMEM((LANES, 4 * LANES), F32),
            pltpu.VMEM((LANES, 4 * LANES), F32),
            pltpu.VMEM((3, slot_num, LANES), jnp.int32),
            pltpu.SMEM((3, slot_num, LANES), jnp.int32),
            pltpu.SMEM((4 * leaf_num * slot_num + 8,), jnp.int32),
            pltpu.SemaphoreType.DMA,
            pltpu.VMEM((LANES, LANES), F32),
        ],
    )(held(own), held(left), held(right), far_count, far_slot, far_class, requests[0].T)
    return call(
        far_body,
        None,
        30,
        in_specs=[VMEM] * 7 + [HBM] * 2,
        out_shape=jax.ShapeDtypeStruct((3, nodes), F32),
        scratch_shapes=[
            pltpu.VMEM(transfer_table.shape, BF16),
            pltpu.VMEM(down_flat.shape, BF16),
            pltpu.VMEM((groups, 4 * LANES - width, GROUP * leaf_num), BF16),
            pltpu.VMEM((GROUP * leaf_num // LANES, width, LANES), F32),
            pltpu.VMEM((8, width * width), F32),
            pltpu.VMEM((GROUP, width * width), BF16),
            pltpu.SemaphoreType.DMA((2,)),
        ],
    )(*[held(x) for x in (table, *kept, own, near)], held(transfer_table, pltpu.HBM), held(down_flat, pltpu.HBM))


def solution(mesh):
    placed = (
        P(None, "patch"),
        P(None, "patch"),
        P("patch", None),
        P("patch"),
        P("patch", None),
        P("patch", None),
        P("patch"),
        P("patch", None, None),
        P("patch", None, None),
        P(),
        P("patch", None, None, None),
    )
    return jax.shard_map(per_device, mesh=mesh, in_specs=placed, out_specs=P(None, "patch"), check_vma=False)
```

```python
import functools
import math

import jax
import jax.numpy as jnp
from jax import lax
from jax.experimental import pallas as pl
from jax.experimental.pallas import tpu as pltpu
from jax.sharding import PartitionSpec as P


KERNEL = 1.0 / (8.0 * math.pi)
BLOB = 0.25
LANES = 128
DEPTH = 2
EARLY = 2
GROUP = 16
F32 = jnp.float32
BF16 = jnp.bfloat16


def iota(shape, dim):
    return lax.broadcasted_iota(jnp.int32, shape, dim)


def front_body(pos_hbm, dens_hbm, src_hbm, count_hbm, up_hbm, own_ref, out_ref, pos_ref, dens_ref, src_ref, count_ref, up_ref, sem):
    refs = ((pos_hbm, pos_ref), (dens_hbm, dens_ref), (src_hbm, src_ref), (count_hbm, count_ref), (up_hbm, up_ref))
    copies = [pltpu.make_async_copy(a, b, sem.at[i]) for i, (a, b) in enumerate(refs)]
    for copy in copies:
        copy.start()
    leaf_num, width, _ = up_ref.shape
    nodes = pos_ref.shape[1]
    slots = src_ref.shape[0]
    own_ref[6:, :nodes] = jnp.zeros((2, nodes), F32)
    own_ref[:, nodes:] = jnp.zeros((slots, LANES), F32)
    for copy in copies[:4]:
        copy.wait()
    own_ref[0:3, :nodes] = pos_ref[...]
    own_ref[3:6, :nodes] = dens_ref[...]
    live = iota((slots, leaf_num), 0) < count_ref[...]
    own_ref[:, nodes : nodes + leaf_num] = jnp.where(live, src_ref[...] + 1, 0).astype(F32)
    copies[4].wait()
    lane = iota((width, LANES), 1)
    cols = jnp.zeros((width, LANES), F32)
    for leaf in range(leaf_num):
        total = None
        for comp in range(3):
            row = dens_ref[comp : comp + 1, leaf * LANES : (leaf + 1) * LANES]
            row = row.astype(BF16).astype(F32)
            part = up_ref[leaf, :, comp * LANES : (comp + 1) * LANES].astype(F32) * row
            total = part if total is None else total + part
        cols = jnp.where(lane == leaf, jnp.sum(total, axis=1, keepdims=True), cols)
    step = width - LANES
    reps = LANES // step
    tails = jnp.concatenate([cols[LANES:]] * reps, 0).T[:leaf_num]
    tails = jnp.where(iota(tails.shape, 1) // step == iota(tails.shape, 0) % reps, tails, 0.0)
    tails = [jnp.sum(tails[i : i + reps], axis=0, keepdims=True) for i in range(0, leaf_num, reps)]
    rows = jnp.concatenate([cols[:LANES].T[:leaf_num]] + tails, 0)
    rows = jnp.concatenate([rows] * 8, 0).astype(BF16)
    for i in range(out_ref.shape[0] // rows.shape[0]):
        out_ref[i * rows.shape[0] : (i + 1) * rows.shape[0]] = rows


def split(x):
    high = x.astype(BF16).astype(F32)
    mid = (x - high).astype(BF16).astype(F32)
    low = (x - high - mid).astype(BF16).astype(F32)
    return high, mid, low


TARGET_PARTS = (0, 0, 1, 0, 2, 1)
SOURCE_PARTS = (0, 1, 0, 2, 0, 1)


def target_rows(tile):
    row = iota(tile.shape, 0)
    x = jnp.where(row < 3, tile, 0.0)
    f = jnp.where(row < 3, pltpu.roll(tile, 5, 0), 0.0)
    norm = jnp.sum(x * x, axis=0, keepdims=True) + BLOB
    cross = jnp.sum(x * f, axis=0, keepdims=True)
    parts, norms, crosses = split(tile), split(norm), split(cross)
    out = []
    for q in range(6):
        extra = norms[q] if q < 3 else crosses[q - 3]
        out.append(jnp.where(row < 6, parts[TARGET_PARTS[q]], jnp.where(row == 6, extra, 1.0 if q < 3 else 0.0)))
    return jnp.concatenate(out, 0)


def source_rows(tile):
    row = iota(tile.shape, 0)
    first, second = row < 3, (row >= 3) & (row < 6)
    x = jnp.where(first, tile, 0.0)
    f = jnp.where(first, pltpu.roll(tile, 5, 0), 0.0)
    norms = split(jnp.sum(x * x, axis=0, keepdims=True))
    crosses = split(-3.0 * jnp.sum(x * f, axis=0, keepdims=True))
    parts = split(tile)
    low = split(pltpu.roll(tile, 3, 0))
    triple = split(3.0 * f)
    rho, ab, ar, br = [], [], [], []
    for q in range(6):
        k = SOURCE_PARTS[q]
        main = jnp.where(first, -2.0 * parts[k], 0.0)
        if q < 3:
            main = jnp.where(row == 6, 1.0, jnp.where(row == 7, norms[q], main))
        rho.append(main)
        ab.append(jnp.where(second, parts[k], 0.0))
        ar.append(jnp.where(second, -low[k], jnp.where(row == 6, 0.0 if q < 3 else 1.0, 0.0)))
        br.append(jnp.where(first, triple[k], jnp.where(row == 7, crosses[q], 0.0) if q < 3 else 0.0))
    return [jnp.concatenate(rows, 0).astype(BF16) for rows in (rho, ab, ar, br)]


def middle_body(rows, own_ref, left_ref, right_ref, count_ref, slot_ref, class_ref, req_ref, table_hbm, near_ref, main_ref, tail_ref, code_ref, kind_ref, kept_ref, table, sem_table, win, lhs, rhs, acc, one, two, list_v, list_s, pairs, sem, flip):
    fetch = pltpu.make_async_copy(table_hbm, table, sem_table)
    fetch.start()
    near_terms(own_ref, left_ref, right_ref, near_ref, win, lhs, rhs, acc, one, two, list_v, list_s, pairs, sem)
    fetch.wait()
    keep_rows(table, kept_ref)
    select_terms(rows, count_ref, slot_ref, class_ref, req_ref, main_ref, tail_ref, code_ref, kind_ref, flip)


def keep_rows(table, kept_ref):
    first = kept_ref.shape[0] - GROUP
    classes = table.shape[0]
    kept_ref[:first] = table[:first]
    whole = classes - classes % 8
    start = (classes - 1) // GROUP * GROUP
    width = 9 * LANES
    for at in range(0, table.shape[1], width):
        cols = slice(at, at + width)
        tail = table[whole:classes, cols].astype(F32)
        tail = jnp.concatenate([tail, jnp.zeros((start + GROUP - classes, width), F32)], 0)
        both = jnp.concatenate([table[start:whole, cols].astype(F32), tail], 0)
        kept_ref[first:, cols] = both.astype(BF16)


def near_terms(own_ref, left_ref, right_ref, near_ref, win, lhs, rhs, acc, one, two, list_v, list_s, pairs, sem):
    leaf_num = acc.shape[0] - 1
    nodes = leaf_num * LANES
    slots = list_v.shape[1]
    device = lax.axis_index("patch")
    halo = (left_ref, own_ref, right_ref)
    leaf_of = iota((slots, LANES), 1)
    for place, ref in enumerate(halo):
        listed = ref[:, nodes:].astype(jnp.int32)
        source = listed - (device * leaf_num + 1)
        mine = (listed > 0) & (source >= 0) & (source < leaf_num)
        list_v[place] = jnp.where(mine, (source << 6) + (leaf_of + place * leaf_num), -1)
        if place == 1:
            list_v[3] = jnp.where(listed > 0, (leaf_of << 6) + (source + leaf_num), -1)
    copy = pltpu.make_async_copy(list_v, list_s, sem)
    copy.start()
    acc[...] = jnp.zeros(acc.shape, F32)
    for place, ref in enumerate(halo):
        for leaf in range(leaf_num):
            tile = ref[:, leaf * LANES : (leaf + 1) * LANES]
            win[place * leaf_num + leaf] = tile
            for k, rows in enumerate(source_rows(tile)):
                rhs[place * leaf_num + leaf, :, k * LANES : (k + 1) * LANES] = rows
            if place == 1:
                lhs[leaf] = target_rows(tile).T.astype(BF16)
    lhs[leaf_num] = jnp.zeros(lhs.shape[1:], BF16)
    copy.wait()

    def scan(leaf, count):
        for place in range(list_s.shape[0]):
            for slot in range(slots):
                code = list_s[place, slot, leaf]
                pairs[count] = code
                count = count + (code >= 0).astype(jnp.int32)
        return count

    count = lax.fori_loop(0, leaf_num, scan, 0)
    for i in range(3 * DEPTH):
        pairs[count + i] = leaf_num * 64

    def products(at, buf):
        pair = pairs[at]
        buf[...] = jnp.dot(lhs[pair >> 6], rhs[pair & 63], preferred_element_type=F32)

    def add_terms(at, buf):
        pair = pairs[at]
        target, source = pair >> 6, pair & 63
        row = [jnp.broadcast_to(win[source, k : k + 1], (8, LANES)) for k in range(6)]
        for part in range(LANES // 8):
            i = slice(part * 8, part * 8 + 8)
            rho_sq, ab, ar, br = [buf[i, k * LANES : (k + 1) * LANES] for k in range(4)]
            inv_one = lax.rsqrt(rho_sq)
            inv_two = inv_one * inv_one
            inv_three = inv_two * inv_one
            coef = (ab + ar * br * inv_two) * inv_three
            ar = ar * inv_three
            acc[target, 0, i] += br * inv_three
            acc[target, 1, i] += coef
            for k in range(3):
                acc[target, 2 + k, i] += row[3 + k] * ar + row[k] * coef

    for i in range(DEPTH):
        products(i, one.at[i])

    def blocks(step, _):
        first = step * (2 * DEPTH)
        for i in range(DEPTH):
            products(first + DEPTH + i, two.at[i])
        for i in range(DEPTH):
            add_terms(first + i, one.at[i])
        for i in range(DEPTH):
            products(first + 2 * DEPTH + i, one.at[i])
        for i in range(DEPTH):
            add_terms(first + DEPTH + i, two.at[i])
        return 0

    lax.fori_loop(0, (count + 2 * DEPTH - 1) // (2 * DEPTH), blocks, 0)
    lane = iota((LANES, LANES), 1)
    for leaf in range(leaf_num):
        flat = jnp.zeros((LANES, LANES), F32)
        for k in range(5):
            flat = jnp.where(lane == k, jnp.sum(acc[leaf, k], axis=1, keepdims=True), flat)
        flat = flat.T
        tile = win[leaf_num + leaf]
        total = flat[0:1] * tile[3:6] * (1.0 / 3.0) + flat[2:5] - flat[1:2] * tile[0:3]
        near_ref[:, leaf * LANES : (leaf + 1) * LANES] = total * KERNEL


def columns(scratch, value):
    rows, width = value.shape
    scratch[0:rows, 0:width] = value.astype(F32)
    return scratch[...].T


def select_terms(rows, count_ref, slot_ref, class_ref, req_ref, main_ref, tail_ref, code_ref, kind_ref, scratch):
    leaf_num, far_num = slot_ref.shape
    cap, peers = req_ref.shape
    reps = LANES // leaf_num
    half = peers // 2
    scratch[...] = jnp.zeros((LANES, LANES), F32)
    asked = columns(scratch, req_ref[...])
    asked = jnp.concatenate([jnp.broadcast_to(asked[:, t : t + 1], (peers, LANES)) for t in range(cap)], 0)
    asked = asked.astype(BF16)
    slots = columns(scratch, slot_ref[...])
    classes = columns(scratch, class_ref[...])
    lane = iota((far_num, LANES), 1)
    row = iota((far_num, LANES), 0)

    def code(row):
        return jnp.where(lane == row % LANES, row // LANES, -1).astype(BF16)

    for leaf in range(leaf_num):
        at = slice(leaf * far_num, (leaf + 1) * far_num)
        slot = jnp.broadcast_to(slots[:far_num, leaf : leaf + 1], (far_num, LANES)).astype(jnp.int32)
        peer = slot // cap
        key = (slot - peer * cap) * peers + peer - lane
        picks = [jnp.where(key == t * peers, 1.0, 0.0).astype(BF16) for t in range(cap)]
        local = jnp.dot(jnp.concatenate(picks, 1), asked, preferred_element_type=F32).astype(jnp.int32)
        upper = (peer >= half).astype(jnp.int32)
        base = (peer - upper * half) * rows
        main_ref[at] = code(base + local)
        tail_ref[at] = code(base + leaf_num + local // reps)
        code_ref[at] = (upper + 2 * (lane // leaf_num == local % reps).astype(jnp.int32)).astype(BF16)
        kind = jnp.broadcast_to(classes[:far_num, leaf : leaf + 1], (far_num, LANES)).astype(jnp.int32)
        keep = (lane % leaf_num == leaf) & (row < count_ref[leaf])
        kind_ref[at] = jnp.where(keep, kind - lane // leaf_num, -LANES).astype(BF16)


def far_body(mom_ref, main_ref, tail_ref, code_ref, kind_ref, kept_ref, own_ref, near_ref, table_hbm, down_hbm, out_ref, table, down, pad, sums, sem):
    early = kept_ref.shape[0] - GROUP
    fetch = pltpu.make_async_copy(table_hbm.at[pl.ds(early, table.shape[0])], table, sem.at[0])
    fetch_down = pltpu.make_async_copy(down_hbm, down, sem.at[1])
    fetch.start()
    fetch_down.start()
    leaf_num, quads, width, _ = down.shape
    groups = pad.shape[0]
    half = mom_ref.shape[0] // 2
    both = jnp.concatenate([mom_ref[:half], mom_ref[half:]], 1)
    one, zero = jnp.ones((), BF16), jnp.zeros((), BF16)

    def hots(ref, count, stride=1):
        codes = ref[...]
        return [jnp.where(codes == i * stride, one, zero) for i in range(count)]

    tiles = half // LANES
    main = jnp.dot(jnp.concatenate(hots(main_ref, tiles), 1), both, preferred_element_type=F32)
    tails = jnp.dot(jnp.concatenate(hots(tail_ref, tiles), 1), both, preferred_element_type=F32)
    code = code_ref[...].astype(F32)
    upper = (code == 1.0) | (code == 3.0)
    main = jnp.where(upper, main[:, LANES:], main[:, :LANES]).T
    tails = jnp.where(upper, tails[:, LANES:], tails[:, :LANES])
    tails = jnp.where(code >= 2, tails, 0.0).T
    extra = width - LANES
    tails = sum(tails[i * extra : (i + 1) * extra] for i in range(LANES // extra))
    src_t = jnp.concatenate([main, tails], 0).astype(BF16)
    lead = 2 * LANES - width
    cols = GROUP * leaf_num
    per = cols // LANES
    hot = hots(kind_ref, groups * per, LANES // leaf_num)
    for g in range(groups):
        pad[g, 0:lead] = jnp.zeros((lead, cols), BF16)
        pad[g, lead + width :] = jnp.zeros((pad.shape[1] - lead - width, cols), BF16)
        part = jnp.dot(src_t, jnp.concatenate(hot[g * per : (g + 1) * per], 1), preferred_element_type=F32)
        pad[g, lead : lead + width] = part.astype(BF16)
    fetch.wait()
    step = width - LANES
    period = LANES // step
    tiles = period + 1
    blocks = width // period
    same = iota((blocks, GROUP, cols), 2) // leaf_num == iota((blocks, GROUP, cols), 1)
    for r in range(period):
        acc = None
        for g in range(groups):
            if g == groups - 1:
                ref, first = kept_ref, early
            elif g * GROUP < early:
                ref, first = kept_ref, g * GROUP
            else:
                ref, first = table, g * GROUP - early
            rows = [ref[first : first + GROUP, (tiles * b + r) * LANES : (tiles * b + r + 2) * LANES] for b in range(blocks)]
            part = jnp.dot(jnp.concatenate(rows, 0), pad[g, lead - step * r : lead - step * r + 2 * LANES], preferred_element_type=F32)
            acc = part if acc is None else acc + part
        acc = jnp.where(same, acc.reshape(blocks, GROUP, cols), 0.0)
        acc = jnp.sum(acc, axis=1)
        for h in range(cols // LANES):
            sums[h, pl.ds(r, blocks, stride=period), :] = acc[:, h * LANES : (h + 1) * LANES]
    fold = jnp.where(iota((leaf_num, cols), 1) % leaf_num == iota((leaf_num, cols), 0), 1.0, 0.0)
    whole = jnp.concatenate([sums[h] for h in range(cols // LANES)], 1)
    expansion = lax.dot_general(fold, whole, (((1,), (1,)), ((), ())), precision=lax.Precision.HIGHEST, preferred_element_type=F32)
    fetch_down.wait()
    which = iota((leaf_num, width), 0)
    field = [None] * quads
    for leaf in range(leaf_num):
        lhs = jnp.where(which == leaf, expansion, 0.0).astype(BF16)
        for q in range(0, quads, 2):
            both = [down[leaf, i] for i in range(q, min(q + 2, quads))]
            part = jnp.dot(lhs, jnp.concatenate(both, 1), preferred_element_type=F32)
            field[q] = part if field[q] is None else field[q] + part
    quad = [field[q - q % 2][:, (q % 2) * LANES : (q % 2 + 1) * LANES] for q in range(quads)]
    for leaf in range(leaf_num):
        at = slice(leaf * LANES, (leaf + 1) * LANES)
        far = []
        for k in range(3):
            far.append(sum(own_ref[3 + c : 4 + c, at] * quad[3 * c + k][leaf : leaf + 1] for c in range(3)))
        out_ref[:, at] = near_ref[:, at] + jnp.concatenate(far, 0)


SMEM = pl.BlockSpec(memory_space=pltpu.SMEM)
VMEM = pl.BlockSpec(memory_space=pltpu.VMEM)
HBM = pl.BlockSpec(memory_space=pltpu.HBM)


def held(x, space=pltpu.VMEM):
    return pltpu.with_memory_space_constraint(x, space)


def call(body, outs, limit, **options):
    if outs is not None:
        shapes = tuple(pltpu.VMEM(o[:-1], o[-1]) for o in outs)
        options["out_shape"] = shapes if len(shapes) > 1 else shapes[0]
    params = pltpu.CompilerParams(vmem_limit_bytes=limit * 2**20)
    return pl.pallas_call(body, compiler_params=params, **options)


def per_device(positions, densities, near_src, near_count, far_slot, far_class, far_count, requests, up_basis, transfer_table, down_basis):
    leaf_num, slot_num = near_src.shape
    nodes = positions.shape[1]
    width = up_basis.shape[1]
    far_num = far_slot.shape[1]
    peers = requests.shape[1]
    classes = transfer_table.shape[0]
    groups = -(-classes // GROUP)
    rows = leaf_num * width // LANES
    up = [(i, i + 1) for i in range(peers - 1)]
    down = [(j, i) for i, j in up]
    slots = leaf_num * far_num
    own, message = call(
        front_body,
        [(8, nodes + LANES, F32), (peers * rows, LANES, BF16)],
        8,
        in_specs=[HBM] * 5,
        scratch_shapes=[
            pltpu.VMEM((3, nodes), F32),
            pltpu.VMEM((3, nodes), F32),
            pltpu.VMEM((slot_num, leaf_num), jnp.int32),
            pltpu.VMEM((1, leaf_num), jnp.int32),
            pltpu.VMEM(up_basis.shape, BF16),
            pltpu.SemaphoreType.DMA((5,)),
        ],
    )(*[held(x, pltpu.HBM) for x in (positions, densities, near_src.T, near_count[None], up_basis)])
    left = lax.ppermute(own, "patch", up)
    right = lax.ppermute(own, "patch", down)
    message = message.reshape(peers, rows // 2, 2, LANES)
    table = lax.all_to_all(message, "patch", split_axis=0, concat_axis=0, tiled=True)
    table = table.reshape(peers * rows, LANES)
    down_flat = down_basis.transpose(0, 2, 1, 3)
    near, *kept = call(
        functools.partial(middle_body, rows),
        [
            (3, nodes, F32),
            (slots, LANES, BF16),
            (slots, LANES, BF16),
            (slots, LANES, BF16),
            (slots, LANES, BF16),
            ((EARLY + 1) * GROUP, width * width, BF16),
        ],
        36,
        in_specs=[VMEM] * 3 + [SMEM] + [VMEM] * 3 + [HBM],
        scratch_shapes=[
            pltpu.VMEM(transfer_table.shape, BF16),
            pltpu.SemaphoreType.DMA,
            pltpu.VMEM((3 * leaf_num, 8, LANES), F32),
            pltpu.VMEM((leaf_num + 1, LANES, 48), BF16),
            pltpu.VMEM((3 * leaf_num, 48, 4 * LANES), BF16),
            pltpu.VMEM((leaf_num + 1, 5, LANES, LANES), F32),
            pltpu.VMEM((DEPTH, LANES, 4 * LANES), F32),
            pltpu.VMEM((DEPTH, LANES, 4 * LANES), F32),
            pltpu.VMEM((4, slot_num, LANES), jnp.int32),
            pltpu.SMEM((4, slot_num, LANES), jnp.int32),
            pltpu.SMEM((4 * leaf_num * slot_num + 3 * DEPTH,), jnp.int32),
            pltpu.SemaphoreType.DMA,
            pltpu.VMEM((LANES, LANES), F32),
        ],
    )(held(own), held(left), held(right), far_count, far_slot, far_class, requests[0].T, held(transfer_table, pltpu.HBM))
    return call(
        far_body,
        None,
        30,
        in_specs=[VMEM] * 8 + [HBM] * 2,
        out_shape=jax.ShapeDtypeStruct((3, nodes), F32),
        scratch_shapes=[
            pltpu.VMEM(((groups - 1 - EARLY) * GROUP, width * width), BF16),
            pltpu.VMEM(down_flat.shape, BF16),
            pltpu.VMEM((groups, 4 * LANES - width, GROUP * leaf_num), BF16),
            pltpu.VMEM((GROUP * leaf_num // LANES, width, LANES), F32),
            pltpu.SemaphoreType.DMA((2,)),
        ],
    )(*[held(x) for x in (table, *kept, own, near)], held(transfer_table, pltpu.HBM), held(down_flat, pltpu.HBM))


def solution(mesh):
    placed = (
        P(None, "patch"),
        P(None, "patch"),
        P("patch", None),
        P("patch"),
        P("patch", None),
        P("patch", None),
        P("patch"),
        P("patch", None, None),
        P("patch", None, None),
        P(),
        P("patch", None, None, None),
    )
    return jax.shard_map(per_device, mesh=mesh, in_specs=placed, out_specs=P(None, "patch"), check_vma=False)
```

```python
import functools
import math

import jax
import jax.numpy as jnp
from jax import lax
from jax.experimental import pallas as pl
from jax.experimental.pallas import tpu as pltpu
from jax.sharding import PartitionSpec as P


KERNEL = 1.0 / (8.0 * math.pi)
BLOB = 0.25
LANES = 128
DEPTH = 2
EARLY = 2
GROUP = 16
F32 = jnp.float32
BF16 = jnp.bfloat16


def iota(shape, dim):
    return lax.broadcasted_iota(jnp.int32, shape, dim)


def front_body(pos_hbm, dens_hbm, src_hbm, count_hbm, up_hbm, own_ref, out_ref, pos_ref, dens_ref, src_ref, count_ref, up_ref, sem):
    refs = ((pos_hbm, pos_ref), (dens_hbm, dens_ref), (src_hbm, src_ref), (count_hbm, count_ref), (up_hbm, up_ref))
    copies = [pltpu.make_async_copy(a, b, sem.at[i]) for i, (a, b) in enumerate(refs)]
    for copy in copies:
        copy.start()
    leaf_num, width, _ = up_ref.shape
    nodes = pos_ref.shape[1]
    slots = src_ref.shape[0]
    own_ref[6:, :nodes] = jnp.zeros((2, nodes), F32)
    own_ref[:, nodes:] = jnp.zeros((slots, LANES), F32)
    for copy in copies[:4]:
        copy.wait()
    own_ref[0:3, :nodes] = pos_ref[...]
    own_ref[3:6, :nodes] = dens_ref[...]
    live = iota((slots, leaf_num), 0) < count_ref[...]
    own_ref[:, nodes : nodes + leaf_num] = jnp.where(live, src_ref[...] + 1, 0).astype(F32)
    copies[4].wait()
    lane = iota((width, LANES), 1)
    cols = jnp.zeros((width, LANES), F32)
    for leaf in range(leaf_num):
        total = None
        for comp in range(3):
            row = dens_ref[comp : comp + 1, leaf * LANES : (leaf + 1) * LANES]
            row = row.astype(BF16).astype(F32)
            part = up_ref[leaf, :, comp * LANES : (comp + 1) * LANES].astype(F32) * row
            total = part if total is None else total + part
        cols = jnp.where(lane == leaf, jnp.sum(total, axis=1, keepdims=True), cols)
    step = width - LANES
    reps = LANES // step
    tails = jnp.concatenate([cols[LANES:]] * reps, 0).T[:leaf_num]
    tails = jnp.where(iota(tails.shape, 1) // step == iota(tails.shape, 0) % reps, tails, 0.0)
    tails = [jnp.sum(tails[i : i + reps], axis=0, keepdims=True) for i in range(0, leaf_num, reps)]
    rows = jnp.concatenate([cols[:LANES].T[:leaf_num]] + tails, 0)
    rows = jnp.concatenate([rows] * 8, 0).astype(BF16)
    for i in range(out_ref.shape[0] // rows.shape[0]):
        out_ref[i * rows.shape[0] : (i + 1) * rows.shape[0]] = rows


def split(x):
    high = x.astype(BF16).astype(F32)
    mid = (x - high).astype(BF16).astype(F32)
    low = (x - high - mid).astype(BF16).astype(F32)
    return high, mid, low


TARGET_PARTS = (0, 0, 1, 0, 2, 1)
SOURCE_PARTS = (0, 1, 0, 2, 0, 1)


def target_rows(tile):
    row = iota(tile.shape, 0)
    x = jnp.where(row < 3, tile, 0.0)
    f = jnp.where(row < 3, pltpu.roll(tile, 5, 0), 0.0)
    norm = jnp.sum(x * x, axis=0, keepdims=True) + BLOB
    cross = jnp.sum(x * f, axis=0, keepdims=True)
    parts, norms, crosses = split(tile), split(norm), split(cross)
    out = []
    for q in range(6):
        extra = norms[q] if q < 3 else crosses[q - 3]
        out.append(jnp.where(row < 6, parts[TARGET_PARTS[q]], jnp.where(row == 6, extra, 1.0 if q < 3 else 0.0)))
    return jnp.concatenate(out, 0)


def source_rows(tile):
    row = iota(tile.shape, 0)
    first, second = row < 3, (row >= 3) & (row < 6)
    x = jnp.where(first, tile, 0.0)
    f = jnp.where(first, pltpu.roll(tile, 5, 0), 0.0)
    norms = split(jnp.sum(x * x, axis=0, keepdims=True))
    crosses = split(-3.0 * jnp.sum(x * f, axis=0, keepdims=True))
    parts = split(tile)
    low = split(pltpu.roll(tile, 3, 0))
    triple = split(3.0 * f)
    rho, ab, ar, br = [], [], [], []
    for q in range(6):
        k = SOURCE_PARTS[q]
        main = jnp.where(first, -2.0 * parts[k], 0.0)
        if q < 3:
            main = jnp.where(row == 6, 1.0, jnp.where(row == 7, norms[q], main))
        rho.append(main)
        ab.append(jnp.where(second, parts[k], 0.0))
        ar.append(jnp.where(second, -low[k], jnp.where(row == 6, 0.0 if q < 3 else 1.0, 0.0)))
        br.append(jnp.where(first, triple[k], jnp.where(row == 7, crosses[q], 0.0) if q < 3 else 0.0))
    return [jnp.concatenate(rows, 0).astype(BF16) for rows in (rho, ab, ar, br)]


def middle_body(rows, own_ref, left_ref, right_ref, count_hbm, slot_hbm, class_hbm, req_hbm, table_hbm, near_ref, main_ref, tail_ref, code_ref, kind_ref, kept_ref, table, count_ref, slot_ref, class_ref, req_ref, sems, win, lhs, rhs, acc, one, two, list_v, list_s, pairs, sem, flip):
    pairs_of = ((table_hbm, table), (count_hbm, count_ref), (slot_hbm, slot_ref), (class_hbm, class_ref), (req_hbm, req_ref))
    fetches = [pltpu.make_async_copy(a, b, sems.at[i]) for i, (a, b) in enumerate(pairs_of)]
    for fetch in fetches:
        fetch.start()
    near_terms(own_ref, left_ref, right_ref, near_ref, win, lhs, rhs, acc, one, two, list_v, list_s, pairs, sem)
    for fetch in fetches:
        fetch.wait()
    keep_rows(table, kept_ref)
    select_terms(rows, count_ref, slot_ref, class_ref, req_ref, main_ref, tail_ref, code_ref, kind_ref, flip)


def keep_rows(table, kept_ref):
    first = kept_ref.shape[0] - GROUP
    classes = table.shape[0]
    kept_ref[:first] = table[:first]
    whole = classes - classes % 8
    start = (classes - 1) // GROUP * GROUP
    width = 9 * LANES
    for at in range(0, table.shape[1], width):
        cols = slice(at, at + width)
        tail = table[whole:classes, cols].astype(F32)
        tail = jnp.concatenate([tail, jnp.zeros((start + GROUP - classes, width), F32)], 0)
        both = jnp.concatenate([table[start:whole, cols].astype(F32), tail], 0)
        kept_ref[first:, cols] = both.astype(BF16)


def near_terms(own_ref, left_ref, right_ref, near_ref, win, lhs, rhs, acc, one, two, list_v, list_s, pairs, sem):
    leaf_num = acc.shape[0] - 1
    nodes = leaf_num * LANES
    slots = list_v.shape[1]
    device = lax.axis_index("patch")
    halo = (left_ref, own_ref, right_ref)
    leaf_of = iota((slots, LANES), 1)
    for place, ref in enumerate(halo):
        listed = ref[:, nodes:].astype(jnp.int32)
        source = listed - (device * leaf_num + 1)
        mine = (listed > 0) & (source >= 0) & (source < leaf_num)
        list_v[place] = jnp.where(mine, (source << 6) + (leaf_of + place * leaf_num), -1)
        if place == 1:
            list_v[3] = jnp.where(listed > 0, (leaf_of << 6) + (source + leaf_num), -1)
    copy = pltpu.make_async_copy(list_v, list_s, sem)
    copy.start()
    acc[...] = jnp.zeros(acc.shape, F32)
    for place, ref in enumerate(halo):
        for leaf in range(leaf_num):
            tile = ref[:, leaf * LANES : (leaf + 1) * LANES]
            win[place * leaf_num + leaf] = tile
            for k, rows in enumerate(source_rows(tile)):
                rhs[place * leaf_num + leaf, :, k * LANES : (k + 1) * LANES] = rows
            if place == 1:
                lhs[leaf] = target_rows(tile).T.astype(BF16)
    lhs[leaf_num] = jnp.zeros(lhs.shape[1:], BF16)
    copy.wait()

    def scan(leaf, count):
        for place in range(list_s.shape[0]):
            for slot in range(slots):
                code = list_s[place, slot, leaf]
                pairs[count] = code
                count = count + (code >= 0).astype(jnp.int32)
        return count

    count = lax.fori_loop(0, leaf_num, scan, 0)
    for i in range(3 * DEPTH):
        pairs[count + i] = leaf_num * 64

    def products(at, buf):
        pair = pairs[at]
        buf[...] = jnp.dot(lhs[pair >> 6], rhs[pair & 63], preferred_element_type=F32)

    def add_terms(at, buf):
        pair = pairs[at]
        target, source = pair >> 6, pair & 63
        row = [jnp.broadcast_to(win[source, k : k + 1], (8, LANES)) for k in range(6)]
        for part in range(LANES // 8):
            i = slice(part * 8, part * 8 + 8)
            rho_sq, ab, ar, br = [buf[i, k * LANES : (k + 1) * LANES] for k in range(4)]
            inv_one = lax.rsqrt(rho_sq)
            inv_two = inv_one * inv_one
            inv_three = inv_two * inv_one
            coef = (ab + ar * br * inv_two) * inv_three
            ar = ar * inv_three
            acc[target, 0, i] += br * inv_three
            acc[target, 1, i] += coef
            for k in range(3):
                acc[target, 2 + k, i] += row[3 + k] * ar + row[k] * coef

    for i in range(DEPTH):
        products(i, one.at[i])

    def blocks(step, _):
        first = step * (2 * DEPTH)
        for i in range(DEPTH):
            products(first + DEPTH + i, two.at[i])
        for i in range(DEPTH):
            add_terms(first + i, one.at[i])
        for i in range(DEPTH):
            products(first + 2 * DEPTH + i, one.at[i])
        for i in range(DEPTH):
            add_terms(first + DEPTH + i, two.at[i])
        return 0

    lax.fori_loop(0, (count + 2 * DEPTH - 1) // (2 * DEPTH), blocks, 0)
    lane = iota((LANES, LANES), 1)
    for leaf in range(leaf_num):
        flat = jnp.zeros((LANES, LANES), F32)
        for k in range(5):
            flat = jnp.where(lane == k, jnp.sum(acc[leaf, k], axis=1, keepdims=True), flat)
        flat = flat.T
        tile = win[leaf_num + leaf]
        total = flat[0:1] * tile[3:6] * (1.0 / 3.0) + flat[2:5] - flat[1:2] * tile[0:3]
        near_ref[:, leaf * LANES : (leaf + 1) * LANES] = total * KERNEL


def columns(scratch, value):
    rows, width = value.shape
    scratch[0:rows, 0:width] = value.astype(F32)
    return scratch[...].T


def select_terms(rows, count_ref, slot_ref, class_ref, req_ref, main_ref, tail_ref, code_ref, kind_ref, scratch):
    leaf_num, far_num = slot_ref.shape
    cap, peers = req_ref.shape
    reps = LANES // leaf_num
    half = peers // 2
    scratch[...] = jnp.zeros((LANES, LANES), F32)
    asked = columns(scratch, req_ref[...])
    asked = jnp.concatenate([jnp.broadcast_to(asked[:, t : t + 1], (peers, LANES)) for t in range(cap)], 0)
    asked = asked.astype(BF16)
    slots = columns(scratch, slot_ref[...])
    classes = columns(scratch, class_ref[...])
    lane = iota((far_num, LANES), 1)
    row = iota((far_num, LANES), 0)

    def code(row):
        return jnp.where(lane == row % LANES, row // LANES, -1).astype(BF16)

    for leaf in range(leaf_num):
        at = slice(leaf * far_num, (leaf + 1) * far_num)
        slot = jnp.broadcast_to(slots[:far_num, leaf : leaf + 1], (far_num, LANES)).astype(jnp.int32)
        peer = slot // cap
        key = (slot - peer * cap) * peers + peer - lane
        picks = [jnp.where(key == t * peers, 1.0, 0.0).astype(BF16) for t in range(cap)]
        local = jnp.dot(jnp.concatenate(picks, 1), asked, preferred_element_type=F32).astype(jnp.int32)
        upper = (peer >= half).astype(jnp.int32)
        base = (peer - upper * half) * rows
        main_ref[at] = code(base + local)
        tail_ref[at] = code(base + leaf_num + local // reps)
        code_ref[at] = (upper + 2 * (lane // leaf_num == local % reps).astype(jnp.int32)).astype(BF16)
        kind = jnp.broadcast_to(classes[:far_num, leaf : leaf + 1], (far_num, LANES)).astype(jnp.int32)
        keep = (lane % leaf_num == leaf) & (row < count_ref[leaf])
        kind_ref[at] = jnp.where(keep, kind - lane // leaf_num, -LANES).astype(BF16)


def far_body(mom_ref, main_ref, tail_ref, code_ref, kind_ref, kept_ref, own_ref, near_ref, table_hbm, down_hbm, out_ref, table, down, pad, sums, sem):
    early = kept_ref.shape[0] - GROUP
    fetch = pltpu.make_async_copy(table_hbm.at[pl.ds(early, table.shape[0])], table, sem.at[0])
    fetch_down = pltpu.make_async_copy(down_hbm, down, sem.at[1])
    fetch.start()
    fetch_down.start()
    leaf_num, quads, width, _ = down.shape
    groups = pad.shape[0]
    lead = 2 * LANES - width
    cols = GROUP * leaf_num

    @pl.when(lax.axis_index("patch") >= 0)
    def _():
        groups = pad.shape[0]
        half = mom_ref.shape[0] // 2
        both = jnp.concatenate([mom_ref[:half], mom_ref[half:]], 1)
        one, zero = jnp.ones((), BF16), jnp.zeros((), BF16)

        def hots(ref, count, stride=1):
            codes = ref[...]
            return [jnp.where(codes == i * stride, one, zero) for i in range(count)]

        tiles = half // LANES
        main = jnp.dot(jnp.concatenate(hots(main_ref, tiles), 1), both, preferred_element_type=F32)
        tails = jnp.dot(jnp.concatenate(hots(tail_ref, tiles), 1), both, preferred_element_type=F32)
        code = code_ref[...].astype(F32)
        upper = (code == 1.0) | (code == 3.0)
        main = jnp.where(upper, main[:, LANES:], main[:, :LANES]).T
        tails = jnp.where(upper, tails[:, LANES:], tails[:, :LANES])
        tails = jnp.where(code >= 2, tails, 0.0).T
        extra = width - LANES
        tails = sum(tails[i * extra : (i + 1) * extra] for i in range(LANES // extra))
        src_t = jnp.concatenate([main, tails], 0).astype(BF16)
        lead = 2 * LANES - width
        cols = GROUP * leaf_num
        per = cols // LANES
        hot = hots(kind_ref, groups * per, LANES // leaf_num)
        for g in range(groups):
            pad[g, 0:lead] = jnp.zeros((lead, cols), BF16)
            pad[g, lead + width :] = jnp.zeros((pad.shape[1] - lead - width, cols), BF16)
            part = jnp.dot(src_t, jnp.concatenate(hot[g * per : (g + 1) * per], 1), preferred_element_type=F32)
            pad[g, lead : lead + width] = part.astype(BF16)

    fetch.wait()
    step = width - LANES
    period = LANES // step
    tiles = period + 1
    blocks = width // period
    same = iota((blocks, GROUP, cols), 2) // leaf_num == iota((blocks, GROUP, cols), 1)
    for r in range(period):
        acc = None
        for g in range(groups):
            if g == groups - 1:
                ref, first = kept_ref, early
            elif g * GROUP < early:
                ref, first = kept_ref, g * GROUP
            else:
                ref, first = table, g * GROUP - early
            rows = [ref[first : first + GROUP, (tiles * b + r) * LANES : (tiles * b + r + 2) * LANES] for b in range(blocks)]
            part = jnp.dot(jnp.concatenate(rows, 0), pad[g, lead - step * r : lead - step * r + 2 * LANES], preferred_element_type=F32)
            acc = part if acc is None else acc + part
        acc = jnp.where(same, acc.reshape(blocks, GROUP, cols), 0.0)
        acc = jnp.sum(acc, axis=1)
        for h in range(cols // LANES):
            sums[h, pl.ds(r, blocks, stride=period), :] = acc[:, h * LANES : (h + 1) * LANES]
    fold = jnp.where(iota((leaf_num, cols), 1) % leaf_num == iota((leaf_num, cols), 0), 1.0, 0.0)
    whole = jnp.concatenate([sums[h] for h in range(cols // LANES)], 1)
    expansion = lax.dot_general(fold, whole, (((1,), (1,)), ((), ())), precision=lax.Precision.HIGHEST, preferred_element_type=F32)
    fetch_down.wait()
    which = iota((leaf_num, width), 0)
    field = [None] * quads
    for leaf in range(leaf_num):
        lhs = jnp.where(which == leaf, expansion, 0.0).astype(BF16)
        for q in range(0, quads, 2):
            both = [down[leaf, i] for i in range(q, min(q + 2, quads))]
            part = jnp.dot(lhs, jnp.concatenate(both, 1), preferred_element_type=F32)
            field[q] = part if field[q] is None else field[q] + part
    quad = [field[q - q % 2][:, (q % 2) * LANES : (q % 2 + 1) * LANES] for q in range(quads)]
    for leaf in range(leaf_num):
        at = slice(leaf * LANES, (leaf + 1) * LANES)
        far = []
        for k in range(3):
            far.append(sum(own_ref[3 + c : 4 + c, at] * quad[3 * c + k][leaf : leaf + 1] for c in range(3)))
        out_ref[:, at] = near_ref[:, at] + jnp.concatenate(far, 0)


SMEM = pl.BlockSpec(memory_space=pltpu.SMEM)
VMEM = pl.BlockSpec(memory_space=pltpu.VMEM)
HBM = pl.BlockSpec(memory_space=pltpu.HBM)


def held(x, space=pltpu.VMEM):
    return pltpu.with_memory_space_constraint(x, space)


def call(body, outs, limit, **options):
    if outs is not None:
        shapes = tuple(pltpu.VMEM(o[:-1], o[-1]) for o in outs)
        options["out_shape"] = shapes if len(shapes) > 1 else shapes[0]
    params = pltpu.CompilerParams(vmem_limit_bytes=limit * 2**20)
    return pl.pallas_call(body, compiler_params=params, **options)


def per_device(positions, densities, near_src, near_count, far_slot, far_class, far_count, requests, up_basis, transfer_table, down_basis):
    leaf_num, slot_num = near_src.shape
    nodes = positions.shape[1]
    width = up_basis.shape[1]
    far_num = far_slot.shape[1]
    peers = requests.shape[1]
    classes = transfer_table.shape[0]
    groups = -(-classes // GROUP)
    rows = leaf_num * width // LANES
    up = [(i, i + 1) for i in range(peers - 1)]
    down = [(j, i) for i, j in up]
    slots = leaf_num * far_num
    own, message = call(
        front_body,
        [(8, nodes + LANES, F32), (peers * rows, LANES, BF16)],
        8,
        in_specs=[HBM] * 5,
        scratch_shapes=[
            pltpu.VMEM((3, nodes), F32),
            pltpu.VMEM((3, nodes), F32),
            pltpu.VMEM((slot_num, leaf_num), jnp.int32),
            pltpu.VMEM((1, leaf_num), jnp.int32),
            pltpu.VMEM(up_basis.shape, BF16),
            pltpu.SemaphoreType.DMA((5,)),
        ],
    )(*[held(x, pltpu.HBM) for x in (positions, densities, near_src.T, near_count[None], up_basis)])
    left = lax.ppermute(own, "patch", up)
    right = lax.ppermute(own, "patch", down)
    message = message.reshape(peers, rows // 2, 2, LANES)
    table = lax.all_to_all(message, "patch", split_axis=0, concat_axis=0, tiled=True)
    table = table.reshape(peers * rows, LANES)
    down_flat = down_basis.transpose(0, 2, 1, 3)
    near, *kept = call(
        functools.partial(middle_body, rows),
        [
            (3, nodes, F32),
            (slots, LANES, BF16),
            (slots, LANES, BF16),
            (slots, LANES, BF16),
            (slots, LANES, BF16),
            ((EARLY + 1) * GROUP, width * width, BF16),
        ],
        36,
        in_specs=[VMEM] * 3 + [HBM] * 5,
        scratch_shapes=[
            pltpu.VMEM(transfer_table.shape, BF16),
            pltpu.SMEM(far_count.shape, jnp.int32),
            pltpu.VMEM(far_slot.shape, jnp.int32),
            pltpu.VMEM(far_class.shape, jnp.int32),
            pltpu.VMEM((requests.shape[2], peers), jnp.int32),
            pltpu.SemaphoreType.DMA((5,)),
            pltpu.VMEM((3 * leaf_num, 8, LANES), F32),
            pltpu.VMEM((leaf_num + 1, LANES, 48), BF16),
            pltpu.VMEM((3 * leaf_num, 48, 4 * LANES), BF16),
            pltpu.VMEM((leaf_num + 1, 5, LANES, LANES), F32),
            pltpu.VMEM((DEPTH, LANES, 4 * LANES), F32),
            pltpu.VMEM((DEPTH, LANES, 4 * LANES), F32),
            pltpu.VMEM((4, slot_num, LANES), jnp.int32),
            pltpu.SMEM((4, slot_num, LANES), jnp.int32),
            pltpu.SMEM((4 * leaf_num * slot_num + 3 * DEPTH,), jnp.int32),
            pltpu.SemaphoreType.DMA,
            pltpu.VMEM((LANES, LANES), F32),
        ],
    )(held(own), held(left), held(right), *[held(x, pltpu.HBM) for x in (far_count, far_slot, far_class, requests[0].T, transfer_table)])
    return call(
        far_body,
        None,
        30,
        in_specs=[VMEM] * 8 + [HBM] * 2,
        out_shape=jax.ShapeDtypeStruct((3, nodes), F32),
        scratch_shapes=[
            pltpu.VMEM(((groups - 1 - EARLY) * GROUP, width * width), BF16),
            pltpu.VMEM(down_flat.shape, BF16),
            pltpu.VMEM((groups, 4 * LANES - width, GROUP * leaf_num), BF16),
            pltpu.VMEM((GROUP * leaf_num // LANES, width, LANES), F32),
            pltpu.SemaphoreType.DMA((2,)),
        ],
    )(*[held(x) for x in (table, *kept, own, near)], held(transfer_table, pltpu.HBM), held(down_flat, pltpu.HBM))


def solution(mesh):
    placed = (
        P(None, "patch"),
        P(None, "patch"),
        P("patch", None),
        P("patch"),
        P("patch", None),
        P("patch", None),
        P("patch"),
        P("patch", None, None),
        P("patch", None, None),
        P(),
        P("patch", None, None, None),
    )
    return jax.shard_map(per_device, mesh=mesh, in_specs=placed, out_specs=P(None, "patch"), check_vma=False)
```

```python
import math

import jax
import jax.numpy as jnp
from jax import lax
from jax.experimental import pallas as pl
from jax.experimental.pallas import tpu as pltpu
from jax.sharding import PartitionSpec as P


KERNEL = 1.0 / (8.0 * math.pi)
BLOB = 0.25
LANES = 128
DEPTH = 2
EARLY = 3
GROUP = 16
F32 = jnp.float32
BF16 = jnp.bfloat16


def iota(shape, dim):
    return lax.broadcasted_iota(jnp.int32, shape, dim)


def front_body(pos_hbm, dens_hbm, src_hbm, count_hbm, up_hbm, own_ref, out_ref, pos_ref, dens_ref, src_ref, count_ref, up_ref, sem):
    refs = ((pos_hbm, pos_ref), (dens_hbm, dens_ref), (src_hbm, src_ref), (count_hbm, count_ref), (up_hbm, up_ref))
    copies = [pltpu.make_async_copy(a, b, sem.at[i]) for i, (a, b) in enumerate(refs)]
    for copy in copies:
        copy.start()
    leaf_num, width, _ = up_ref.shape
    nodes = pos_ref.shape[1]
    slots = src_ref.shape[0]
    own_ref[6:, :nodes] = jnp.zeros((2, nodes), F32)
    own_ref[:, nodes:] = jnp.zeros((slots, LANES), F32)
    for copy in copies[:4]:
        copy.wait()
    own_ref[0:3, :nodes] = pos_ref[...]
    own_ref[3:6, :nodes] = dens_ref[...]
    live = iota((slots, leaf_num), 0) < count_ref[...]
    own_ref[:, nodes : nodes + leaf_num] = jnp.where(live, src_ref[...] + 1, 0).astype(F32)
    copies[4].wait()
    lane = iota((width, LANES), 1)
    cols = jnp.zeros((width, LANES), F32)
    for leaf in range(leaf_num):
        total = None
        for comp in range(3):
            row = dens_ref[comp : comp + 1, leaf * LANES : (leaf + 1) * LANES]
            row = row.astype(BF16).astype(F32)
            part = up_ref[leaf, :, comp * LANES : (comp + 1) * LANES].astype(F32) * row
            total = part if total is None else total + part
        cols = jnp.where(lane == leaf, jnp.sum(total, axis=1, keepdims=True), cols)
    step = width - LANES
    reps = LANES // step
    tails = jnp.concatenate([cols[LANES:]] * reps, 0).T[:leaf_num]
    tails = jnp.where(iota(tails.shape, 1) // step == iota(tails.shape, 0) % reps, tails, 0.0)
    tails = [jnp.sum(tails[i : i + reps], axis=0, keepdims=True) for i in range(0, leaf_num, reps)]
    rows = jnp.concatenate([cols[:LANES].T[:leaf_num]] + tails, 0)
    rows = jnp.concatenate([rows] * 8, 0).astype(BF16)
    for i in range(out_ref.shape[0] // rows.shape[0]):
        out_ref[i * rows.shape[0] : (i + 1) * rows.shape[0]] = rows


def split(x):
    high = x.astype(BF16).astype(F32)
    mid = (x - high).astype(BF16).astype(F32)
    low = (x - high - mid).astype(BF16).astype(F32)
    return high, mid, low


TARGET_PARTS = (0, 0, 1, 0, 2, 1)
SOURCE_PARTS = (0, 1, 0, 2, 0, 1)


def target_rows(tile):
    row = iota(tile.shape, 0)
    x = jnp.where(row < 3, tile, 0.0)
    f = jnp.where(row < 3, pltpu.roll(tile, 5, 0), 0.0)
    norm = jnp.sum(x * x, axis=0, keepdims=True) + BLOB
    cross = jnp.sum(x * f, axis=0, keepdims=True)
    parts, norms, crosses = split(tile), split(norm), split(cross)
    out = []
    for q in range(6):
        extra = norms[q] if q < 3 else crosses[q - 3]
        out.append(jnp.where(row < 6, parts[TARGET_PARTS[q]], jnp.where(row == 6, extra, 1.0 if q < 3 else 0.0)))
    return jnp.concatenate(out, 0)


def source_rows(tile):
    row = iota(tile.shape, 0)
    first, second = row < 3, (row >= 3) & (row < 6)
    x = jnp.where(first, tile, 0.0)
    f = jnp.where(first, pltpu.roll(tile, 5, 0), 0.0)
    norms = split(jnp.sum(x * x, axis=0, keepdims=True))
    crosses = split(-3.0 * jnp.sum(x * f, axis=0, keepdims=True))
    parts = split(tile)
    low = split(pltpu.roll(tile, 3, 0))
    triple = split(3.0 * f)
    rho, ab, ar, br = [], [], [], []
    for q in range(6):
        k = SOURCE_PARTS[q]
        main = jnp.where(first, -2.0 * parts[k], 0.0)
        if q < 3:
            main = jnp.where(row == 6, 1.0, jnp.where(row == 7, norms[q], main))
        rho.append(main)
        ab.append(jnp.where(second, parts[k], 0.0))
        ar.append(jnp.where(second, -low[k], jnp.where(row == 6, 0.0 if q < 3 else 1.0, 0.0)))
        br.append(jnp.where(first, triple[k], jnp.where(row == 7, crosses[q], 0.0) if q < 3 else 0.0))
    return [jnp.concatenate(rows, 0).astype(BF16) for rows in (rho, ab, ar, br)]


def middle_body(own_ref, left_ref, right_ref, count_hbm, slot_hbm, class_hbm, req_hbm, table_hbm, near_ref, slot_ref, req_ref, kind_ref, kept_ref, table, count_ref, class_ref, sems, win, lhs, rhs, acc, one, two, list_v, list_s, pairs, sem, flip):
    pairs_of = ((table_hbm, table), (count_hbm, count_ref), (slot_hbm, slot_ref), (class_hbm, class_ref), (req_hbm, req_ref))
    fetches = [pltpu.make_async_copy(a, b, sems.at[i]) for i, (a, b) in enumerate(pairs_of)]
    for fetch in fetches:
        fetch.start()
    near_terms(own_ref, left_ref, right_ref, near_ref, win, lhs, rhs, acc, one, two, list_v, list_s, pairs, sem)
    for fetch in fetches:
        fetch.wait()
    keep_rows(table, kept_ref)
    class_terms(count_ref, class_ref, kind_ref, flip)


def keep_rows(table, kept_ref):
    first = kept_ref.shape[0] - GROUP
    classes = table.shape[0]
    kept_ref[:first] = table[:first]
    whole = classes - classes % 8
    start = (classes - 1) // GROUP * GROUP
    width = 9 * LANES
    for at in range(0, table.shape[1], width):
        cols = slice(at, at + width)
        tail = table[whole:classes, cols].astype(F32)
        tail = jnp.concatenate([tail, jnp.zeros((start + GROUP - classes, width), F32)], 0)
        both = jnp.concatenate([table[start:whole, cols].astype(F32), tail], 0)
        kept_ref[first:, cols] = both.astype(BF16)


def near_terms(own_ref, left_ref, right_ref, near_ref, win, lhs, rhs, acc, one, two, list_v, list_s, pairs, sem):
    leaf_num = acc.shape[0] - 1
    nodes = leaf_num * LANES
    slots = list_v.shape[1]
    device = lax.axis_index("patch")
    halo = (left_ref, own_ref, right_ref)
    leaf_of = iota((slots, LANES), 1)
    for place, ref in enumerate(halo):
        listed = ref[:, nodes:].astype(jnp.int32)
        source = listed - (device * leaf_num + 1)
        mine = (listed > 0) & (source >= 0) & (source < leaf_num)
        list_v[place] = jnp.where(mine, (source << 6) + (leaf_of + place * leaf_num), -1)
        if place == 1:
            list_v[3] = jnp.where(listed > 0, (leaf_of << 6) + (source + leaf_num), -1)
    copy = pltpu.make_async_copy(list_v, list_s, sem)
    copy.start()

    def clear(leaf, _):
        acc[leaf] = jnp.zeros(acc.shape[1:], F32)
        return 0

    lax.fori_loop(0, leaf_num, clear, 0)
    lhs[leaf_num] = jnp.zeros(lhs.shape[1:], BF16)
    copy.wait()
    dead, seen = jnp.int32(0), 0
    for leaf in range(leaf_num):
        for place, ref in enumerate(halo):
            tile = ref[:, leaf * LANES : (leaf + 1) * LANES]
            win[place * leaf_num + leaf] = tile
            for k, rows in enumerate(source_rows(tile)):
                rhs[place * leaf_num + leaf, :, k * LANES : (k + 1) * LANES] = rows
            if place == 1:
                lhs[leaf] = target_rows(tile).T.astype(BF16)
        for place in range(list_s.shape[0]):
            for slot in range(slots):
                code = list_s[place, slot, leaf]
                pairs[dead + seen] = code
                dead = dead + (code >> 31)
                seen = seen + 1
    count = dead + seen
    for i in range(3 * DEPTH):
        pairs[count + i] = leaf_num * 64

    def products(at, buf):
        pair = pairs[at]
        buf[...] = jnp.dot(lhs[pair >> 6], rhs[pair & 63], preferred_element_type=F32)

    def add_terms(at, buf):
        pair = pairs[at]
        target, source = pair >> 6, pair & 63
        row = [jnp.broadcast_to(win[source, k : k + 1], (8, LANES)) for k in range(6)]
        for part in range(LANES // 8):
            i = slice(part * 8, part * 8 + 8)
            rho_sq, ab, ar, br = [buf[i, k * LANES : (k + 1) * LANES] for k in range(4)]
            inv_one = lax.rsqrt(rho_sq)
            inv_two = inv_one * inv_one
            inv_three = inv_two * inv_one
            coef = (ab + ar * br * inv_two) * inv_three
            ar = ar * inv_three
            acc[target, 0, i] += br * inv_three
            acc[target, 1, i] += coef
            for k in range(3):
                acc[target, 2 + k, i] += row[3 + k] * ar + row[k] * coef

    for i in range(DEPTH):
        products(i, one.at[i])

    def blocks(step, _):
        first = step * (2 * DEPTH)
        for i in range(DEPTH):
            products(first + DEPTH + i, two.at[i])
        for i in range(DEPTH):
            add_terms(first + i, one.at[i])
        for i in range(DEPTH):
            products(first + 2 * DEPTH + i, one.at[i])
        for i in range(DEPTH):
            add_terms(first + DEPTH + i, two.at[i])
        return 0

    lax.fori_loop(0, (count + 2 * DEPTH - 1) // (2 * DEPTH), blocks, 0)
    lane = iota((LANES, LANES), 1)
    for leaf in range(leaf_num):
        flat = jnp.zeros((LANES, LANES), F32)
        for k in range(5):
            flat = jnp.where(lane == k, jnp.sum(acc[leaf, k], axis=1, keepdims=True), flat)
        flat = flat.T
        tile = win[leaf_num + leaf]
        total = flat[0:1] * tile[3:6] * (1.0 / 3.0) + flat[2:5] - flat[1:2] * tile[0:3]
        near_ref[:, leaf * LANES : (leaf + 1) * LANES] = total * KERNEL


def columns(scratch, value):
    rows, width = value.shape
    scratch[0:rows, 0:width] = value.astype(F32)
    return scratch[...].T


def class_terms(count_ref, class_ref, kind_ref, scratch):
    leaf_num, far_num = class_ref.shape
    scratch[...] = jnp.zeros((LANES, LANES), F32)
    classes = columns(scratch, class_ref[...])
    lane = iota((far_num, LANES), 1)
    row = iota((far_num, LANES), 0)
    for leaf in range(leaf_num):
        at = slice(leaf * far_num, (leaf + 1) * far_num)
        kind = jnp.broadcast_to(classes[:far_num, leaf : leaf + 1], (far_num, LANES)).astype(jnp.int32)
        keep = (lane % leaf_num == leaf) & (row < count_ref[leaf])
        kind_ref[at] = jnp.where(keep, kind - lane // leaf_num, -LANES).astype(BF16)


def slot_terms(rows, slot_ref, req_ref, main_ref, tail_ref, code_ref, scratch):
    leaf_num, far_num = slot_ref.shape
    cap, peers = req_ref.shape
    reps = LANES // leaf_num
    half = peers // 2
    scratch[...] = jnp.zeros((LANES, LANES), F32)
    asked = columns(scratch, req_ref[...])
    asked = jnp.concatenate([jnp.broadcast_to(asked[:, t : t + 1], (peers, LANES)) for t in range(cap)], 0)
    asked = asked.astype(BF16)
    slots = columns(scratch, slot_ref[...])
    slot = jnp.concatenate([jnp.broadcast_to(slots[:far_num, i : i + 1], (far_num, LANES)) for i in range(leaf_num)], 0)
    slot = slot.astype(jnp.int32)
    lane = iota(slot.shape, 1)
    peer = slot // cap
    key = (slot - peer * cap) * peers + peer - lane
    picks = [jnp.where(key == t * peers, 1.0, 0.0).astype(BF16) for t in range(cap)]
    local = jnp.dot(jnp.concatenate(picks, 1), asked, preferred_element_type=F32).astype(jnp.int32)
    upper = (peer >= half).astype(jnp.int32)
    base = (peer - upper * half) * rows

    def code(row):
        return jnp.where(lane == row % LANES, row // LANES, -1).astype(BF16)

    main_ref[...] = code(base + local)
    tail_ref[...] = code(base + leaf_num + local // reps)
    code_ref[...] = (upper + 2 * (lane // leaf_num == local % reps).astype(jnp.int32)).astype(BF16)


def far_body(mom_ref, slot_ref, req_ref, kind_ref, kept_ref, own_ref, near_ref, table_hbm, down_hbm, out_ref, main_ref, tail_ref, code_ref, flip, table, down, pad, sums, sem):
    early = kept_ref.shape[0] - GROUP
    fetch = pltpu.make_async_copy(table_hbm.at[pl.ds(early, table.shape[0])], table, sem.at[0])
    fetch_down = pltpu.make_async_copy(down_hbm, down, sem.at[1])
    fetch.start()
    fetch_down.start()
    leaf_num, quads, width, _ = down.shape
    groups = pad.shape[0]
    lead = 2 * LANES - width
    cols = GROUP * leaf_num

    @pl.when(lax.axis_index("patch") >= 0)
    def _():
        slot_terms(mom_ref.shape[0] // (req_ref.shape[1]), slot_ref, req_ref, main_ref, tail_ref, code_ref, flip)
        half = mom_ref.shape[0] // 2
        both = jnp.concatenate([mom_ref[:half], mom_ref[half:]], 1)
        one, zero = jnp.ones((), BF16), jnp.zeros((), BF16)

        def hots(ref, count, stride=1):
            codes = ref[...]
            return [jnp.where(codes == i * stride, one, zero) for i in range(count)]

        tiles = half // LANES
        main = jnp.dot(jnp.concatenate(hots(main_ref, tiles), 1), both, preferred_element_type=F32)
        tails = jnp.dot(jnp.concatenate(hots(tail_ref, tiles), 1), both, preferred_element_type=F32)
        code = code_ref[...].astype(F32)
        upper = (code == 1.0) | (code == 3.0)
        main = jnp.where(upper, main[:, LANES:], main[:, :LANES]).T
        tails = jnp.where(upper, tails[:, LANES:], tails[:, :LANES])
        tails = jnp.where(code >= 2, tails, 0.0).T
        extra = width - LANES
        tails = sum(tails[i * extra : (i + 1) * extra] for i in range(LANES // extra))
        src_t = jnp.concatenate([main, tails], 0).astype(BF16)
        per = cols // LANES
        hot = hots(kind_ref, groups * per, LANES // leaf_num)
        for g in range(groups):
            pad[g, 0:lead] = jnp.zeros((lead, cols), BF16)
            pad[g, lead + width :] = jnp.zeros((pad.shape[1] - lead - width, cols), BF16)
            part = jnp.dot(src_t, jnp.concatenate(hot[g * per : (g + 1) * per], 1), preferred_element_type=F32)
            pad[g, lead : lead + width] = part.astype(BF16)

    fetch.wait()
    step = width - LANES
    period = LANES // step
    tiles = period + 1
    blocks = width // period
    same = iota((blocks, GROUP, cols), 2) // leaf_num == iota((blocks, GROUP, cols), 1)
    for r in range(period):
        acc = None
        for g in range(groups):
            if g == groups - 1:
                ref, first = kept_ref, early
            elif g * GROUP < early:
                ref, first = kept_ref, g * GROUP
            else:
                ref, first = table, g * GROUP - early
            rows = [ref[first : first + GROUP, (tiles * b + r) * LANES : (tiles * b + r + 2) * LANES] for b in range(blocks)]
            part = jnp.dot(jnp.concatenate(rows, 0), pad[g, lead - step * r : lead - step * r + 2 * LANES], preferred_element_type=F32)
            acc = part if acc is None else acc + part
        acc = jnp.where(same, acc.reshape(blocks, GROUP, cols), 0.0)
        acc = jnp.sum(acc, axis=1)
        for h in range(cols // LANES):
            sums[h, pl.ds(r, blocks, stride=period), :] = acc[:, h * LANES : (h + 1) * LANES]
    fold = jnp.where(iota((leaf_num, cols), 1) % leaf_num == iota((leaf_num, cols), 0), 1.0, 0.0)
    whole = jnp.concatenate([sums[h] for h in range(cols // LANES)], 1)
    expansion = lax.dot_general(fold, whole, (((1,), (1,)), ((), ())), precision=lax.Precision.HIGHEST, preferred_element_type=F32)
    fetch_down.wait()
    which = iota((leaf_num, width), 0)
    field = [None] * quads
    for leaf in range(leaf_num):
        lhs = jnp.where(which == leaf, expansion, 0.0).astype(BF16)
        for q in range(0, quads, 2):
            both = [down[leaf, i] for i in range(q, min(q + 2, quads))]
            part = jnp.dot(lhs, jnp.concatenate(both, 1), preferred_element_type=F32)
            field[q] = part if field[q] is None else field[q] + part
    quad = [field[q - q % 2][:, (q % 2) * LANES : (q % 2 + 1) * LANES] for q in range(quads)]
    for leaf in range(leaf_num):
        at = slice(leaf * LANES, (leaf + 1) * LANES)
        far = []
        for k in range(3):
            far.append(sum(own_ref[3 + c : 4 + c, at] * quad[3 * c + k][leaf : leaf + 1] for c in range(3)))
        out_ref[:, at] = near_ref[:, at] + jnp.concatenate(far, 0)


SMEM = pl.BlockSpec(memory_space=pltpu.SMEM)
VMEM = pl.BlockSpec(memory_space=pltpu.VMEM)
HBM = pl.BlockSpec(memory_space=pltpu.HBM)


def held(x, space=pltpu.VMEM):
    return pltpu.with_memory_space_constraint(x, space)


def call(body, outs, limit, **options):
    if outs is not None:
        shapes = tuple(pltpu.VMEM(o[:-1], o[-1]) for o in outs)
        options["out_shape"] = shapes if len(shapes) > 1 else shapes[0]
    params = pltpu.CompilerParams(vmem_limit_bytes=limit * 2**20)
    return pl.pallas_call(body, compiler_params=params, **options)


def per_device(positions, densities, near_src, near_count, far_slot, far_class, far_count, requests, up_basis, transfer_table, down_basis):
    leaf_num, slot_num = near_src.shape
    nodes = positions.shape[1]
    width = up_basis.shape[1]
    far_num = far_slot.shape[1]
    peers = requests.shape[1]
    classes = transfer_table.shape[0]
    groups = -(-classes // GROUP)
    rows = leaf_num * width // LANES
    up = [(i, i + 1) for i in range(peers - 1)]
    down = [(j, i) for i, j in up]
    slots = leaf_num * far_num
    own, message = call(
        front_body,
        [(8, nodes + LANES, F32), (peers * rows, LANES, BF16)],
        8,
        in_specs=[HBM] * 5,
        scratch_shapes=[
            pltpu.VMEM((3, nodes), F32),
            pltpu.VMEM((3, nodes), F32),
            pltpu.VMEM((slot_num, leaf_num), jnp.int32),
            pltpu.VMEM((1, leaf_num), jnp.int32),
            pltpu.VMEM(up_basis.shape, BF16),
            pltpu.SemaphoreType.DMA((5,)),
        ],
    )(*[held(x, pltpu.HBM) for x in (positions, densities, near_src.T, near_count[None], up_basis)])
    left = lax.ppermute(own, "patch", up)
    right = lax.ppermute(own, "patch", down)
    message = message.reshape(peers, rows // 2, 2, LANES)
    table = lax.all_to_all(message, "patch", split_axis=0, concat_axis=0, tiled=True)
    table = table.reshape(peers * rows, LANES)
    down_flat = down_basis.transpose(0, 2, 1, 3)
    near, *kept = call(
        middle_body,
        [
            (3, nodes, F32),
            far_slot.shape + (jnp.int32,),
            (requests.shape[2], peers, jnp.int32),
            (slots, LANES, BF16),
            ((EARLY + 1) * GROUP, width * width, BF16),
        ],
        36,
        in_specs=[VMEM] * 3 + [HBM] * 5,
        scratch_shapes=[
            pltpu.VMEM(transfer_table.shape, BF16),
            pltpu.SMEM(far_count.shape, jnp.int32),
            pltpu.VMEM(far_class.shape, jnp.int32),
            pltpu.SemaphoreType.DMA((5,)),
            pltpu.VMEM((3 * leaf_num, 8, LANES), F32),
            pltpu.VMEM((leaf_num + 1, LANES, 48), BF16),
            pltpu.VMEM((3 * leaf_num, 48, 4 * LANES), BF16),
            pltpu.VMEM((leaf_num + 1, 5, LANES, LANES), F32),
            pltpu.VMEM((DEPTH, LANES, 4 * LANES), F32),
            pltpu.VMEM((DEPTH, LANES, 4 * LANES), F32),
            pltpu.VMEM((4, slot_num, LANES), jnp.int32),
            pltpu.SMEM((4, slot_num, LANES), jnp.int32),
            pltpu.SMEM((4 * leaf_num * slot_num + 3 * DEPTH,), jnp.int32),
            pltpu.SemaphoreType.DMA,
            pltpu.VMEM((LANES, LANES), F32),
        ],
    )(held(own), held(left), held(right), *[held(x, pltpu.HBM) for x in (far_count, far_slot, far_class, requests[0].T, transfer_table)])
    return call(
        far_body,
        None,
        30,
        in_specs=[VMEM] * 7 + [HBM] * 2,
        out_shape=jax.ShapeDtypeStruct((3, nodes), F32),
        scratch_shapes=[
            pltpu.VMEM((slots, LANES), BF16),
            pltpu.VMEM((slots, LANES), BF16),
            pltpu.VMEM((slots, LANES), BF16),
            pltpu.VMEM((LANES, LANES), F32),
            pltpu.VMEM(((groups - 1 - EARLY) * GROUP, width * width), BF16),
            pltpu.VMEM(down_flat.shape, BF16),
            pltpu.VMEM((groups, 4 * LANES - width, GROUP * leaf_num), BF16),
            pltpu.VMEM((GROUP * leaf_num // LANES, width, LANES), F32),
            pltpu.SemaphoreType.DMA((2,)),
        ],
    )(*[held(x) for x in (table, *kept, own, near)], held(transfer_table, pltpu.HBM), held(down_flat, pltpu.HBM))


def solution(mesh):
    placed = (
        P(None, "patch"),
        P(None, "patch"),
        P("patch", None),
        P("patch"),
        P("patch", None),
        P("patch", None),
        P("patch"),
        P("patch", None, None),
        P("patch", None, None),
        P(),
        P("patch", None, None, None),
    )
    return jax.shard_map(per_device, mesh=mesh, in_specs=placed, out_specs=P(None, "patch"), check_vma=False)
```

```python
import math

import jax
import jax.numpy as jnp
from jax import lax
from jax.experimental import pallas as pl
from jax.experimental.pallas import tpu as pltpu
from jax.sharding import PartitionSpec as P


KERNEL = 1.0 / (8.0 * math.pi)
BLOB = 0.25
LANES = 128
DEPTH = 3
EARLY = 2
GROUP = 16
F32 = jnp.float32
BF16 = jnp.bfloat16


def iota(shape, dim):
    return lax.broadcasted_iota(jnp.int32, shape, dim)


def front_body(pos_hbm, dens_hbm, src_hbm, count_hbm, up_hbm, own_ref, out_ref, pos_ref, dens_ref, src_ref, count_ref, up_ref, sem):
    refs = ((pos_hbm, pos_ref), (dens_hbm, dens_ref), (src_hbm, src_ref), (count_hbm, count_ref), (up_hbm, up_ref))
    copies = [pltpu.make_async_copy(a, b, sem.at[i]) for i, (a, b) in enumerate(refs)]
    for copy in copies:
        copy.start()
    leaf_num, width, _ = up_ref.shape
    nodes = pos_ref.shape[1]
    slots = src_ref.shape[0]
    own_ref[6:, :nodes] = jnp.zeros((2, nodes), F32)
    own_ref[:, nodes:] = jnp.zeros((slots, LANES), F32)
    for copy in copies[:4]:
        copy.wait()
    own_ref[0:3, :nodes] = pos_ref[...]
    own_ref[3:6, :nodes] = dens_ref[...]
    live = iota((slots, leaf_num), 0) < count_ref[...]
    own_ref[:, nodes : nodes + leaf_num] = jnp.where(live, src_ref[...] + 1, 0).astype(F32)
    copies[4].wait()
    lane = iota((width, LANES), 1)
    cols = jnp.zeros((width, LANES), F32)
    for leaf in range(leaf_num):
        total = None
        for comp in range(3):
            row = dens_ref[comp : comp + 1, leaf * LANES : (leaf + 1) * LANES]
            row = row.astype(BF16).astype(F32)
            part = up_ref[leaf, :, comp * LANES : (comp + 1) * LANES].astype(F32) * row
            total = part if total is None else total + part
        cols = jnp.where(lane == leaf, jnp.sum(total, axis=1, keepdims=True), cols)
    step = width - LANES
    reps = LANES // step
    tails = jnp.concatenate([cols[LANES:]] * reps, 0).T[:leaf_num]
    tails = jnp.where(iota(tails.shape, 1) // step == iota(tails.shape, 0) % reps, tails, 0.0)
    tails = [jnp.sum(tails[i : i + reps], axis=0, keepdims=True) for i in range(0, leaf_num, reps)]
    rows = jnp.concatenate([cols[:LANES].T[:leaf_num]] + tails, 0)
    rows = jnp.concatenate([rows] * 8, 0).astype(BF16)
    for i in range(out_ref.shape[0] // rows.shape[0]):
        out_ref[i * rows.shape[0] : (i + 1) * rows.shape[0]] = rows


def split(x):
    high = x.astype(BF16).astype(F32)
    mid = (x - high).astype(BF16).astype(F32)
    low = (x - high - mid).astype(BF16).astype(F32)
    return high, mid, low


TARGET_PARTS = (0, 0, 1, 0, 2, 1)
SOURCE_PARTS = (0, 1, 0, 2, 0, 1)


def target_rows(tile):
    row = iota(tile.shape, 0)
    x = jnp.where(row < 3, tile, 0.0)
    f = jnp.where(row < 3, pltpu.roll(tile, 5, 0), 0.0)
    norm = jnp.sum(x * x, axis=0, keepdims=True) + BLOB
    cross = jnp.sum(x * f, axis=0, keepdims=True)
    parts, norms, crosses = split(tile), split(norm), split(cross)
    out = []
    for q in range(6):
        extra = norms[q] if q < 3 else crosses[q - 3]
        out.append(jnp.where(row < 6, parts[TARGET_PARTS[q]], jnp.where(row == 6, extra, 1.0 if q < 3 else 0.0)))
    return jnp.concatenate(out, 0)


def source_rows(tile):
    row = iota(tile.shape, 0)
    first, second = row < 3, (row >= 3) & (row < 6)
    x = jnp.where(first, tile, 0.0)
    f = jnp.where(first, pltpu.roll(tile, 5, 0), 0.0)
    norms = split(jnp.sum(x * x, axis=0, keepdims=True))
    crosses = split(-3.0 * jnp.sum(x * f, axis=0, keepdims=True))
    parts = split(tile)
    low = split(pltpu.roll(tile, 3, 0))
    triple = split(3.0 * f)
    rho, ab, ar, br = [], [], [], []
    for q in range(6):
        k = SOURCE_PARTS[q]
        main = jnp.where(first, -2.0 * parts[k], 0.0)
        if q < 3:
            main = jnp.where(row == 6, 1.0, jnp.where(row == 7, norms[q], main))
        rho.append(main)
        ab.append(jnp.where(second, parts[k], 0.0))
        ar.append(jnp.where(second, -low[k], jnp.where(row == 6, 0.0 if q < 3 else 1.0, 0.0)))
        br.append(jnp.where(first, triple[k], jnp.where(row == 7, crosses[q], 0.0) if q < 3 else 0.0))
    return [jnp.concatenate(rows, 0).astype(BF16) for rows in (rho, ab, ar, br)]


def middle_body(own_ref, left_ref, right_ref, count_hbm, slot_hbm, class_hbm, req_hbm, table_hbm, near_ref, slot_ref, req_ref, kind_ref, kept_ref, table, count_ref, class_ref, sems, win, lhs, rhs, acc, list_v, list_s, pairs, sem, flip):
    pairs_of = ((table_hbm, table), (count_hbm, count_ref), (slot_hbm, slot_ref), (class_hbm, class_ref), (req_hbm, req_ref))
    fetches = [pltpu.make_async_copy(a, b, sems.at[i]) for i, (a, b) in enumerate(pairs_of)]
    for fetch in fetches:
        fetch.start()
    near_terms(own_ref, left_ref, right_ref, near_ref, win, lhs, rhs, acc, list_v, list_s, pairs, sem)
    for fetch in fetches:
        fetch.wait()
    keep_rows(table, kept_ref)
    class_terms(count_ref, class_ref, kind_ref, flip)


def keep_rows(table, kept_ref):
    first = kept_ref.shape[0] - GROUP
    classes = table.shape[0]
    kept_ref[:first] = table[:first]
    whole = classes - classes % 8
    start = (classes - 1) // GROUP * GROUP
    width = 9 * LANES
    for at in range(0, table.shape[1], width):
        cols = slice(at, at + width)
        tail = table[whole:classes, cols].astype(F32)
        tail = jnp.concatenate([tail, jnp.zeros((start + GROUP - classes, width), F32)], 0)
        both = jnp.concatenate([table[start:whole, cols].astype(F32), tail], 0)
        kept_ref[first:, cols] = both.astype(BF16)


def near_terms(own_ref, left_ref, right_ref, near_ref, win, lhs, rhs, acc, list_v, list_s, pairs, sem):
    leaf_num = acc.shape[0] - 1
    nodes = leaf_num * LANES
    slots = list_v.shape[1]
    device = lax.axis_index("patch")
    halo = (left_ref, own_ref, right_ref)
    leaf_of = iota((slots, LANES), 1)
    for place, ref in enumerate(halo):
        listed = ref[:, nodes:].astype(jnp.int32)
        source = listed - (device * leaf_num + 1)
        mine = (listed > 0) & (source >= 0) & (source < leaf_num)
        list_v[place] = jnp.where(mine, (source << 6) + (leaf_of + place * leaf_num), -1)
        if place == 1:
            list_v[3] = jnp.where(listed > 0, (leaf_of << 6) + (source + leaf_num), -1)
    copy = pltpu.make_async_copy(list_v, list_s, sem)
    copy.start()

    def clear(leaf, _):
        acc[leaf] = jnp.zeros(acc.shape[1:], F32)
        return 0

    lax.fori_loop(0, leaf_num, clear, 0)
    lhs[leaf_num] = jnp.zeros(lhs.shape[1:], BF16)
    copy.wait()
    dead, seen = jnp.int32(0), 0
    for leaf in range(leaf_num):
        for place, ref in enumerate(halo):
            tile = ref[:, leaf * LANES : (leaf + 1) * LANES]
            win[place * leaf_num + leaf] = tile
            for k, rows in enumerate(source_rows(tile)):
                rhs[place * leaf_num + leaf, :, k * LANES : (k + 1) * LANES] = rows
            if place == 1:
                rows = target_rows(tile)
                rows = jnp.concatenate([rows, jnp.zeros((LANES - rows.shape[0], LANES), F32)], 0)
                lhs[leaf] = rows.T.astype(BF16)
        for place in range(list_s.shape[0]):
            for slot in range(slots):
                code = list_s[place, slot, leaf]
                pairs[dead + seen] = code
                dead = dead + (code >> 31)
                seen = seen + 1
    count = dead + seen
    for i in range(3 * DEPTH):
        pairs[count + i] = leaf_num * 64

    def products(at, bufs, register):
        pair = pairs[at]
        left = jnp.concatenate([lhs[pair >> 6], jnp.zeros((LANES, LANES), BF16)], 1)
        for unit, buf in enumerate(bufs):
            right = rhs[pair & 63, :, unit * 2 * LANES : (unit + 1) * 2 * LANES]
            right = jnp.concatenate([right, jnp.zeros((2 * LANES - right.shape[0], 2 * LANES), BF16)], 0)
            pltpu.matmul_push_rhs(right, staging_register=register, mxu_index=unit)
            pltpu.matmul_acc_lhs(buf, left, load_staged_rhs=register)

    def add_terms(at, bufs):
        pair = pairs[at]
        target, source = pair >> 6, pair & 63
        row = [jnp.broadcast_to(win[source, k : k + 1], (8, LANES)) for k in range(6)]
        first, second = [pltpu.matmul_pop(buf) for buf in bufs]
        for part in range(LANES // 8):
            i = slice(part * 8, part * 8 + 8)
            rho_sq, ab = first[i, :LANES], first[i, LANES:]
            ar, br = second[i, :LANES], second[i, LANES:]
            inv_one = lax.rsqrt(rho_sq)
            inv_two = inv_one * inv_one
            inv_three = inv_two * inv_one
            coef = (ab + ar * br * inv_two) * inv_three
            ar = ar * inv_three
            acc[target, 0, i] += br * inv_three
            acc[target, 1, i] += coef
            for k in range(3):
                acc[target, 2 + k, i] += row[3 + k] * ar + row[k] * coef

    def run(*bufs):
        bufs = [bufs[i : i + 2] for i in range(0, 4 * DEPTH, 2)]
        for pair in bufs:
            for buf in pair:
                pltpu.matmul_pop(buf)
        for i in range(DEPTH):
            products(i, bufs[i], i % 2)

        def blocks(step, _):
            start = step * (2 * DEPTH)
            for i in range(DEPTH):
                products(start + DEPTH + i, bufs[DEPTH + i], i % 2)
            for i in range(DEPTH):
                add_terms(start + i, bufs[i])
            for i in range(DEPTH):
                products(start + 2 * DEPTH + i, bufs[i], i % 2)
            for i in range(DEPTH):
                add_terms(start + DEPTH + i, bufs[DEPTH + i])
            return 0

        lax.fori_loop(0, (count + 2 * DEPTH - 1) // (2 * DEPTH), blocks, 0)
        for pair in bufs[:DEPTH]:
            for buf in pair:
                pltpu.matmul_pop(buf)

    pl.run_scoped(run, *[pltpu.ACC(i % 2)((LANES, 2 * LANES), F32) for i in range(4 * DEPTH)])
    lane = iota((LANES, LANES), 1)
    for leaf in range(leaf_num):
        flat = jnp.zeros((LANES, LANES), F32)
        for k in range(5):
            flat = jnp.where(lane == k, jnp.sum(acc[leaf, k], axis=1, keepdims=True), flat)
        flat = flat.T
        tile = win[leaf_num + leaf]
        total = flat[0:1] * tile[3:6] * (1.0 / 3.0) + flat[2:5] - flat[1:2] * tile[0:3]
        near_ref[:, leaf * LANES : (leaf + 1) * LANES] = total * KERNEL


def columns(scratch, value):
    rows, width = value.shape
    scratch[0:rows, 0:width] = value.astype(F32)
    return scratch[...].T


def class_terms(count_ref, class_ref, kind_ref, scratch):
    leaf_num, far_num = class_ref.shape
    scratch[...] = jnp.zeros((LANES, LANES), F32)
    classes = columns(scratch, class_ref[...])
    lane = iota((far_num, LANES), 1)
    row = iota((far_num, LANES), 0)
    for leaf in range(leaf_num):
        at = slice(leaf * far_num, (leaf + 1) * far_num)
        kind = jnp.broadcast_to(classes[:far_num, leaf : leaf + 1], (far_num, LANES)).astype(jnp.int32)
        keep = (lane % leaf_num == leaf) & (row < count_ref[leaf])
        kind_ref[at] = jnp.where(keep, kind - lane // leaf_num, -LANES).astype(BF16)


def slot_terms(rows, slot_ref, req_ref, main_ref, tail_ref, code_ref, scratch):
    leaf_num, far_num = slot_ref.shape
    cap, peers = req_ref.shape
    reps = LANES // leaf_num
    half = peers // 2
    scratch[...] = jnp.zeros((LANES, LANES), F32)
    asked = columns(scratch, req_ref[...])
    asked = jnp.concatenate([jnp.broadcast_to(asked[:, t : t + 1], (peers, LANES)) for t in range(cap)], 0)
    asked = asked.astype(BF16)
    slots = columns(scratch, slot_ref[...])
    slot = jnp.concatenate([jnp.broadcast_to(slots[:far_num, i : i + 1], (far_num, LANES)) for i in range(leaf_num)], 0)
    slot = slot.astype(jnp.int32)
    lane = iota(slot.shape, 1)
    peer = slot // cap
    key = (slot - peer * cap) * peers + peer - lane
    picks = [jnp.where(key == t * peers, 1.0, 0.0).astype(BF16) for t in range(cap)]
    local = jnp.dot(jnp.concatenate(picks, 1), asked, preferred_element_type=F32).astype(jnp.int32)
    upper = (peer >= half).astype(jnp.int32)
    base = (peer - upper * half) * rows

    def code(row):
        return jnp.where(lane == row % LANES, row // LANES, -1).astype(BF16)

    main_ref[...] = code(base + local)
    tail_ref[...] = code(base + leaf_num + local // reps)
    code_ref[...] = (upper + 2 * (lane // leaf_num == local % reps).astype(jnp.int32)).astype(BF16)


def far_body(mom_ref, slot_ref, req_ref, kind_ref, kept_ref, own_ref, near_ref, table_hbm, down_hbm, out_ref, main_ref, tail_ref, code_ref, flip, table, down, pad, sums, sem):
    early = kept_ref.shape[0] - GROUP
    fetch = pltpu.make_async_copy(table_hbm.at[pl.ds(early, table.shape[0])], table, sem.at[0])
    fetch_down = pltpu.make_async_copy(down_hbm, down, sem.at[1])
    fetch.start()
    fetch_down.start()
    leaf_num, quads, width, _ = down.shape
    groups = pad.shape[0]
    lead = 2 * LANES - width
    cols = GROUP * leaf_num

    @pl.when(lax.axis_index("patch") >= 0)
    def _():
        slot_terms(mom_ref.shape[0] // (req_ref.shape[1]), slot_ref, req_ref, main_ref, tail_ref, code_ref, flip)
        half = mom_ref.shape[0] // 2
        both = jnp.concatenate([mom_ref[:half], mom_ref[half:]], 1)
        one, zero = jnp.ones((), BF16), jnp.zeros((), BF16)

        def hots(ref, count, stride=1):
            codes = ref[...]
            return [jnp.where(codes == i * stride, one, zero) for i in range(count)]

        tiles = half // LANES
        main = jnp.dot(jnp.concatenate(hots(main_ref, tiles), 1), both, preferred_element_type=F32)
        tails = jnp.dot(jnp.concatenate(hots(tail_ref, tiles), 1), both, preferred_element_type=F32)
        code = code_ref[...].astype(F32)
        upper = (code == 1.0) | (code == 3.0)
        main = jnp.where(upper, main[:, LANES:], main[:, :LANES]).T
        tails = jnp.where(upper, tails[:, LANES:], tails[:, :LANES])
        tails = jnp.where(code >= 2, tails, 0.0).T
        extra = width - LANES
        tails = sum(tails[i * extra : (i + 1) * extra] for i in range(LANES // extra))
        src_t = jnp.concatenate([main, tails], 0).astype(BF16)
        per = cols // LANES
        hot = hots(kind_ref, groups * per, LANES // leaf_num)
        for g in range(groups):
            pad[g, 0:lead] = jnp.zeros((lead, cols), BF16)
            pad[g, lead + width :] = jnp.zeros((pad.shape[1] - lead - width, cols), BF16)
            part = jnp.dot(src_t, jnp.concatenate(hot[g * per : (g + 1) * per], 1), preferred_element_type=F32)
            pad[g, lead : lead + width] = part.astype(BF16)

    fetch.wait()
    step = width - LANES
    period = LANES // step
    tiles = period + 1
    blocks = width // period
    same = iota((blocks, GROUP, cols), 2) // leaf_num == iota((blocks, GROUP, cols), 1)
    for r in range(period):
        acc = None
        for g in range(groups):
            if g == groups - 1:
                ref, first = kept_ref, early
            elif g * GROUP < early:
                ref, first = kept_ref, g * GROUP
            else:
                ref, first = table, g * GROUP - early
            rows = [ref[first : first + GROUP, (tiles * b + r) * LANES : (tiles * b + r + 2) * LANES] for b in range(blocks)]
            part = jnp.dot(jnp.concatenate(rows, 0), pad[g, lead - step * r : lead - step * r + 2 * LANES], preferred_element_type=F32)
            acc = part if acc is None else acc + part
        acc = jnp.where(same, acc.reshape(blocks, GROUP, cols), 0.0)
        acc = jnp.sum(acc, axis=1)
        for h in range(cols // LANES):
            sums[h, pl.ds(r, blocks, stride=period), :] = acc[:, h * LANES : (h + 1) * LANES]
    fold = jnp.where(iota((leaf_num, cols), 1) % leaf_num == iota((leaf_num, cols), 0), 1.0, 0.0)
    whole = jnp.concatenate([sums[h] for h in range(cols // LANES)], 1)
    expansion = lax.dot_general(fold, whole, (((1,), (1,)), ((), ())), precision=lax.Precision.HIGHEST, preferred_element_type=F32)
    fetch_down.wait()
    which = iota((leaf_num, width), 0)
    field = [None] * quads
    for leaf in range(leaf_num):
        lhs = jnp.where(which == leaf, expansion, 0.0).astype(BF16)
        for q in range(0, quads, 2):
            both = [down[leaf, i] for i in range(q, min(q + 2, quads))]
            part = jnp.dot(lhs, jnp.concatenate(both, 1), preferred_element_type=F32)
            field[q] = part if field[q] is None else field[q] + part
    quad = [field[q - q % 2][:, (q % 2) * LANES : (q % 2 + 1) * LANES] for q in range(quads)]
    for leaf in range(leaf_num):
        at = slice(leaf * LANES, (leaf + 1) * LANES)
        far = []
        for k in range(3):
            far.append(sum(own_ref[3 + c : 4 + c, at] * quad[3 * c + k][leaf : leaf + 1] for c in range(3)))
        out_ref[:, at] = near_ref[:, at] + jnp.concatenate(far, 0)


SMEM = pl.BlockSpec(memory_space=pltpu.SMEM)
VMEM = pl.BlockSpec(memory_space=pltpu.VMEM)
HBM = pl.BlockSpec(memory_space=pltpu.HBM)


def held(x, space=pltpu.VMEM):
    return pltpu.with_memory_space_constraint(x, space)


def call(body, outs, limit, **options):
    if outs is not None:
        shapes = tuple(pltpu.VMEM(o[:-1], o[-1]) for o in outs)
        options["out_shape"] = shapes if len(shapes) > 1 else shapes[0]
    params = pltpu.CompilerParams(vmem_limit_bytes=limit * 2**20)
    return pl.pallas_call(body, compiler_params=params, **options)


def per_device(positions, densities, near_src, near_count, far_slot, far_class, far_count, requests, up_basis, transfer_table, down_basis):
    leaf_num, slot_num = near_src.shape
    nodes = positions.shape[1]
    width = up_basis.shape[1]
    far_num = far_slot.shape[1]
    peers = requests.shape[1]
    classes = transfer_table.shape[0]
    groups = -(-classes // GROUP)
    rows = leaf_num * width // LANES
    up = [(i, i + 1) for i in range(peers - 1)]
    down = [(j, i) for i, j in up]
    slots = leaf_num * far_num
    own, message = call(
        front_body,
        [(8, nodes + LANES, F32), (peers * rows, LANES, BF16)],
        8,
        in_specs=[HBM] * 5,
        scratch_shapes=[
            pltpu.VMEM((3, nodes), F32),
            pltpu.VMEM((3, nodes), F32),
            pltpu.VMEM((slot_num, leaf_num), jnp.int32),
            pltpu.VMEM((1, leaf_num), jnp.int32),
            pltpu.VMEM(up_basis.shape, BF16),
            pltpu.SemaphoreType.DMA((5,)),
        ],
    )(*[held(x, pltpu.HBM) for x in (positions, densities, near_src.T, near_count[None], up_basis)])
    left = lax.ppermute(own, "patch", up)
    right = lax.ppermute(own, "patch", down)
    message = message.reshape(peers, rows // 2, 2, LANES)
    table = lax.all_to_all(message, "patch", split_axis=0, concat_axis=0, tiled=True)
    table = table.reshape(peers * rows, LANES)
    down_flat = down_basis.transpose(0, 2, 1, 3)
    near, *kept = call(
        middle_body,
        [
            (3, nodes, F32),
            far_slot.shape + (jnp.int32,),
            (requests.shape[2], peers, jnp.int32),
            (slots, LANES, BF16),
            ((EARLY + 1) * GROUP, width * width, BF16),
        ],
        36,
        in_specs=[VMEM] * 3 + [HBM] * 5,
        scratch_shapes=[
            pltpu.VMEM(transfer_table.shape, BF16),
            pltpu.SMEM(far_count.shape, jnp.int32),
            pltpu.VMEM(far_class.shape, jnp.int32),
            pltpu.SemaphoreType.DMA((5,)),
            pltpu.VMEM((3 * leaf_num, 8, LANES), F32),
            pltpu.VMEM((leaf_num + 1, LANES, LANES), BF16),
            pltpu.VMEM((3 * leaf_num, 48, 4 * LANES), BF16),
            pltpu.VMEM((leaf_num + 1, 5, LANES, LANES), F32),
            pltpu.VMEM((4, slot_num, LANES), jnp.int32),
            pltpu.SMEM((4, slot_num, LANES), jnp.int32),
            pltpu.SMEM((4 * leaf_num * slot_num + 3 * DEPTH,), jnp.int32),
            pltpu.SemaphoreType.DMA,
            pltpu.VMEM((LANES, LANES), F32),
        ],
    )(held(own), held(left), held(right), *[held(x, pltpu.HBM) for x in (far_count, far_slot, far_class, requests[0].T, transfer_table)])
    return call(
        far_body,
        None,
        30,
        in_specs=[VMEM] * 7 + [HBM] * 2,
        out_shape=jax.ShapeDtypeStruct((3, nodes), F32),
        scratch_shapes=[
            pltpu.VMEM((slots, LANES), BF16),
            pltpu.VMEM((slots, LANES), BF16),
            pltpu.VMEM((slots, LANES), BF16),
            pltpu.VMEM((LANES, LANES), F32),
            pltpu.VMEM(((groups - 1 - EARLY) * GROUP, width * width), BF16),
            pltpu.VMEM(down_flat.shape, BF16),
            pltpu.VMEM((groups, 4 * LANES - width, GROUP * leaf_num), BF16),
            pltpu.VMEM((GROUP * leaf_num // LANES, width, LANES), F32),
            pltpu.SemaphoreType.DMA((2,)),
        ],
    )(*[held(x) for x in (table, *kept, own, near)], held(transfer_table, pltpu.HBM), held(down_flat, pltpu.HBM))


def solution(mesh):
    placed = (
        P(None, "patch"),
        P(None, "patch"),
        P("patch", None),
        P("patch"),
        P("patch", None),
        P("patch", None),
        P("patch"),
        P("patch", None, None),
        P("patch", None, None),
        P(),
        P("patch", None, None, None),
    )
    return jax.shard_map(per_device, mesh=mesh, in_specs=placed, out_specs=P(None, "patch"), check_vma=False)
```

```python
import math

import jax
import jax.numpy as jnp
from jax import lax
from jax.experimental import pallas as pl
from jax.experimental.pallas import tpu as pltpu
from jax.sharding import PartitionSpec as P


KERNEL = 1.0 / (8.0 * math.pi)
BLOB = 0.25
LANES = 128
DEPTH = 3
EARLY = 2
GROUP = 16
F32 = jnp.float32
BF16 = jnp.bfloat16


def iota(shape, dim):
    return lax.broadcasted_iota(jnp.int32, shape, dim)


def quotient(x, n):
    return x >> (n.bit_length() - 1) if n & (n - 1) == 0 else x // n


def remainder(x, n):
    return x & (n - 1) if n & (n - 1) == 0 else x % n


def front_body(pos_hbm, dens_hbm, src_hbm, count_hbm, up_hbm, own_ref, out_ref, pos_ref, dens_ref, src_ref, count_ref, up_ref, sem):
    refs = [(pos_hbm, pos_ref), (dens_hbm, dens_ref), (src_hbm, src_ref), (count_hbm, count_ref)]
    refs += [(up_hbm.at[pl.ds(i, 4)], up_ref.at[pl.ds(i, 4)]) for i in range(0, up_ref.shape[0], 4)]
    copies = [pltpu.make_async_copy(a, b, sem.at[i]) for i, (a, b) in enumerate(refs)]
    for copy in copies:
        copy.start()
    leaf_num, width, _ = up_ref.shape
    nodes = pos_ref.shape[1]
    slots = src_ref.shape[0]
    own_ref[6:, :nodes] = jnp.zeros((2, nodes), F32)
    own_ref[:, nodes:] = jnp.zeros((slots, LANES), F32)
    for copy in copies[:4]:
        copy.wait()
    own_ref[0:3, :nodes] = pos_ref[...]
    own_ref[3:6, :nodes] = dens_ref[...]
    live = iota((slots, leaf_num), 0) < count_ref[...]
    own_ref[:, nodes : nodes + leaf_num] = jnp.where(live, src_ref[...] + 1, 0).astype(F32)
    lane = iota((width, LANES), 1)
    cols = jnp.zeros((width, LANES), F32)
    for leaf in range(leaf_num):
        if leaf % 4 == 0:
            copies[4 + leaf // 4].wait()
        total = None
        for comp in range(3):
            row = dens_ref[comp : comp + 1, leaf * LANES : (leaf + 1) * LANES]
            row = row.astype(BF16).astype(F32)
            part = up_ref[leaf, :, comp * LANES : (comp + 1) * LANES].astype(F32) * row
            total = part if total is None else total + part
        cols = jnp.where(lane == leaf, jnp.sum(total, axis=1, keepdims=True), cols)
    step = width - LANES
    reps = LANES // step
    tails = jnp.concatenate([cols[LANES:]] * reps, 0).T[:leaf_num]
    tails = jnp.where(iota(tails.shape, 1) // step == iota(tails.shape, 0) % reps, tails, 0.0)
    tails = [jnp.sum(tails[i : i + reps], axis=0, keepdims=True) for i in range(0, leaf_num, reps)]
    rows = jnp.concatenate([cols[:LANES].T[:leaf_num]] + tails, 0)
    rows = jnp.concatenate([rows] * 8, 0).astype(BF16)
    for i in range(out_ref.shape[0] // rows.shape[0]):
        out_ref[i * rows.shape[0] : (i + 1) * rows.shape[0]] = rows


def split(x):
    high = x.astype(BF16).astype(F32)
    mid = (x - high).astype(BF16).astype(F32)
    low = (x - high - mid).astype(BF16).astype(F32)
    return high, mid, low


TARGET_PARTS = (0, 0, 1, 0, 2, 1)
SOURCE_PARTS = (0, 1, 0, 2, 0, 1)


def target_rows(tile):
    row = iota(tile.shape, 0)
    x = jnp.where(row < 3, tile, 0.0)
    f = jnp.where(row < 3, pltpu.roll(tile, 5, 0), 0.0)
    norm = jnp.sum(x * x, axis=0, keepdims=True) + BLOB
    cross = jnp.sum(x * f, axis=0, keepdims=True)
    parts, norms, crosses = split(tile), split(norm), split(cross)
    out = []
    for q in range(6):
        extra = norms[q] if q < 3 else crosses[q - 3]
        out.append(jnp.where(row < 6, parts[TARGET_PARTS[q]], jnp.where(row == 6, extra, 1.0 if q < 3 else 0.0)))
    return jnp.concatenate(out, 0)


def source_rows(tile):
    row = iota(tile.shape, 0)
    first, second = row < 3, (row >= 3) & (row < 6)
    x = jnp.where(first, tile, 0.0)
    f = jnp.where(first, pltpu.roll(tile, 5, 0), 0.0)
    norms = split(jnp.sum(x * x, axis=0, keepdims=True))
    crosses = split(-3.0 * jnp.sum(x * f, axis=0, keepdims=True))
    parts = split(tile)
    low = split(pltpu.roll(tile, 3, 0))
    triple = split(3.0 * f)
    rho, ab, ar, br = [], [], [], []
    for q in range(6):
        k = SOURCE_PARTS[q]
        main = jnp.where(first, -2.0 * parts[k], 0.0)
        if q < 3:
            main = jnp.where(row == 6, 1.0, jnp.where(row == 7, norms[q], main))
        rho.append(main)
        ab.append(jnp.where(second, parts[k], 0.0))
        ar.append(jnp.where(second, -low[k], jnp.where(row == 6, 0.0 if q < 3 else 1.0, 0.0)))
        br.append(jnp.where(first, triple[k], jnp.where(row == 7, crosses[q], 0.0) if q < 3 else 0.0))
    return [jnp.concatenate(rows, 0).astype(BF16) for rows in (rho, ab, ar, br)]


def middle_body(own_ref, left_ref, right_ref, count_hbm, slot_hbm, class_hbm, req_hbm, table_hbm, near_ref, slot_ref, req_ref, kind_ref, kept_ref, table, count_ref, class_ref, sems, win, lhs, rhs, acc, list_v, list_s, pairs, sem, flip):
    pairs_of = ((table_hbm, table), (count_hbm, count_ref), (slot_hbm, slot_ref), (class_hbm, class_ref), (req_hbm, req_ref))
    fetches = [pltpu.make_async_copy(a, b, sems.at[i]) for i, (a, b) in enumerate(pairs_of)]
    for fetch in fetches:
        fetch.start()
    near_terms(own_ref, left_ref, right_ref, near_ref, win, lhs, rhs, acc, list_v, list_s, pairs, sem)
    for fetch in fetches:
        fetch.wait()
    keep_rows(table, kept_ref)
    class_terms(count_ref, class_ref, kind_ref, flip)


def keep_rows(table, kept_ref):
    first = kept_ref.shape[0] - GROUP
    classes = table.shape[0]
    kept_ref[:first] = table[:first]
    whole = classes - classes % 8
    start = (classes - 1) // GROUP * GROUP
    width = 9 * LANES
    for at in range(0, table.shape[1], width):
        cols = slice(at, at + width)
        tail = table[whole:classes, cols].astype(F32)
        tail = jnp.concatenate([tail, jnp.zeros((start + GROUP - classes, width), F32)], 0)
        both = jnp.concatenate([table[start:whole, cols].astype(F32), tail], 0)
        kept_ref[first:, cols] = both.astype(BF16)


def near_terms(own_ref, left_ref, right_ref, near_ref, win, lhs, rhs, acc, list_v, list_s, pairs, sem):
    leaf_num = acc.shape[0] - 1
    nodes = leaf_num * LANES
    slots = list_v.shape[1]
    device = lax.axis_index("patch")
    halo = (left_ref, own_ref, right_ref)
    leaf_of = iota((slots, LANES), 1)
    for place, ref in enumerate(halo):
        listed = ref[:, nodes:].astype(jnp.int32)
        source = listed - (device * leaf_num + 1)
        mine = (listed > 0) & (source >= 0) & (source < leaf_num)
        list_v[place] = jnp.where(mine, (source << 6) + (leaf_of + place * leaf_num), -1)
        if place == 1:
            list_v[3] = jnp.where(listed > 0, (leaf_of << 6) + (source + leaf_num), -1)
    copy = pltpu.make_async_copy(list_v, list_s, sem)
    copy.start()

    def clear(leaf, _):
        acc[leaf] = jnp.zeros(acc.shape[1:], F32)
        return 0

    lax.fori_loop(0, leaf_num, clear, 0)
    lhs[leaf_num] = jnp.zeros(lhs.shape[1:], BF16)
    copy.wait()
    dead, seen = jnp.int32(0), 0
    for leaf in range(leaf_num):
        for place, ref in enumerate(halo):
            tile = ref[:, leaf * LANES : (leaf + 1) * LANES]
            win[place * leaf_num + leaf] = tile
            for k, rows in enumerate(source_rows(tile)):
                rhs[place * leaf_num + leaf, :, k * LANES : (k + 1) * LANES] = rows
            if place == 1:
                rows = target_rows(tile)
                rows = jnp.concatenate([rows, jnp.zeros((LANES - rows.shape[0], LANES), F32)], 0)
                lhs[leaf] = rows.T.astype(BF16)
        for place in range(list_s.shape[0]):
            for slot in range(slots):
                code = list_s[place, slot, leaf]
                pairs[dead + seen] = code
                dead = dead + (code >> 31)
                seen = seen + 1
    count = dead + seen
    for i in range(3 * DEPTH):
        pairs[count + i] = leaf_num * 64

    def products(at, bufs, register):
        pair = pairs[at]
        left = jnp.concatenate([lhs[pair >> 6], jnp.zeros((LANES, LANES), BF16)], 1)
        for unit, buf in enumerate(bufs):
            right = rhs[pair & 63, :, unit * 2 * LANES : (unit + 1) * 2 * LANES]
            right = jnp.concatenate([right, jnp.zeros((2 * LANES - right.shape[0], 2 * LANES), BF16)], 0)
            pltpu.matmul_push_rhs(right, staging_register=register, mxu_index=unit)
            pltpu.matmul_acc_lhs(buf, left, load_staged_rhs=register)

    def add_terms(at, bufs):
        pair = pairs[at]
        target, source = pair >> 6, pair & 63
        row = [jnp.broadcast_to(win[source, k : k + 1], (8, LANES)) for k in range(6)]
        first, second = [pltpu.matmul_pop(buf) for buf in bufs]
        for part in range(LANES // 8):
            i = slice(part * 8, part * 8 + 8)
            rho_sq, ab = first[i, :LANES], first[i, LANES:]
            ar, br = second[i, :LANES], second[i, LANES:]
            inv_one = lax.rsqrt(rho_sq)
            inv_two = inv_one * inv_one
            inv_three = inv_two * inv_one
            coef = (ab + ar * br * inv_two) * inv_three
            ar = ar * inv_three
            acc[target, 0, i] += br * inv_three
            acc[target, 1, i] += coef
            for k in range(3):
                acc[target, 2 + k, i] += row[3 + k] * ar + row[k] * coef

    def run(*bufs):
        bufs = [bufs[i : i + 2] for i in range(0, 4 * DEPTH, 2)]
        for pair in bufs:
            for buf in pair:
                pltpu.matmul_pop(buf)
        for i in range(DEPTH):
            products(i, bufs[i], i % 2)

        def blocks(step, _):
            start = step * (2 * DEPTH)
            for i in range(DEPTH):
                products(start + DEPTH + i, bufs[DEPTH + i], i % 2)
            for i in range(DEPTH):
                add_terms(start + i, bufs[i])
            for i in range(DEPTH):
                products(start + 2 * DEPTH + i, bufs[i], i % 2)
            for i in range(DEPTH):
                add_terms(start + DEPTH + i, bufs[DEPTH + i])
            return 0

        lax.fori_loop(0, (count + 2 * DEPTH - 1) // (2 * DEPTH), blocks, 0)
        for pair in bufs[:DEPTH]:
            for buf in pair:
                pltpu.matmul_pop(buf)

    pl.run_scoped(run, *[pltpu.ACC(i % 2)((LANES, 2 * LANES), F32) for i in range(4 * DEPTH)])
    lane = iota((LANES, LANES), 1)
    for leaf in range(leaf_num):
        flat = jnp.zeros((LANES, LANES), F32)
        for k in range(5):
            flat = jnp.where(lane == k, jnp.sum(acc[leaf, k], axis=1, keepdims=True), flat)
        flat = flat.T
        tile = win[leaf_num + leaf]
        total = flat[0:1] * tile[3:6] * (1.0 / 3.0) + flat[2:5] - flat[1:2] * tile[0:3]
        near_ref[:, leaf * LANES : (leaf + 1) * LANES] = total * KERNEL


def columns(scratch, value):
    rows, width = value.shape
    scratch[0:rows, 0:width] = value.astype(F32)
    return scratch[...].T


def class_terms(count_ref, class_ref, kind_ref, scratch):
    leaf_num, far_num = class_ref.shape
    scratch[...] = jnp.zeros((LANES, LANES), F32)
    classes = columns(scratch, class_ref[...])
    lane = iota((far_num, LANES), 1)
    row = iota((far_num, LANES), 0)
    for leaf in range(leaf_num):
        at = slice(leaf * far_num, (leaf + 1) * far_num)
        kind = jnp.broadcast_to(classes[:far_num, leaf : leaf + 1], (far_num, LANES)).astype(jnp.int32)
        keep = (remainder(lane, leaf_num) == leaf) & (row < count_ref[leaf])
        kind_ref[at] = jnp.where(keep, kind - quotient(lane, leaf_num), -LANES).astype(BF16)


def slot_terms(rows, slot_ref, req_ref, main_ref, tail_ref, code_ref, scratch):
    leaf_num, far_num = slot_ref.shape
    cap, peers = req_ref.shape
    reps = LANES // leaf_num
    half = peers // 2
    scratch[...] = jnp.zeros((LANES, LANES), F32)
    asked = columns(scratch, req_ref[...])
    asked = jnp.concatenate([jnp.broadcast_to(asked[:, t : t + 1], (peers, LANES)) for t in range(cap)], 0)
    asked = asked.astype(BF16)
    slots = columns(scratch, slot_ref[...])
    slot = jnp.concatenate([jnp.broadcast_to(slots[:far_num, i : i + 1], (far_num, LANES)) for i in range(leaf_num)], 0)
    slot = slot.astype(jnp.int32)
    lane = iota(slot.shape, 1)
    peer = quotient(slot, cap)
    key = (slot - peer * cap) * peers + peer - lane
    picks = [jnp.where(key == t * peers, 1.0, 0.0).astype(BF16) for t in range(cap)]
    local = jnp.dot(jnp.concatenate(picks, 1), asked, preferred_element_type=F32).astype(jnp.int32)
    upper = (peer >= half).astype(jnp.int32)
    base = (peer - upper * half) * rows

    def code(row):
        return jnp.where(lane == remainder(row, LANES), quotient(row, LANES), -1).astype(BF16)

    main_ref[...] = code(base + local)
    tail_ref[...] = code(base + leaf_num + quotient(local, reps))
    code_ref[...] = (upper + 2 * (quotient(lane, leaf_num) == remainder(local, reps)).astype(jnp.int32)).astype(BF16)


def far_body(mom_ref, slot_ref, req_ref, kind_ref, kept_ref, own_ref, near_ref, table_hbm, down_hbm, out_ref, main_ref, tail_ref, code_ref, flip, table, down, pad, sums, sem):
    early = kept_ref.shape[0] - GROUP
    fetch = pltpu.make_async_copy(table_hbm.at[pl.ds(early, table.shape[0])], table, sem.at[0])
    fetch_down = pltpu.make_async_copy(down_hbm, down, sem.at[1])
    fetch.start()
    fetch_down.start()
    leaf_num, quads, width, _ = down.shape
    groups = pad.shape[0]
    lead = 2 * LANES - width
    cols = GROUP * leaf_num

    @pl.when(lax.axis_index("patch") >= 0)
    def _():
        slot_terms(mom_ref.shape[0] // (req_ref.shape[1]), slot_ref, req_ref, main_ref, tail_ref, code_ref, flip)
        half = mom_ref.shape[0] // 2
        both = jnp.concatenate([mom_ref[:half], mom_ref[half:]], 1)
        one, zero = jnp.ones((), BF16), jnp.zeros((), BF16)

        def hots(ref, count, stride=1):
            codes = ref[...]
            return [jnp.where(codes == i * stride, one, zero) for i in range(count)]

        tiles = half // LANES
        main = jnp.dot(jnp.concatenate(hots(main_ref, tiles), 1), both, preferred_element_type=F32)
        tails = jnp.dot(jnp.concatenate(hots(tail_ref, tiles), 1), both, preferred_element_type=F32)
        code = code_ref[...].astype(F32)
        upper = (code == 1.0) | (code == 3.0)
        main = jnp.where(upper, main[:, LANES:], main[:, :LANES]).T
        tails = jnp.where(upper, tails[:, LANES:], tails[:, :LANES])
        tails = jnp.where(code >= 2, tails, 0.0).T
        extra = width - LANES
        tails = sum(tails[i * extra : (i + 1) * extra] for i in range(LANES // extra))
        src_t = jnp.concatenate([main, tails], 0).astype(BF16)
        per = cols // LANES
        hot = hots(kind_ref, groups * per, LANES // leaf_num)
        for g in range(groups):
            pad[g, 0:lead] = jnp.zeros((lead, cols), BF16)
            pad[g, lead + width :] = jnp.zeros((pad.shape[1] - lead - width, cols), BF16)
            part = jnp.dot(src_t, jnp.concatenate(hot[g * per : (g + 1) * per], 1), preferred_element_type=F32)
            pad[g, lead : lead + width] = part.astype(BF16)

    fetch.wait()
    step = width - LANES
    period = LANES // step
    tiles = period + 1
    blocks = width // period
    same = quotient(iota((blocks, GROUP, cols), 2), leaf_num) == iota((blocks, GROUP, cols), 1)
    for r in range(period):
        acc = None
        for g in range(groups):
            if g == groups - 1:
                ref, first = kept_ref, early
            elif g * GROUP < early:
                ref, first = kept_ref, g * GROUP
            else:
                ref, first = table, g * GROUP - early
            rows = [ref[first : first + GROUP, (tiles * b + r) * LANES : (tiles * b + r + 2) * LANES] for b in range(blocks)]
            part = jnp.dot(jnp.concatenate(rows, 0), pad[g, lead - step * r : lead - step * r + 2 * LANES], preferred_element_type=F32)
            acc = part if acc is None else acc + part
        acc = jnp.where(same, acc.reshape(blocks, GROUP, cols), 0.0)
        acc = jnp.sum(acc, axis=1)
        for h in range(cols // LANES):
            sums[h, pl.ds(r, blocks, stride=period), :] = acc[:, h * LANES : (h + 1) * LANES]
    fold = jnp.where(remainder(iota((leaf_num, cols), 1), leaf_num) == iota((leaf_num, cols), 0), 1.0, 0.0)
    whole = jnp.concatenate([sums[h] for h in range(cols // LANES)], 1)
    expansion = lax.dot_general(fold, whole, (((1,), (1,)), ((), ())), precision=lax.Precision.HIGHEST, preferred_element_type=F32)
    fetch_down.wait()
    which = iota((leaf_num, width), 0)
    field = [None] * quads
    for leaf in range(leaf_num):
        lhs = jnp.where(which == leaf, expansion, 0.0).astype(BF16)
        for q in range(0, quads, 2):
            both = [down[leaf, i] for i in range(q, min(q + 2, quads))]
            part = jnp.dot(lhs, jnp.concatenate(both, 1), preferred_element_type=F32)
            field[q] = part if field[q] is None else field[q] + part
    quad = [field[q - q % 2][:, (q % 2) * LANES : (q % 2 + 1) * LANES] for q in range(quads)]
    for leaf in range(leaf_num):
        at = slice(leaf * LANES, (leaf + 1) * LANES)
        far = []
        for k in range(3):
            far.append(sum(own_ref[3 + c : 4 + c, at] * quad[3 * c + k][leaf : leaf + 1] for c in range(3)))
        out_ref[:, at] = near_ref[:, at] + jnp.concatenate(far, 0)


SMEM = pl.BlockSpec(memory_space=pltpu.SMEM)
VMEM = pl.BlockSpec(memory_space=pltpu.VMEM)
HBM = pl.BlockSpec(memory_space=pltpu.HBM)


def held(x, space=pltpu.VMEM):
    return pltpu.with_memory_space_constraint(x, space)


def call(body, outs, limit, **options):
    if outs is not None:
        shapes = tuple(pltpu.VMEM(o[:-1], o[-1]) for o in outs)
        options["out_shape"] = shapes if len(shapes) > 1 else shapes[0]
    params = pltpu.CompilerParams(vmem_limit_bytes=limit * 2**20)
    return pl.pallas_call(body, compiler_params=params, **options)


def per_device(positions, densities, near_src, near_count, far_slot, far_class, far_count, requests, up_basis, transfer_table, down_basis):
    leaf_num, slot_num = near_src.shape
    nodes = positions.shape[1]
    width = up_basis.shape[1]
    far_num = far_slot.shape[1]
    peers = requests.shape[1]
    classes = transfer_table.shape[0]
    groups = -(-classes // GROUP)
    rows = leaf_num * width // LANES
    up = [(i, (i + 1) % peers) for i in range(peers)]
    down = [(j, i) for i, j in up]
    slots = leaf_num * far_num
    own, message = call(
        front_body,
        [(8, nodes + LANES, F32), (peers * rows, LANES, BF16)],
        8,
        in_specs=[HBM] * 5,
        scratch_shapes=[
            pltpu.VMEM((3, nodes), F32),
            pltpu.VMEM((3, nodes), F32),
            pltpu.VMEM((slot_num, leaf_num), jnp.int32),
            pltpu.VMEM((1, leaf_num), jnp.int32),
            pltpu.VMEM(up_basis.shape, BF16),
            pltpu.SemaphoreType.DMA((4 + leaf_num // 4,)),
        ],
    )(*[held(x, pltpu.HBM) for x in (positions, densities, near_src.T, near_count[None], up_basis)])
    left = lax.ppermute(own, "patch", up)
    right = lax.ppermute(own, "patch", down)
    message = message.reshape(peers, rows // 2, 2, LANES)
    table = lax.all_to_all(message, "patch", split_axis=0, concat_axis=0, tiled=True)
    table = table.reshape(peers * rows, LANES)
    down_flat = down_basis.transpose(0, 2, 1, 3)
    near, *kept = call(
        middle_body,
        [
            (3, nodes, F32),
            far_slot.shape + (jnp.int32,),
            (requests.shape[2], peers, jnp.int32),
            (slots, LANES, BF16),
            ((EARLY + 1) * GROUP, width * width, BF16),
        ],
        36,
        in_specs=[VMEM] * 3 + [HBM] * 5,
        scratch_shapes=[
            pltpu.VMEM(transfer_table.shape, BF16),
            pltpu.SMEM(far_count.shape, jnp.int32),
            pltpu.VMEM(far_class.shape, jnp.int32),
            pltpu.SemaphoreType.DMA((5,)),
            pltpu.VMEM((3 * leaf_num, 8, LANES), F32),
            pltpu.VMEM((leaf_num + 1, LANES, LANES), BF16),
            pltpu.VMEM((3 * leaf_num, 48, 4 * LANES), BF16),
            pltpu.VMEM((leaf_num + 1, 5, LANES, LANES), F32),
            pltpu.VMEM((4, slot_num, LANES), jnp.int32),
            pltpu.SMEM((4, slot_num, LANES), jnp.int32),
            pltpu.SMEM((4 * leaf_num * slot_num + 3 * DEPTH,), jnp.int32),
            pltpu.SemaphoreType.DMA,
            pltpu.VMEM((LANES, LANES), F32),
        ],
    )(held(own), held(left), held(right), *[held(x, pltpu.HBM) for x in (far_count, far_slot, far_class, requests[0].T, transfer_table)])
    return call(
        far_body,
        None,
        30,
        in_specs=[VMEM] * 7 + [HBM] * 2,
        out_shape=jax.ShapeDtypeStruct((3, nodes), F32),
        scratch_shapes=[
            pltpu.VMEM((slots, LANES), BF16),
            pltpu.VMEM((slots, LANES), BF16),
            pltpu.VMEM((slots, LANES), BF16),
            pltpu.VMEM((LANES, LANES), F32),
            pltpu.VMEM(((groups - 1 - EARLY) * GROUP, width * width), BF16),
            pltpu.VMEM(down_flat.shape, BF16),
            pltpu.VMEM((groups, 4 * LANES - width, GROUP * leaf_num), BF16),
            pltpu.VMEM((GROUP * leaf_num // LANES, width, LANES), F32),
            pltpu.SemaphoreType.DMA((2,)),
        ],
    )(*[held(x) for x in (table, *kept, own, near)], held(transfer_table, pltpu.HBM), held(down_flat, pltpu.HBM))


def solution(mesh):
    placed = (
        P(None, "patch"),
        P(None, "patch"),
        P("patch", None),
        P("patch"),
        P("patch", None),
        P("patch", None),
        P("patch"),
        P("patch", None, None),
        P("patch", None, None),
        P(),
        P("patch", None, None, None),
    )
    return jax.shard_map(per_device, mesh=mesh, in_specs=placed, out_specs=P(None, "patch"), check_vma=False)
```

```python
import math

import jax
import jax.numpy as jnp
from jax import lax
from jax.experimental import pallas as pl
from jax.experimental.pallas import tpu as pltpu
from jax.sharding import PartitionSpec as P


KERNEL = 1.0 / (8.0 * math.pi)
BLOB = 0.25
LANES = 128
DEPTH = 3
EARLY = 2
GROUP = 16
F32 = jnp.float32
BF16 = jnp.bfloat16


def iota(shape, dim):
    return lax.broadcasted_iota(jnp.int32, shape, dim)


def quotient(x, n):
    return x >> (n.bit_length() - 1) if n & (n - 1) == 0 else x // n


def remainder(x, n):
    return x & (n - 1) if n & (n - 1) == 0 else x % n


def front_body(pos_hbm, dens_hbm, src_hbm, count_hbm, up_hbm, own_ref, out_ref, pos_ref, dens_ref, src_ref, count_ref, up_ref, sem):
    refs = [(pos_hbm, pos_ref), (dens_hbm, dens_ref), (src_hbm, src_ref), (count_hbm, count_ref)]
    refs += [(up_hbm.at[pl.ds(i, 4)], up_ref.at[pl.ds(i, 4)]) for i in range(0, up_ref.shape[0], 4)]
    copies = [pltpu.make_async_copy(a, b, sem.at[i]) for i, (a, b) in enumerate(refs)]
    for copy in copies:
        copy.start()
    leaf_num, width, _ = up_ref.shape
    nodes = pos_ref.shape[1]
    slots = src_ref.shape[0]
    own_ref[6:, :nodes] = jnp.zeros((2, nodes), F32)
    own_ref[:, nodes:] = jnp.zeros((slots, LANES), F32)
    for copy in copies[:4]:
        copy.wait()
    own_ref[0:3, :nodes] = pos_ref[...]
    own_ref[3:6, :nodes] = dens_ref[...]
    live = iota((slots, leaf_num), 0) < count_ref[...]
    own_ref[:, nodes : nodes + leaf_num] = jnp.where(live, src_ref[...] + 1, 0).astype(F32)
    lane = iota((width, LANES), 1)
    cols = jnp.zeros((width, LANES), F32)
    for leaf in range(leaf_num):
        if leaf % 4 == 0:
            copies[4 + leaf // 4].wait()
        total = None
        for comp in range(3):
            row = dens_ref[comp : comp + 1, leaf * LANES : (leaf + 1) * LANES]
            row = row.astype(BF16).astype(F32)
            part = up_ref[leaf, :, comp * LANES : (comp + 1) * LANES].astype(F32) * row
            total = part if total is None else total + part
        cols = jnp.where(lane == leaf, jnp.sum(total, axis=1, keepdims=True), cols)
    step = width - LANES
    reps = LANES // step
    tails = jnp.concatenate([cols[LANES:]] * reps, 0).T[:leaf_num]
    tails = jnp.where(iota(tails.shape, 1) // step == iota(tails.shape, 0) % reps, tails, 0.0)
    tails = [jnp.sum(tails[i : i + reps], axis=0, keepdims=True) for i in range(0, leaf_num, reps)]
    rows = jnp.concatenate([cols[:LANES].T[:leaf_num]] + tails, 0)
    rows = jnp.concatenate([rows] * 8, 0).astype(BF16)
    for i in range(out_ref.shape[0] // rows.shape[0]):
        out_ref[i * rows.shape[0] : (i + 1) * rows.shape[0]] = rows


def split(x):
    high = x.astype(BF16).astype(F32)
    mid = (x - high).astype(BF16).astype(F32)
    low = (x - high - mid).astype(BF16).astype(F32)
    return high, mid, low


TARGET_PARTS = (0, 0, 1, 0, 2, 1)
SOURCE_PARTS = (0, 1, 0, 2, 0, 1)


def target_rows(tile):
    row = iota(tile.shape, 0)
    x = jnp.where(row < 3, tile, 0.0)
    f = jnp.where(row < 3, pltpu.roll(tile, 5, 0), 0.0)
    norm = jnp.sum(x * x, axis=0, keepdims=True) + BLOB
    cross = jnp.sum(x * f, axis=0, keepdims=True)
    parts, norms, crosses = split(tile), split(norm), split(cross)
    out = []
    for q in range(6):
        extra = norms[q] if q < 3 else crosses[q - 3]
        out.append(jnp.where(row < 6, parts[TARGET_PARTS[q]], jnp.where(row == 6, extra, 1.0 if q < 3 else 0.0)))
    return jnp.concatenate(out, 0)


def source_rows(tile):
    row = iota(tile.shape, 0)
    first, second = row < 3, (row >= 3) & (row < 6)
    x = jnp.where(first, tile, 0.0)
    f = jnp.where(first, pltpu.roll(tile, 5, 0), 0.0)
    norms = split(jnp.sum(x * x, axis=0, keepdims=True))
    crosses = split(-3.0 * jnp.sum(x * f, axis=0, keepdims=True))
    parts = split(tile)
    low = split(pltpu.roll(tile, 3, 0))
    triple = split(3.0 * f)
    rho, ab, ar, br = [], [], [], []
    for q in range(6):
        k = SOURCE_PARTS[q]
        main = jnp.where(first, -2.0 * parts[k], 0.0)
        if q < 3:
            main = jnp.where(row == 6, 1.0, jnp.where(row == 7, norms[q], main))
        rho.append(main)
        ab.append(jnp.where(second, parts[k], 0.0))
        ar.append(jnp.where(second, -low[k], jnp.where(row == 6, 0.0 if q < 3 else 1.0, 0.0)))
        br.append(jnp.where(first, triple[k], jnp.where(row == 7, crosses[q], 0.0) if q < 3 else 0.0))
    return [jnp.concatenate(rows, 0).astype(BF16) for rows in (rho, ab, ar, br)]


def middle_body(own_ref, pair_ref, next_ref, count_hbm, slot_hbm, class_hbm, req_hbm, table_hbm, near_ref, slot_ref, req_ref, kind_ref, kept_ref, table, count_ref, class_ref, sems, win, lhs, rhs, acc, list_v, list_s, pairs, sem, flip):
    pairs_of = ((table_hbm, table), (count_hbm, count_ref), (slot_hbm, slot_ref), (class_hbm, class_ref), (req_hbm, req_ref))
    fetches = [pltpu.make_async_copy(a, b, sems.at[i]) for i, (a, b) in enumerate(pairs_of)]
    for fetch in fetches:
        fetch.start()
    near_terms(own_ref, pair_ref, next_ref, near_ref, win, lhs, rhs, acc, list_v, list_s, pairs, sem)
    for fetch in fetches:
        fetch.wait()
    keep_rows(table, kept_ref)
    class_terms(count_ref, class_ref, kind_ref, flip)


def keep_rows(table, kept_ref):
    first = kept_ref.shape[0] - GROUP
    classes = table.shape[0]
    kept_ref[:first] = table[:first]
    whole = classes - classes % 8
    start = (classes - 1) // GROUP * GROUP
    width = 9 * LANES
    for at in range(0, table.shape[1], width):
        cols = slice(at, at + width)
        tail = table[whole:classes, cols].astype(F32)
        tail = jnp.concatenate([tail, jnp.zeros((start + GROUP - classes, width), F32)], 0)
        both = jnp.concatenate([table[start:whole, cols].astype(F32), tail], 0)
        kept_ref[first:, cols] = both.astype(BF16)


def near_terms(own_ref, pair_ref, next_ref, near_ref, win, lhs, rhs, acc, list_v, list_s, pairs, sem):
    leaf_num = acc.shape[0] - 1
    nodes = leaf_num * LANES
    slots = list_v.shape[1]
    device = lax.axis_index("patch")
    odd = device & 1
    inner = (device > 0) & (device < lax.axis_size("patch") - 1)
    halo = (pair_ref, own_ref, next_ref)
    starts = ((1 - odd) * (2 * leaf_num), leaf_num, odd * (2 * leaf_num))
    leaf_of = iota((slots, LANES), 1)
    for place, ref in enumerate(halo):
        listed = ref[:, nodes:].astype(jnp.int32)
        source = listed - (device * leaf_num + 1)
        limit = leaf_num if place < 2 else jnp.where(inner, leaf_num, 0)
        mine = (listed > 0) & (source >= 0) & (source < limit)
        list_v[place] = jnp.where(mine, (source << 6) + (leaf_of + starts[place]), -1)
        if place == 1:
            list_v[3] = jnp.where(listed > 0, (leaf_of << 6) + (source + leaf_num), -1)
    copy = pltpu.make_async_copy(list_v, list_s, sem)
    copy.start()

    def clear(leaf, _):
        acc[leaf] = jnp.zeros(acc.shape[1:], F32)
        return 0

    lax.fori_loop(0, leaf_num, clear, 0)
    lhs[leaf_num] = jnp.zeros(lhs.shape[1:], BF16)
    copy.wait()
    dead, seen = jnp.int32(0), 0
    for leaf in range(leaf_num):
        for place, ref in enumerate(halo):
            tile = ref[:, leaf * LANES : (leaf + 1) * LANES]
            win[starts[place] + leaf] = tile
            for k, rows in enumerate(source_rows(tile)):
                rhs[starts[place] + leaf, :, k * LANES : (k + 1) * LANES] = rows
            if place == 1:
                rows = target_rows(tile)
                rows = jnp.concatenate([rows, jnp.zeros((LANES - rows.shape[0], LANES), F32)], 0)
                lhs[leaf] = rows.T.astype(BF16)
        for place in range(list_s.shape[0]):
            for slot in range(slots):
                code = list_s[place, slot, leaf]
                pairs[dead + seen] = code
                dead = dead + (code >> 31)
                seen = seen + 1
    count = dead + seen
    for i in range(3 * DEPTH):
        pairs[count + i] = leaf_num * 64

    def products(at, bufs, register):
        pair = pairs[at]
        left = jnp.concatenate([lhs[pair >> 6], jnp.zeros((LANES, LANES), BF16)], 1)
        for unit, buf in enumerate(bufs):
            right = rhs[pair & 63, :, unit * 2 * LANES : (unit + 1) * 2 * LANES]
            right = jnp.concatenate([right, jnp.zeros((2 * LANES - right.shape[0], 2 * LANES), BF16)], 0)
            pltpu.matmul_push_rhs(right, staging_register=register, mxu_index=unit)
            pltpu.matmul_acc_lhs(buf, left, load_staged_rhs=register)

    def add_terms(at, bufs):
        pair = pairs[at]
        target, source = pair >> 6, pair & 63
        row = [jnp.broadcast_to(win[source, k : k + 1], (8, LANES)) for k in range(6)]
        first, second = [pltpu.matmul_pop(buf) for buf in bufs]
        for part in range(LANES // 8):
            i = slice(part * 8, part * 8 + 8)
            rho_sq, ab = first[i, :LANES], first[i, LANES:]
            ar, br = second[i, :LANES], second[i, LANES:]
            inv_one = lax.rsqrt(rho_sq)
            inv_two = inv_one * inv_one
            inv_three = inv_two * inv_one
            coef = (ab + ar * br * inv_two) * inv_three
            ar = ar * inv_three
            acc[target, 0, i] += br * inv_three
            acc[target, 1, i] += coef
            for k in range(3):
                acc[target, 2 + k, i] += row[3 + k] * ar + row[k] * coef

    def run(*bufs):
        bufs = [bufs[i : i + 2] for i in range(0, 4 * DEPTH, 2)]
        for pair in bufs:
            for buf in pair:
                pltpu.matmul_pop(buf)
        for i in range(DEPTH):
            products(i, bufs[i], i % 2)

        def blocks(step, _):
            start = step * (2 * DEPTH)
            for i in range(DEPTH):
                products(start + DEPTH + i, bufs[DEPTH + i], i % 2)
            for i in range(DEPTH):
                add_terms(start + i, bufs[i])
            for i in range(DEPTH):
                products(start + 2 * DEPTH + i, bufs[i], i % 2)
            for i in range(DEPTH):
                add_terms(start + DEPTH + i, bufs[DEPTH + i])
            return 0

        lax.fori_loop(0, (count + 2 * DEPTH - 1) // (2 * DEPTH), blocks, 0)
        for pair in bufs[:DEPTH]:
            for buf in pair:
                pltpu.matmul_pop(buf)

    pl.run_scoped(run, *[pltpu.ACC(i % 2)((LANES, 2 * LANES), F32) for i in range(4 * DEPTH)])
    lane = iota((LANES, LANES), 1)
    for leaf in range(leaf_num):
        flat = jnp.zeros((LANES, LANES), F32)
        for k in range(5):
            flat = jnp.where(lane == k, jnp.sum(acc[leaf, k], axis=1, keepdims=True), flat)
        flat = flat.T
        tile = win[leaf_num + leaf]
        total = flat[0:1] * tile[3:6] * (1.0 / 3.0) + flat[2:5] - flat[1:2] * tile[0:3]
        near_ref[:, leaf * LANES : (leaf + 1) * LANES] = total * KERNEL


def columns(scratch, value):
    rows, width = value.shape
    scratch[0:rows, 0:width] = value.astype(F32)
    return scratch[...].T


def class_terms(count_ref, class_ref, kind_ref, scratch):
    leaf_num, far_num = class_ref.shape
    scratch[...] = jnp.zeros((LANES, LANES), F32)
    classes = columns(scratch, class_ref[...])
    lane = iota((far_num, LANES), 1)
    row = iota((far_num, LANES), 0)
    for leaf in range(leaf_num):
        at = slice(leaf * far_num, (leaf + 1) * far_num)
        kind = jnp.broadcast_to(classes[:far_num, leaf : leaf + 1], (far_num, LANES)).astype(jnp.int32)
        keep = (remainder(lane, leaf_num) == leaf) & (row < count_ref[leaf])
        kind_ref[at] = jnp.where(keep, kind - quotient(lane, leaf_num), -LANES).astype(BF16)


def slot_terms(rows, slot_ref, req_ref, main_ref, tail_ref, code_ref, scratch):
    leaf_num, far_num = slot_ref.shape
    cap, peers = req_ref.shape
    reps = LANES // leaf_num
    half = peers // 2
    scratch[...] = jnp.zeros((LANES, LANES), F32)
    asked = columns(scratch, req_ref[...])
    asked = jnp.concatenate([jnp.broadcast_to(asked[:, t : t + 1], (peers, LANES)) for t in range(cap)], 0)
    asked = asked.astype(BF16)
    slots = columns(scratch, slot_ref[...])
    slot = jnp.concatenate([jnp.broadcast_to(slots[:far_num, i : i + 1], (far_num, LANES)) for i in range(leaf_num)], 0)
    slot = slot.astype(jnp.int32)
    lane = iota(slot.shape, 1)
    peer = quotient(slot, cap)
    key = (slot - peer * cap) * peers + peer - lane
    picks = [jnp.where(key == t * peers, 1.0, 0.0).astype(BF16) for t in range(cap)]
    local = jnp.dot(jnp.concatenate(picks, 1), asked, preferred_element_type=F32).astype(jnp.int32)
    upper = (peer >= half).astype(jnp.int32)
    base = (peer - upper * half) * rows

    def code(row):
        return jnp.where(lane == remainder(row, LANES), quotient(row, LANES), -1).astype(BF16)

    main_ref[...] = code(base + local)
    tail_ref[...] = code(base + leaf_num + quotient(local, reps))
    code_ref[...] = (upper + 2 * (quotient(lane, leaf_num) == remainder(local, reps)).astype(jnp.int32)).astype(BF16)


def far_body(mom_ref, slot_ref, req_ref, kind_ref, kept_ref, own_ref, near_ref, table_hbm, down_hbm, out_ref, main_ref, tail_ref, code_ref, flip, table, down, pad, sums, sem):
    early = kept_ref.shape[0] - GROUP
    fetch = pltpu.make_async_copy(table_hbm.at[pl.ds(early, table.shape[0])], table, sem.at[0])
    fetch_down = pltpu.make_async_copy(down_hbm, down, sem.at[1])
    fetch.start()
    fetch_down.start()
    leaf_num, quads, width, _ = down.shape
    groups = pad.shape[0]
    lead = 2 * LANES - width
    cols = GROUP * leaf_num

    @pl.when(lax.axis_index("patch") >= 0)
    def _():
        slot_terms(mom_ref.shape[0] // (req_ref.shape[1]), slot_ref, req_ref, main_ref, tail_ref, code_ref, flip)
        half = mom_ref.shape[0] // 2
        both = jnp.concatenate([mom_ref[:half], mom_ref[half:]], 1)
        one, zero = jnp.ones((), BF16), jnp.zeros((), BF16)

        def hots(ref, count, stride=1):
            codes = ref[...]
            return [jnp.where(codes == i * stride, one, zero) for i in range(count)]

        tiles = half // LANES
        main = jnp.dot(jnp.concatenate(hots(main_ref, tiles), 1), both, preferred_element_type=F32)
        tails = jnp.dot(jnp.concatenate(hots(tail_ref, tiles), 1), both, preferred_element_type=F32)
        code = code_ref[...].astype(F32)
        upper = (code == 1.0) | (code == 3.0)
        main = jnp.where(upper, main[:, LANES:], main[:, :LANES]).T
        tails = jnp.where(upper, tails[:, LANES:], tails[:, :LANES])
        tails = jnp.where(code >= 2, tails, 0.0).T
        extra = width - LANES
        tails = sum(tails[i * extra : (i + 1) * extra] for i in range(LANES // extra))
        src_t = jnp.concatenate([main, tails], 0).astype(BF16)
        per = cols // LANES
        hot = hots(kind_ref, groups * per, LANES // leaf_num)
        for g in range(groups):
            pad[g, 0:lead] = jnp.zeros((lead, cols), BF16)
            pad[g, lead + width :] = jnp.zeros((pad.shape[1] - lead - width, cols), BF16)
            part = jnp.dot(src_t, jnp.concatenate(hot[g * per : (g + 1) * per], 1), preferred_element_type=F32)
            pad[g, lead : lead + width] = part.astype(BF16)

    fetch.wait()
    step = width - LANES
    period = LANES // step
    tiles = period + 1
    blocks = width // period
    same = quotient(iota((blocks, GROUP, cols), 2), leaf_num) == iota((blocks, GROUP, cols), 1)
    for r in range(period):
        acc = None
        for g in range(groups):
            if g == groups - 1:
                ref, first = kept_ref, early
            elif g * GROUP < early:
                ref, first = kept_ref, g * GROUP
            else:
                ref, first = table, g * GROUP - early
            rows = [ref[first : first + GROUP, (tiles * b + r) * LANES : (tiles * b + r + 2) * LANES] for b in range(blocks)]
            part = jnp.dot(jnp.concatenate(rows, 0), pad[g, lead - step * r : lead - step * r + 2 * LANES], preferred_element_type=F32)
            acc = part if acc is None else acc + part
        acc = jnp.where(same, acc.reshape(blocks, GROUP, cols), 0.0)
        acc = jnp.sum(acc, axis=1)
        for h in range(cols // LANES):
            sums[h, pl.ds(r, blocks, stride=period), :] = acc[:, h * LANES : (h + 1) * LANES]
    fold = jnp.where(remainder(iota((leaf_num, cols), 1), leaf_num) == iota((leaf_num, cols), 0), 1.0, 0.0)
    whole = jnp.concatenate([sums[h] for h in range(cols // LANES)], 1)
    expansion = lax.dot_general(fold, whole, (((1,), (1,)), ((), ())), precision=lax.Precision.HIGHEST, preferred_element_type=F32)
    fetch_down.wait()
    which = iota((leaf_num, width), 0)
    field = [None] * quads
    for leaf in range(leaf_num):
        lhs = jnp.where(which == leaf, expansion, 0.0).astype(BF16)
        for q in range(0, quads, 2):
            both = [down[leaf, i] for i in range(q, min(q + 2, quads))]
            part = jnp.dot(lhs, jnp.concatenate(both, 1), preferred_element_type=F32)
            field[q] = part if field[q] is None else field[q] + part
    quad = [field[q - q % 2][:, (q % 2) * LANES : (q % 2 + 1) * LANES] for q in range(quads)]
    for leaf in range(leaf_num):
        at = slice(leaf * LANES, (leaf + 1) * LANES)
        far = []
        for k in range(3):
            far.append(sum(own_ref[3 + c : 4 + c, at] * quad[3 * c + k][leaf : leaf + 1] for c in range(3)))
        out_ref[:, at] = near_ref[:, at] + jnp.concatenate(far, 0)


SMEM = pl.BlockSpec(memory_space=pltpu.SMEM)
VMEM = pl.BlockSpec(memory_space=pltpu.VMEM)
HBM = pl.BlockSpec(memory_space=pltpu.HBM)


def held(x, space=pltpu.VMEM):
    return pltpu.with_memory_space_constraint(x, space)


def call(body, outs, limit, **options):
    if outs is not None:
        shapes = tuple(pltpu.VMEM(o[:-1], o[-1]) for o in outs)
        options["out_shape"] = shapes if len(shapes) > 1 else shapes[0]
    params = pltpu.CompilerParams(vmem_limit_bytes=limit * 2**20)
    return pl.pallas_call(body, compiler_params=params, **options)


def per_device(positions, densities, near_src, near_count, far_slot, far_class, far_count, requests, up_basis, transfer_table, down_basis):
    leaf_num, slot_num = near_src.shape
    nodes = positions.shape[1]
    width = up_basis.shape[1]
    far_num = far_slot.shape[1]
    peers = requests.shape[1]
    classes = transfer_table.shape[0]
    groups = -(-classes // GROUP)
    rows = leaf_num * width // LANES
    pairs = [(i, i ^ 1) for i in range(peers)]
    nexts = [(i, i if i in (0, peers - 1) else ((i + 1) ^ 1) - 1) for i in range(peers)]
    slots = leaf_num * far_num
    own, message = call(
        front_body,
        [(8, nodes + LANES, F32), (peers * rows, LANES, BF16)],
        8,
        in_specs=[HBM] * 5,
        scratch_shapes=[
            pltpu.VMEM((3, nodes), F32),
            pltpu.VMEM((3, nodes), F32),
            pltpu.VMEM((slot_num, leaf_num), jnp.int32),
            pltpu.VMEM((1, leaf_num), jnp.int32),
            pltpu.VMEM(up_basis.shape, BF16),
            pltpu.SemaphoreType.DMA((4 + leaf_num // 4,)),
        ],
    )(*[held(x, pltpu.HBM) for x in (positions, densities, near_src.T, near_count[None], up_basis)])
    next_own = lax.ppermute(own, "patch", nexts)
    pair_own = lax.ppermute(own, "patch", pairs)
    message = message.reshape(peers, rows // 2, 2, LANES)
    table = lax.all_to_all(message, "patch", split_axis=0, concat_axis=0, tiled=True)
    table = table.reshape(peers * rows, LANES)
    down_flat = down_basis.transpose(0, 2, 1, 3)
    near, *kept = call(
        middle_body,
        [
            (3, nodes, F32),
            far_slot.shape + (jnp.int32,),
            (requests.shape[2], peers, jnp.int32),
            (slots, LANES, BF16),
            ((EARLY + 1) * GROUP, width * width, BF16),
        ],
        36,
        in_specs=[VMEM] * 3 + [HBM] * 5,
        scratch_shapes=[
            pltpu.VMEM(transfer_table.shape, BF16),
            pltpu.SMEM(far_count.shape, jnp.int32),
            pltpu.VMEM(far_class.shape, jnp.int32),
            pltpu.SemaphoreType.DMA((5,)),
            pltpu.VMEM((3 * leaf_num, 8, LANES), F32),
            pltpu.VMEM((leaf_num + 1, LANES, LANES), BF16),
            pltpu.VMEM((3 * leaf_num, 48, 4 * LANES), BF16),
            pltpu.VMEM((leaf_num + 1, 5, LANES, LANES), F32),
            pltpu.VMEM((4, slot_num, LANES), jnp.int32),
            pltpu.SMEM((4, slot_num, LANES), jnp.int32),
            pltpu.SMEM((4 * leaf_num * slot_num + 3 * DEPTH,), jnp.int32),
            pltpu.SemaphoreType.DMA,
            pltpu.VMEM((LANES, LANES), F32),
        ],
    )(held(own), held(pair_own), held(next_own), *[held(x, pltpu.HBM) for x in (far_count, far_slot, far_class, requests[0].T, transfer_table)])
    return call(
        far_body,
        None,
        30,
        in_specs=[VMEM] * 7 + [HBM] * 2,
        out_shape=jax.ShapeDtypeStruct((3, nodes), F32),
        scratch_shapes=[
            pltpu.VMEM((slots, LANES), BF16),
            pltpu.VMEM((slots, LANES), BF16),
            pltpu.VMEM((slots, LANES), BF16),
            pltpu.VMEM((LANES, LANES), F32),
            pltpu.VMEM(((groups - 1 - EARLY) * GROUP, width * width), BF16),
            pltpu.VMEM(down_flat.shape, BF16),
            pltpu.VMEM((groups, 4 * LANES - width, GROUP * leaf_num), BF16),
            pltpu.VMEM((GROUP * leaf_num // LANES, width, LANES), F32),
            pltpu.SemaphoreType.DMA((2,)),
        ],
    )(*[held(x) for x in (table, *kept, own, near)], held(transfer_table, pltpu.HBM), held(down_flat, pltpu.HBM))


def solution(mesh):
    placed = (
        P(None, "patch"),
        P(None, "patch"),
        P("patch", None),
        P("patch"),
        P("patch", None),
        P("patch", None),
        P("patch"),
        P("patch", None, None),
        P("patch", None, None),
        P(),
        P("patch", None, None, None),
    )
    return jax.shard_map(per_device, mesh=mesh, in_specs=placed, out_specs=P(None, "patch"), check_vma=False)
```

```python
import math

import jax
import jax.numpy as jnp
from jax import lax
from jax.experimental import pallas as pl
from jax.experimental.pallas import tpu as pltpu
from jax.sharding import PartitionSpec as P


KERNEL = 1.0 / (8.0 * math.pi)
BLOB = 0.25
LANES = 128
DEPTH = 3
EARLY = 2
GROUP = 16
F32 = jnp.float32
BF16 = jnp.bfloat16


def iota(shape, dim):
    return lax.broadcasted_iota(jnp.int32, shape, dim)


def quotient(x, n):
    return x >> (n.bit_length() - 1) if n & (n - 1) == 0 else x // n


def remainder(x, n):
    return x & (n - 1) if n & (n - 1) == 0 else x % n


def front_body(pos_hbm, dens_hbm, src_hbm, count_hbm, up_hbm, own_ref, out_ref, pos_ref, dens_ref, src_ref, count_ref, up_ref, sem):
    refs = [(pos_hbm, pos_ref), (dens_hbm, dens_ref), (src_hbm, src_ref), (count_hbm, count_ref)]
    refs += [(up_hbm.at[pl.ds(i, 4)], up_ref.at[pl.ds(i, 4)]) for i in range(0, up_ref.shape[0], 4)]
    copies = [pltpu.make_async_copy(a, b, sem.at[i]) for i, (a, b) in enumerate(refs)]
    for copy in copies:
        copy.start()
    leaf_num, width, _ = up_ref.shape
    nodes = pos_ref.shape[1]
    slots = src_ref.shape[0]
    own_ref[6:, :nodes] = jnp.zeros((2, nodes), F32)
    own_ref[:, nodes:] = jnp.zeros((slots, LANES), F32)
    for copy in copies[:4]:
        copy.wait()
    own_ref[0:3, :nodes] = pos_ref[...]
    own_ref[3:6, :nodes] = dens_ref[...]
    live = iota((slots, leaf_num), 0) < count_ref[...]
    own_ref[:, nodes : nodes + leaf_num] = jnp.where(live, src_ref[...] + 1, 0).astype(F32)
    lane = iota((width, LANES), 1)
    cols = jnp.zeros((width, LANES), F32)
    for leaf in range(leaf_num):
        if leaf % 4 == 0:
            copies[4 + leaf // 4].wait()
        total = None
        for comp in range(3):
            row = dens_ref[comp : comp + 1, leaf * LANES : (leaf + 1) * LANES]
            row = row.astype(BF16).astype(F32)
            part = up_ref[leaf, :, comp * LANES : (comp + 1) * LANES].astype(F32) * row
            total = part if total is None else total + part
        cols = jnp.where(lane == leaf, jnp.sum(total, axis=1, keepdims=True), cols)
    step = width - LANES
    reps = LANES // step
    tails = jnp.concatenate([cols[LANES:]] * reps, 0).T[:leaf_num]
    tails = jnp.where(iota(tails.shape, 1) // step == iota(tails.shape, 0) % reps, tails, 0.0)
    tails = [jnp.sum(tails[i : i + reps], axis=0, keepdims=True) for i in range(0, leaf_num, reps)]
    rows = jnp.concatenate([cols[:LANES].T[:leaf_num]] + tails, 0)
    rows = jnp.concatenate([rows] * 8, 0).astype(BF16)
    for i in range(out_ref.shape[0] // rows.shape[0]):
        out_ref[i * rows.shape[0] : (i + 1) * rows.shape[0]] = rows


def split(x):
    high = x.astype(BF16).astype(F32)
    mid = (x - high).astype(BF16).astype(F32)
    low = (x - high - mid).astype(BF16).astype(F32)
    return high, mid, low


TARGET_PARTS = (0, 0, 1, 0, 2, 1)
SOURCE_PARTS = (0, 1, 0, 2, 0, 1)


def target_rows(tile):
    row = iota(tile.shape, 0)
    x = jnp.where(row < 3, tile, 0.0)
    f = jnp.where(row < 3, pltpu.roll(tile, 5, 0), 0.0)
    norm = jnp.sum(x * x, axis=0, keepdims=True) + BLOB
    cross = jnp.sum(x * f, axis=0, keepdims=True)
    parts, norms, crosses = split(tile), split(norm), split(cross)
    out = []
    for q in range(6):
        extra = norms[q] if q < 3 else crosses[q - 3]
        out.append(jnp.where(row < 6, parts[TARGET_PARTS[q]], jnp.where(row == 6, extra, 1.0 if q < 3 else 0.0)))
    return jnp.concatenate(out, 0)


def source_rows(tile):
    row = iota(tile.shape, 0)
    first, second = row < 3, (row >= 3) & (row < 6)
    x = jnp.where(first, tile, 0.0)
    f = jnp.where(first, pltpu.roll(tile, 5, 0), 0.0)
    norms = split(jnp.sum(x * x, axis=0, keepdims=True))
    crosses = split(-3.0 * jnp.sum(x * f, axis=0, keepdims=True))
    parts = split(tile)
    low = split(pltpu.roll(tile, 3, 0))
    triple = split(3.0 * f)
    rho, ab, ar, br = [], [], [], []
    for q in range(6):
        k = SOURCE_PARTS[q]
        main = jnp.where(first, -2.0 * parts[k], 0.0)
        if q < 3:
            main = jnp.where(row == 6, 1.0, jnp.where(row == 7, norms[q], main))
        rho.append(main)
        ab.append(jnp.where(second, parts[k], 0.0))
        ar.append(jnp.where(second, -low[k], jnp.where(row == 6, 0.0 if q < 3 else 1.0, 0.0)))
        br.append(jnp.where(first, triple[k], jnp.where(row == 7, crosses[q], 0.0) if q < 3 else 0.0))
    return [jnp.concatenate(rows, 0).astype(BF16) for rows in (rho, ab, ar, br)]


def middle_body(own_ref, pair_ref, next_ref, count_hbm, slot_hbm, class_hbm, req_hbm, table_hbm, near_ref, slot_ref, req_ref, kind_ref, kept_ref, table, count_ref, class_ref, sems, win, lhs, rhs, acc, list_v, list_s, pairs, sem, flip):
    pairs_of = ((table_hbm, table), (count_hbm, count_ref), (slot_hbm, slot_ref), (class_hbm, class_ref), (req_hbm, req_ref))
    fetches = [pltpu.make_async_copy(a, b, sems.at[i]) for i, (a, b) in enumerate(pairs_of)]
    for fetch in fetches:
        fetch.start()
    near_terms(own_ref, pair_ref, next_ref, near_ref, win, lhs, rhs, acc, list_v, list_s, pairs, sem)
    for fetch in fetches:
        fetch.wait()
    keep_rows(table, kept_ref)
    class_terms(count_ref, class_ref, kind_ref, flip)


def keep_rows(table, kept_ref):
    first = kept_ref.shape[0] - GROUP
    classes = table.shape[0]
    kept_ref[:first] = table[:first]
    whole = classes - classes % 8
    start = (classes - 1) // GROUP * GROUP
    width = 9 * LANES
    for at in range(0, table.shape[1], width):
        cols = slice(at, at + width)
        tail = table[whole:classes, cols].astype(F32)
        tail = jnp.concatenate([tail, jnp.zeros((start + GROUP - classes, width), F32)], 0)
        both = jnp.concatenate([table[start:whole, cols].astype(F32), tail], 0)
        kept_ref[first:, cols] = both.astype(BF16)


def near_terms(own_ref, pair_ref, next_ref, near_ref, win, lhs, rhs, acc, list_v, list_s, pairs, sem):
    leaf_num = acc.shape[0] - 1
    nodes = leaf_num * LANES
    slots = list_v.shape[1]
    device = lax.axis_index("patch")
    odd = device & 1
    inner = (device > 0) & (device < lax.axis_size("patch") - 1)
    halo = (pair_ref, own_ref, next_ref)
    starts = ((1 - odd) * (2 * leaf_num), leaf_num, odd * (2 * leaf_num))
    leaf_of = iota((slots, LANES), 1)
    for place, ref in enumerate(halo):
        listed = ref[:, nodes:].astype(jnp.int32)
        source = listed - (device * leaf_num + 1)
        limit = leaf_num if place < 2 else jnp.where(inner, leaf_num, 0)
        mine = (listed > 0) & (source >= 0) & (source < limit)
        list_v[place] = jnp.where(mine, (source << 6) + (leaf_of + starts[place]), -1)
        if place == 1:
            list_v[3] = jnp.where(listed > 0, (leaf_of << 6) + (source + leaf_num), -1)
    copy = pltpu.make_async_copy(list_v, list_s, sem)
    copy.start()

    def clear(leaf, _):
        acc[leaf] = jnp.zeros(acc.shape[1:], F32)
        return 0

    lax.fori_loop(0, leaf_num, clear, 0)
    lhs[leaf_num] = jnp.zeros(lhs.shape[1:], BF16)
    copy.wait()
    dead, seen = jnp.int32(0), 0
    for leaf in range(leaf_num):
        for place, ref in enumerate(halo):
            tile = ref[:, leaf * LANES : (leaf + 1) * LANES]
            win[starts[place] + leaf] = tile
            for k, rows in enumerate(source_rows(tile)):
                rhs[starts[place] + leaf, :, k * LANES : (k + 1) * LANES] = rows
            if place == 1:
                rows = target_rows(tile)
                rows = jnp.concatenate([rows, jnp.zeros((LANES - rows.shape[0], LANES), F32)], 0)
                lhs[leaf] = rows.T.astype(BF16)
        for place in range(list_s.shape[0]):
            for slot in range(slots):
                code = list_s[place, slot, leaf]
                pairs[dead + seen] = code
                dead = dead + (code >> 31)
                seen = seen + 1
    count = dead + seen
    for i in range(3 * DEPTH):
        pairs[count + i] = leaf_num * 64

    def products(at, bufs, register):
        pair = pairs[at]
        left = jnp.concatenate([lhs[pair >> 6], jnp.zeros((LANES, LANES), BF16)], 1)
        for unit, buf in enumerate(bufs):
            right = rhs[pair & 63, :, unit * 2 * LANES : (unit + 1) * 2 * LANES]
            right = jnp.concatenate([right, jnp.zeros((2 * LANES - right.shape[0], 2 * LANES), BF16)], 0)
            pltpu.matmul_push_rhs(right, staging_register=register, mxu_index=unit)
            pltpu.matmul_acc_lhs(buf, left, load_staged_rhs=register)

    def add_terms(at, bufs):
        pair = pairs[at]
        target, source = pair >> 6, pair & 63
        row = [jnp.broadcast_to(win[source, k : k + 1], (8, LANES)) for k in range(6)]
        first, second = [pltpu.matmul_pop(buf) for buf in bufs]
        for part in range(LANES // 8):
            i = slice(part * 8, part * 8 + 8)
            rho_sq, ab = first[i, :LANES], first[i, LANES:]
            ar, br = second[i, :LANES], second[i, LANES:]
            inv_one = lax.rsqrt(rho_sq)
            inv_two = inv_one * inv_one
            inv_three = inv_two * inv_one
            coef = (ab + ar * br * inv_two) * inv_three
            ar = ar * inv_three
            acc[target, 0, i] += br * inv_three
            acc[target, 1, i] += coef
            for k in range(3):
                acc[target, 2 + k, i] += row[3 + k] * ar + row[k] * coef

    def run(*bufs):
        bufs = [bufs[i : i + 2] for i in range(0, 4 * DEPTH, 2)]
        for pair in bufs:
            for buf in pair:
                pltpu.matmul_pop(buf)
        for i in range(DEPTH):
            products(i, bufs[i], i % 2)

        def blocks(step, _):
            start = step * (2 * DEPTH)
            for i in range(DEPTH):
                products(start + DEPTH + i, bufs[DEPTH + i], i % 2)
            for i in range(DEPTH):
                add_terms(start + i, bufs[i])
            for i in range(DEPTH):
                products(start + 2 * DEPTH + i, bufs[i], i % 2)
            for i in range(DEPTH):
                add_terms(start + DEPTH + i, bufs[DEPTH + i])
            return 0

        lax.fori_loop(0, (count + 2 * DEPTH - 1) // (2 * DEPTH), blocks, 0)
        for pair in bufs[:DEPTH]:
            for buf in pair:
                pltpu.matmul_pop(buf)

    pl.run_scoped(run, *[pltpu.ACC(i % 2)((LANES, 2 * LANES), F32) for i in range(4 * DEPTH)])
    lane = iota((LANES, LANES), 1)
    for leaf in range(leaf_num):
        flat = jnp.zeros((LANES, LANES), F32)
        for k in range(5):
            flat = jnp.where(lane == k, jnp.sum(acc[leaf, k], axis=1, keepdims=True), flat)
        flat = flat.T
        tile = win[leaf_num + leaf]
        total = flat[0:1] * tile[3:6] * (1.0 / 3.0) + flat[2:5] - flat[1:2] * tile[0:3]
        near_ref[:, leaf * LANES : (leaf + 1) * LANES] = total * KERNEL


def columns(scratch, value):
    rows, width = value.shape
    scratch[0:rows, 0:width] = value.astype(F32)
    return scratch[...].T


def class_terms(count_ref, class_ref, kind_ref, scratch):
    leaf_num, far_num = class_ref.shape
    scratch[...] = jnp.zeros((LANES, LANES), F32)
    classes = columns(scratch, class_ref[...])
    lane = iota((far_num, LANES), 1)
    row = iota((far_num, LANES), 0)
    for leaf in range(leaf_num):
        at = slice(leaf * far_num, (leaf + 1) * far_num)
        kind = jnp.broadcast_to(classes[:far_num, leaf : leaf + 1], (far_num, LANES)).astype(jnp.int32)
        keep = (remainder(lane, leaf_num) == leaf) & (row < count_ref[leaf])
        kind_ref[at] = jnp.where(keep, kind - quotient(lane, leaf_num), -LANES).astype(BF16)


def slot_terms(rows, slot_ref, req_ref, main_ref, tail_ref, code_ref, scratch):
    leaf_num, far_num = slot_ref.shape
    cap, peers = req_ref.shape
    reps = LANES // leaf_num
    half = peers // 2
    scratch[...] = jnp.zeros((LANES, LANES), F32)
    asked = columns(scratch, req_ref[...])
    asked = jnp.concatenate([jnp.broadcast_to(asked[:, t : t + 1], (peers, LANES)) for t in range(cap)], 0)
    asked = asked.astype(BF16)
    slots = columns(scratch, slot_ref[...])
    slot = jnp.concatenate([jnp.broadcast_to(slots[:far_num, i : i + 1], (far_num, LANES)) for i in range(leaf_num)], 0)
    slot = slot.astype(jnp.int32)
    lane = iota(slot.shape, 1)
    peer = quotient(slot, cap)
    key = (slot - peer * cap) * peers + peer - lane
    picks = [jnp.where(key == t * peers, 1.0, 0.0).astype(BF16) for t in range(cap)]
    local = jnp.dot(jnp.concatenate(picks, 1), asked, preferred_element_type=F32).astype(jnp.int32)
    upper = (peer >= half).astype(jnp.int32)
    base = (peer - upper * half) * rows

    def code(row):
        return jnp.where(lane == remainder(row, LANES), quotient(row, LANES), -1).astype(BF16)

    main_ref[...] = code(base + local)
    tail_ref[...] = code(base + leaf_num + quotient(local, reps))
    code_ref[...] = (upper + 2 * (quotient(lane, leaf_num) == remainder(local, reps)).astype(jnp.int32)).astype(BF16)


def far_body(mom_ref, slot_ref, req_ref, kind_ref, kept_ref, own_ref, near_ref, table_hbm, down_hbm, out_ref, main_ref, tail_ref, code_ref, flip, table, down, pad, sums, ahead, sem):
    early = kept_ref.shape[0] - GROUP
    fetch = pltpu.make_async_copy(table_hbm.at[pl.ds(early, table.shape[0])], table, sem.at[0])
    fetch_down = pltpu.make_async_copy(down_hbm, down, sem.at[1])
    fetch.start()
    fetch_down.start()
    leaf_num, quads, width, _ = down.shape
    groups = pad.shape[0]
    lead = 2 * LANES - width
    cols = GROUP * leaf_num

    step = width - LANES
    period = LANES // step
    steps = period + 1
    blocks = width // period
    early_groups = [g for g in range(groups) if g * GROUP < early or g == groups - 1]
    late_groups = [g for g in range(groups) if g not in early_groups]

    def products(r, chosen):
        acc = None
        for g in chosen:
            if g == groups - 1:
                ref, first = kept_ref, early
            elif g * GROUP < early:
                ref, first = kept_ref, g * GROUP
            else:
                ref, first = table, g * GROUP - early
            rows = [ref[first : first + GROUP, (steps * b + r) * LANES : (steps * b + r + 2) * LANES] for b in range(blocks)]
            part = jnp.dot(jnp.concatenate(rows, 0), pad[g, lead - step * r : lead - step * r + 2 * LANES], preferred_element_type=F32)
            acc = part if acc is None else acc + part
        return acc

    @pl.when(lax.axis_index("patch") >= 0)
    def _():
        slot_terms(mom_ref.shape[0] // (req_ref.shape[1]), slot_ref, req_ref, main_ref, tail_ref, code_ref, flip)
        half = mom_ref.shape[0] // 2
        both = jnp.concatenate([mom_ref[:half], mom_ref[half:]], 1)
        one, zero = jnp.ones((), BF16), jnp.zeros((), BF16)

        def hots(ref, count, stride=1):
            codes = ref[...]
            return [jnp.where(codes == i * stride, one, zero) for i in range(count)]

        tiles = half // LANES
        main = jnp.dot(jnp.concatenate(hots(main_ref, tiles), 1), both, preferred_element_type=F32)
        tails = jnp.dot(jnp.concatenate(hots(tail_ref, tiles), 1), both, preferred_element_type=F32)
        code = code_ref[...].astype(F32)
        upper = (code == 1.0) | (code == 3.0)
        main = jnp.where(upper, main[:, LANES:], main[:, :LANES]).T
        tails = jnp.where(upper, tails[:, LANES:], tails[:, :LANES])
        tails = jnp.where(code >= 2, tails, 0.0).T
        extra = width - LANES
        tails = sum(tails[i * extra : (i + 1) * extra] for i in range(LANES // extra))
        src_t = jnp.concatenate([main, tails], 0).astype(BF16)
        per = cols // LANES
        hot = hots(kind_ref, groups * per, LANES // leaf_num)
        for g in range(groups):
            pad[g, 0:lead] = jnp.zeros((lead, cols), BF16)
            pad[g, lead + width :] = jnp.zeros((pad.shape[1] - lead - width, cols), BF16)
            part = jnp.dot(src_t, jnp.concatenate(hot[g * per : (g + 1) * per], 1), preferred_element_type=F32)
            pad[g, lead : lead + width] = part.astype(BF16)

        for r in range(period):
            ahead[r] = products(r, early_groups)

    fetch.wait()
    same = quotient(iota((blocks, GROUP, cols), 2), leaf_num) == iota((blocks, GROUP, cols), 1)
    for r in range(period):
        acc = ahead[r] + products(r, late_groups)
        acc = jnp.where(same, acc.reshape(blocks, GROUP, cols), 0.0)
        acc = jnp.sum(acc, axis=1)
        for h in range(cols // LANES):
            sums[h, pl.ds(r, blocks, stride=period), :] = acc[:, h * LANES : (h + 1) * LANES]
    fold = jnp.where(remainder(iota((leaf_num, cols), 1), leaf_num) == iota((leaf_num, cols), 0), 1.0, 0.0)
    whole = jnp.concatenate([sums[h] for h in range(cols // LANES)], 1)
    expansion = lax.dot_general(fold, whole, (((1,), (1,)), ((), ())), precision=lax.Precision.HIGHEST, preferred_element_type=F32)
    fetch_down.wait()
    which = iota((leaf_num, width), 0)
    field = [None] * quads
    for leaf in range(leaf_num):
        lhs = jnp.where(which == leaf, expansion, 0.0).astype(BF16)
        for q in range(0, quads, 2):
            both = [down[leaf, i] for i in range(q, min(q + 2, quads))]
            part = jnp.dot(lhs, jnp.concatenate(both, 1), preferred_element_type=F32)
            field[q] = part if field[q] is None else field[q] + part
    quad = [field[q - q % 2][:, (q % 2) * LANES : (q % 2 + 1) * LANES] for q in range(quads)]
    for leaf in range(leaf_num):
        at = slice(leaf * LANES, (leaf + 1) * LANES)
        far = []
        for k in range(3):
            far.append(sum(own_ref[3 + c : 4 + c, at] * quad[3 * c + k][leaf : leaf + 1] for c in range(3)))
        out_ref[:, at] = near_ref[:, at] + jnp.concatenate(far, 0)


SMEM = pl.BlockSpec(memory_space=pltpu.SMEM)
VMEM = pl.BlockSpec(memory_space=pltpu.VMEM)
HBM = pl.BlockSpec(memory_space=pltpu.HBM)


def held(x, space=pltpu.VMEM):
    return pltpu.with_memory_space_constraint(x, space)


def call(body, outs, limit, **options):
    if outs is not None:
        shapes = tuple(pltpu.VMEM(o[:-1], o[-1]) for o in outs)
        options["out_shape"] = shapes if len(shapes) > 1 else shapes[0]
    params = pltpu.CompilerParams(vmem_limit_bytes=limit * 2**20)
    return pl.pallas_call(body, compiler_params=params, **options)


def per_device(positions, densities, near_src, near_count, far_slot, far_class, far_count, requests, up_basis, transfer_table, down_basis):
    leaf_num, slot_num = near_src.shape
    nodes = positions.shape[1]
    width = up_basis.shape[1]
    far_num = far_slot.shape[1]
    peers = requests.shape[1]
    classes = transfer_table.shape[0]
    groups = -(-classes // GROUP)
    rows = leaf_num * width // LANES
    pairs = [(i, i ^ 1) for i in range(peers)]
    nexts = [(i, i if i in (0, peers - 1) else ((i + 1) ^ 1) - 1) for i in range(peers)]
    slots = leaf_num * far_num
    own, message = call(
        front_body,
        [(8, nodes + LANES, F32), (peers * rows, LANES, BF16)],
        8,
        in_specs=[HBM] * 5,
        scratch_shapes=[
            pltpu.VMEM((3, nodes), F32),
            pltpu.VMEM((3, nodes), F32),
            pltpu.VMEM((slot_num, leaf_num), jnp.int32),
            pltpu.VMEM((1, leaf_num), jnp.int32),
            pltpu.VMEM(up_basis.shape, BF16),
            pltpu.SemaphoreType.DMA((4 + leaf_num // 4,)),
        ],
    )(*[held(x, pltpu.HBM) for x in (positions, densities, near_src.T, near_count[None], up_basis)])
    pair_own = lax.ppermute(own, "patch", pairs)
    next_own = lax.ppermute(own, "patch", nexts)
    message = message.reshape(peers, rows // 2, 2, LANES)
    table = lax.all_to_all(message, "patch", split_axis=0, concat_axis=0, tiled=True)
    table = table.reshape(peers * rows, LANES)
    down_flat = down_basis.transpose(0, 2, 1, 3)
    near, *kept = call(
        middle_body,
        [
            (3, nodes, F32),
            far_slot.shape + (jnp.int32,),
            (requests.shape[2], peers, jnp.int32),
            (slots, LANES, BF16),
            ((EARLY + 1) * GROUP, width * width, BF16),
        ],
        36,
        in_specs=[VMEM] * 3 + [HBM] * 5,
        scratch_shapes=[
            pltpu.VMEM(transfer_table.shape, BF16),
            pltpu.SMEM(far_count.shape, jnp.int32),
            pltpu.VMEM(far_class.shape, jnp.int32),
            pltpu.SemaphoreType.DMA((5,)),
            pltpu.VMEM((3 * leaf_num, 8, LANES), F32),
            pltpu.VMEM((leaf_num + 1, LANES, LANES), BF16),
            pltpu.VMEM((3 * leaf_num, 48, 4 * LANES), BF16),
            pltpu.VMEM((leaf_num + 1, 5, LANES, LANES), F32),
            pltpu.VMEM((4, slot_num, LANES), jnp.int32),
            pltpu.SMEM((4, slot_num, LANES), jnp.int32),
            pltpu.SMEM((4 * leaf_num * slot_num + 3 * DEPTH,), jnp.int32),
            pltpu.SemaphoreType.DMA,
            pltpu.VMEM((LANES, LANES), F32),
        ],
    )(held(own), held(pair_own), held(next_own), *[held(x, pltpu.HBM) for x in (far_count, far_slot, far_class, requests[0].T, transfer_table)])
    return call(
        far_body,
        None,
        34,
        in_specs=[VMEM] * 7 + [HBM] * 2,
        out_shape=jax.ShapeDtypeStruct((3, nodes), F32),
        scratch_shapes=[
            pltpu.VMEM((slots, LANES), BF16),
            pltpu.VMEM((slots, LANES), BF16),
            pltpu.VMEM((slots, LANES), BF16),
            pltpu.VMEM((LANES, LANES), F32),
            pltpu.VMEM(((groups - 1 - EARLY) * GROUP, width * width), BF16),
            pltpu.VMEM(down_flat.shape, BF16),
            pltpu.VMEM((groups, 4 * LANES - width, GROUP * leaf_num), BF16),
            pltpu.VMEM((GROUP * leaf_num // LANES, width, LANES), F32),
            pltpu.VMEM((LANES // (width - LANES), GROUP * width // (LANES // (width - LANES)), GROUP * leaf_num), F32),
            pltpu.SemaphoreType.DMA((2,)),
        ],
    )(*[held(x) for x in (table, *kept, own, near)], held(transfer_table, pltpu.HBM), held(down_flat, pltpu.HBM))


def solution(mesh):
    placed = (
        P(None, "patch"),
        P(None, "patch"),
        P("patch", None),
        P("patch"),
        P("patch", None),
        P("patch", None),
        P("patch"),
        P("patch", None, None),
        P("patch", None, None),
        P(),
        P("patch", None, None, None),
    )
    return jax.shard_map(per_device, mesh=mesh, in_specs=placed, out_specs=P(None, "patch"), check_vma=False)
```
